32 devices in a mesh: dp: 4 (over z), row: 2 (over core), col: 4 (over y, x).
Axes of the slice: x: 2, y: 2, z: 4, core: 2. Of those that a mesh axis runs over, the one named last changes fastest.
Arguments:
- block_input: bfloat16 [4096, 2048], P(('dp', 'col'), 'row'), may hold values from -60 to 60
- segment_ids: int32 [8, 512], P('dp'), may hold values from 0 to 15, as said below
- positions: int32 [8, 512], P('dp'), may hold values from 0 to 511, as said below
- attention_gain: float32 [2048], P('row'), may hold values from 0.1 to 1.9
- attention_shift: float32 [2048], P('row'), may hold values from -3 to 3
- projection_weight: bfloat16 [2048, 3, 2048], P('row', None, 'col'), may hold values from -0.125 to 0.125
- projection_bias: float32 [3, 2048], P(None, 'col'), may hold values from -14 to 14
- mixing_weight: bfloat16 [2048, 2048], P('col', 'row'), may hold values from -0.25 to 0.25
- feedforward_gain: float32 [2048], P('row'), may hold values from 0.1 to 1.9
- feedforward_shift: float32 [2048], P('row'), may hold values from -3 to 3
- gating_weight: bfloat16 [2048, 2, 5632], P('row', None, 'col'), may hold values from -0.125 to 0.125
- lowering_weight: bfloat16 [5632, 2048], P('col', 'row'), may hold values from -0.109375 to 0.109375
- cotangent: bfloat16 [4096, 2048], P(('dp', 'col'), 'row'), may hold values from -6 to 6
Outputs:
- block_output: bfloat16 [4096, 2048], P(('dp', 'col'), 'row')
- input_grad: bfloat16 [4096, 2048], P(('dp', 'col'), 'row')
- attention_gain_grad: float32 [2048], P('row')
- attention_shift_grad: float32 [2048], P('row')
- projection_wgrad: float32 [2048, 3, 2048], P('row', None, 'col')
- projection_bgrad: float32 [3, 2048], P(None, 'col')
- mixing_wgrad: float32 [2048, 2048], P('col', 'row')
- feedforward_gain_grad: float32 [2048], P('row')
- feedforward_shift_grad: float32 [2048], P('row')
- gating_wgrad: float32 [2048, 2, 5632], P('row', None, 'col')
- lowering_wgrad: float32 [5632, 2048], P('col', 'row')
The draws below stay inside these ranges and needn't reach their ends.
Inputs may be any that keep to these rules, and one draw needn't show every extreme that they name: `segment_ids`: within each packed sequence the numbers start at 0 at its first token and never fall; at most 16 documents a sequence. `positions`: a token's offset from the first token of its document.
All inputs are finite; a program needn't handle non-finite values.
Results may differ from the reference program's by a relative error of at most 0.018.
The reference program's roundings to bfloat16 on the way count: a program that leaves them out, or rounds other values in their place, can miss the bound.
Values may be sent and summed in bfloat16 or wider, within the bound.
A program may use at most 192 MiB of HBM per device.

```python
import math
import jax
import jax.numpy as jnp
from jax import lax

D = 2048
FF = 5632
HD = 64
SEQ_LEN = 512
SEQS = 8
TOKENS = 4096


def layout_tables(key):
    inner = jax.random.fold_in(key, 7)
    order = jnp.arange(SEQ_LEN)
    sequence = jnp.arange(SEQS)[:, None]
    candidate = jax.random.randint(inner, (SEQS, SEQ_LEN), 0, 40) == 0
    candidate = candidate & (sequence != 0)
    candidate = candidate | (order == 0)[None, :]
    spacing = SEQ_LEN // 16
    candidate = candidate | (sequence == SEQS - 1) & (order % spacing == 0)[None, :]
    counted = jnp.cumsum(candidate.astype(jnp.int32), axis=1)
    starts_here = candidate & (counted <= 16)
    segment = jnp.cumsum(starts_here.astype(jnp.int32), axis=1) - 1
    begins = lax.cummax(jnp.where(starts_here, order[None, :], 0), axis=1)
    return (segment.astype(jnp.int32), (order[None, :] - begins).astype(jnp.int32))


def draw_segment_ids(key, part):
    return layout_tables(key)[0]


def draw_positions(key, part):
    return layout_tables(key)[1]


def draw_block_input(key, part):
    keys = jax.random.split(jax.random.fold_in(key, 11), 3)
    base = jnp.clip(jax.random.normal(keys[0], (TOKENS, D)), -6.0, 6.0)
    rows = jnp.exp(jax.random.uniform(keys[1], (TOKENS, 1), minval=math.log(0.4), maxval=math.log(4.0)))
    cols = jnp.exp(jnp.linspace(math.log(0.4), math.log(4.0), D) + jax.random.uniform(keys[2], (D,), minval=-0.2, maxval=0.2))
    return jnp.clip(base * rows * cols[None, :], -60.0, 60.0).astype(jnp.bfloat16)


def draw_projection_bias(key, part):
    keys = jax.random.split(jax.random.fold_in(key, 13), 1)
    return jnp.clip(0.3 * jax.random.normal(keys[0], (3, D)), -1.2, 1.2).astype(jnp.float32)


def level_of(key, shape, shards, least, high):
    level, own = 1.0, jax.random.fold_in(key, 6)
    for dim, parts in shards:
        heights = jnp.exp(jax.random.uniform(jax.random.fold_in(own, dim), (parts,), jnp.float32, least / len(shards), high / len(shards)))
        level = level * jnp.repeat(heights, shape[dim] // parts).reshape([-1 if axis == dim else 1 for axis in range(len(shape))])
    return level


def gaussian(rng, dims, scale, reach, cuts=(), kind=jnp.bfloat16):
    result = jax.random.normal(rng, dims, jnp.float32) * scale
    if len(cuts) > 0:
        result = level_of(rng, dims, cuts, -0.22, 0.18) * result
    return jnp.clip(result, min=-reach, max=reach).astype(kind)


def setup_inputs(seed: int = 0) -> dict:
    key_list = jax.random.split(jax.random.key(seed), 14)
    block_input = draw_block_input(jax.random.fold_in(key_list[13], 71), 0)
    segment_ids = draw_segment_ids(jax.random.fold_in(key_list[13], 71), 0)
    positions = draw_positions(jax.random.fold_in(key_list[13], 71), 0)
    attention_gain = jnp.clip(1.0 + 0.18 * jax.random.normal(key_list[3], (D,), jnp.float32), 0.1, 1.9)
    attention_shift = gaussian(key_list[4], (D,), 0.5, 3.0, ((0, 2),), jnp.float32)
    projection_weight = gaussian(key_list[5], (D, 3, D), D ** -0.5, 0.125, ((0, 2), (2, 4)))
    projection_bias = draw_projection_bias(jax.random.fold_in(key_list[13], 71), 0)
    mixing_weight = gaussian(key_list[7], (D, D), (D // 4) ** -0.5, 0.25, ((0, 4), (1, 2)))
    feedforward_gain = jnp.clip(1.0 + 0.18 * jax.random.normal(key_list[8], (D,), jnp.float32), 0.1, 1.9)
    feedforward_shift = gaussian(key_list[9], (D,), 0.5, 3.0, ((0, 2),), jnp.float32)
    gating_weight = gaussian(key_list[10], (D, 2, FF), D ** -0.5, 0.125, ((0, 2), (2, 4)))
    lowering_weight = gaussian(key_list[11], (FF, D), (FF // 2) ** -0.5, 0.109375, ((0, 4), (1, 2)))
    cotangent = gaussian(key_list[12], (TOKENS, D), 1.0, 6.0, ((0, 16), (1, 2)))
    return {"block_input": block_input, "segment_ids": segment_ids, "positions": positions, "attention_gain": attention_gain, "attention_shift": attention_shift, "projection_weight": projection_weight, "projection_bias": projection_bias, "mixing_weight": mixing_weight, "feedforward_gain": feedforward_gain, "feedforward_shift": feedforward_shift, "gating_weight": gating_weight, "lowering_weight": lowering_weight, "cotangent": cotangent}


EPSILON = 1e-05
MASKED = -1e+30

def rotary_tables(positions, head_size):
    half = head_size // 8
    freq = jnp.exp(jnp.arange(half, dtype=jnp.float32) * (-math.log(10000.0) / half))
    theta = positions.astype(jnp.float32)[..., None] * freq
    return (jnp.cos(theta), jnp.sin(theta))

def rotate_forward(values, cosine, sine):
    half = cosine.shape[-1]
    first = values[..., :half]
    second = values[..., half:2 * half]
    return jnp.concatenate([first * cosine - second * sine, second * cosine + first * sine, values[..., 2 * half:]], -1)

def rotate_backward(grads, cosine, sine):
    half = cosine.shape[-1]
    first = grads[..., :half]
    second = grads[..., half:2 * half]
    return jnp.concatenate([first * cosine + second * sine, second * cosine - first * sine, grads[..., 2 * half:]], -1)

def moments(values):
    center = lax.optimization_barrier(jnp.mean(values, -1, keepdims=True))
    spread = lax.optimization_barrier(jnp.mean(values * values, -1, keepdims=True)) - center * center
    inverse = lax.rsqrt(spread + EPSILON)
    return ((values - center) * inverse, inverse)

def norm_back(upstream, gain, scaled, inverse):
    weighted = upstream * gain
    return inverse * (weighted - lax.optimization_barrier(jnp.mean(weighted, -1, keepdims=True)) - scaled * lax.optimization_barrier(jnp.mean(weighted * scaled, -1, keepdims=True)))

def as_wire(values):
    return lax.optimization_barrier(values.astype(jnp.bfloat16)).astype(jnp.float32)

def one_sequence(params, tokens_in, segment, position, upstream):
    att_gain, att_shift, proj_w, proj_b, mix_w, ffn_gain, ffn_shift, gate_w, lower_w = params
    length = tokens_in.shape[0]
    heads = D // HD
    scale_factor = 1.0 / math.sqrt(HD)
    residual = tokens_in.astype(jnp.float32)
    scaled_one, inverse_one = moments(residual)
    normed_one = (scaled_one * att_gain + att_shift).astype(jnp.bfloat16)
    flat_proj = proj_w.reshape(D, 3 * D)
    projected = jnp.dot(normed_one, flat_proj, preferred_element_type=jnp.float32) + proj_b.reshape(3 * D)
    projected = projected.reshape(length, 3, heads, HD)
    cosine, sine = rotary_tables(position, HD)
    cosine = cosine[:, None, :]
    sine = sine[:, None, :]
    queries = rotate_forward(projected[:, 0], cosine, sine).astype(jnp.bfloat16)
    keys_rope = rotate_forward(projected[:, 1], cosine, sine).astype(jnp.bfloat16)
    values_here = projected[:, 2].astype(jnp.bfloat16)
    query_f = queries.astype(jnp.float32)
    key_f = keys_rope.astype(jnp.float32)
    value_f = values_here.astype(jnp.float32)
    order = jnp.arange(length)
    allowed = (segment[:, None] == segment[None, :]) & (order[None, :] <= order[:, None])
    scores = jnp.einsum('qhe,khe->hqk', query_f, key_f) * scale_factor
    scores = jnp.where(allowed[None], scores, MASKED)
    peak = lax.optimization_barrier(jnp.max(scores, -1, keepdims=True))
    raised = jnp.exp(scores - peak)
    denominator = lax.optimization_barrier(jnp.sum(raised, -1, keepdims=True))
    log_total = peak + jnp.log(denominator)
    probs = as_wire(raised / denominator)
    attended = jnp.einsum('hqk,khe->qhe', probs, value_f).astype(jnp.bfloat16).reshape(length, D)
    middle = residual + jnp.dot(attended, mix_w, preferred_element_type=jnp.float32)
    scaled_two, inverse_two = moments(middle)
    normed_two = (scaled_two * ffn_gain + ffn_shift).astype(jnp.bfloat16)
    flat_gate = gate_w.reshape(D, 2 * FF)
    gating = jnp.dot(normed_two, flat_gate, preferred_element_type=jnp.float32).reshape(length, 2, FF)
    gate_value = gating[:, 0]
    up_value = gating[:, 1]
    sigmoid_gate = jax.nn.sigmoid(gate_value)
    hidden = (gate_value * sigmoid_gate * up_value).astype(jnp.bfloat16)
    block_out = (middle + jnp.dot(hidden, lower_w, preferred_element_type=jnp.float32)).astype(jnp.bfloat16)
    hidden_grad = jnp.dot(upstream, lower_w.T, preferred_element_type=jnp.float32)
    lower_grad = jnp.dot(hidden.T, upstream, preferred_element_type=jnp.float32)
    gate_grad = hidden_grad * up_value * sigmoid_gate * (1.0 + gate_value * (1.0 - sigmoid_gate))
    up_grad = hidden_grad * gate_value * sigmoid_gate
    gating_back = jnp.stack([gate_grad, up_grad], 1).astype(jnp.bfloat16).reshape(length, 2 * FF)
    gate_wgrad = jnp.dot(normed_two.T, gating_back, preferred_element_type=jnp.float32).reshape(D, 2, FF)
    normed_two_grad = jnp.dot(gating_back, flat_gate.T, preferred_element_type=jnp.float32)
    ffn_gain_grad = lax.optimization_barrier(jnp.sum(normed_two_grad * scaled_two, 0))
    ffn_shift_grad = lax.optimization_barrier(jnp.sum(normed_two_grad, 0))
    middle_grad = upstream.astype(jnp.float32) + norm_back(normed_two_grad, ffn_gain, scaled_two, inverse_two)
    middle_wire = middle_grad.astype(jnp.bfloat16)
    mix_grad = jnp.dot(attended.T, middle_wire, preferred_element_type=jnp.float32)
    attended_grad = jnp.dot(middle_wire, mix_w.T, preferred_element_type=jnp.float32).astype(jnp.bfloat16)
    attended_grad_f = attended_grad.reshape(length, heads, HD).astype(jnp.float32)
    attended_f = attended.reshape(length, heads, HD).astype(jnp.float32)
    recovered = jnp.exp(scores - log_total)
    prob_grad = jnp.einsum('qhe,khe->hqk', attended_grad_f, value_f)
    row_dot = jnp.einsum('qhe,qhe->hq', attended_grad_f, attended_f)
    score_grad = as_wire(recovered * (prob_grad - row_dot[..., None]) * scale_factor)
    query_grad = jnp.einsum('hqk,khe->qhe', score_grad, key_f)
    key_grad = jnp.einsum('hqk,qhe->khe', score_grad, query_f)
    value_grad = jnp.einsum('hqk,qhe->khe', as_wire(recovered), attended_grad_f)
    query_grad = rotate_backward(query_grad, cosine, sine)
    key_grad = rotate_backward(key_grad, cosine, sine)
    proj_back = jnp.stack([query_grad, key_grad, value_grad], 1).astype(jnp.bfloat16).reshape(length, 3 * D)
    proj_bgrad = lax.optimization_barrier(jnp.sum(proj_back.astype(jnp.float32), 0)).reshape(3, D)
    proj_wgrad = jnp.dot(normed_one.T, proj_back, preferred_element_type=jnp.float32).reshape(D, 3, D)
    normed_one_grad = jnp.dot(proj_back, flat_proj.T, preferred_element_type=jnp.float32)
    att_gain_grad = lax.optimization_barrier(jnp.sum(normed_one_grad * scaled_one, 0))
    att_shift_grad = lax.optimization_barrier(jnp.sum(normed_one_grad, 0))
    input_back = (middle_grad + norm_back(normed_one_grad, att_gain, scaled_one, inverse_one)).astype(jnp.bfloat16)
    grads = (att_gain_grad, att_shift_grad, proj_wgrad, proj_bgrad, mix_grad, ffn_gain_grad, ffn_shift_grad, gate_wgrad, lower_grad)
    return (block_out, input_back, grads)

def reference(block_input, segment_ids, positions, attention_gain, attention_shift, projection_weight, projection_bias, mixing_weight, feedforward_gain, feedforward_shift, gating_weight, lowering_weight, cotangent):
    params = (attention_gain, attention_shift, projection_weight, projection_bias, mixing_weight, feedforward_gain, feedforward_shift, gating_weight, lowering_weight)
    inputs_seq = block_input.reshape(SEQS, SEQ_LEN, D)
    upstream_seq = cotangent.reshape(SEQS, SEQ_LEN, D)
    start = tuple((jnp.zeros(p.shape, jnp.float32) for p in params))

    def step(carry, item):
        tokens_in, segment, position, upstream = item
        block_out, input_back, grads = one_sequence(params, tokens_in, segment, position, upstream)
        return (tuple((a + b for a, b in zip(carry, grads))), (block_out, input_back))
    totals, (outputs, backs) = lax.scan(step, start, (inputs_seq, segment_ids, positions, upstream_seq))
    return (outputs.reshape(TOKENS, D), backs.reshape(TOKENS, D), totals[0], totals[1], totals[2], totals[3], totals[4], totals[5], totals[6], totals[7], totals[8])
```

```python
import functools
import math

import jax
import jax.numpy as jnp
from jax import lax
from jax.experimental import pallas as pl
from jax.experimental.pallas import tpu as pltpu
from jax.sharding import PartitionSpec as P

D = 2048
HD = 64


EPSILON = 1e-05
MASKED = -1e30
BF16 = jnp.bfloat16
F32 = jnp.float32


def col_swap(values, bit):
    count = lax.axis_size("col")
    return lax.ppermute(values, "col", [(i, i ^ bit) for i in range(count)])


def row_swap(values):
    return lax.ppermute(values, "row", [(0, 1), (1, 0)])


def gather_tokens(values):
    count = lax.axis_size("col")
    if count == 4:
        half = values.shape[0] // 2
        first = col_swap(values, 1)
        second = col_swap(values, 2)
        third_a = col_swap(second[:half], 1)
        third_b = col_swap(first[half:], 2)
        return jnp.concatenate([values, first, second, third_a, third_b], 0)
    bit = 1
    while bit < count:
        values = jnp.concatenate([values, col_swap(values, bit)], 0)
        bit *= 2
    return values


def sum_tokens(partial_rows):
    count = lax.axis_size("col")
    size = partial_rows.shape[0] // count
    if count == 4:
        half = size // 2
        own, first, second, third = (partial_rows[i * size : (i + 1) * size] for i in range(4))
        third = third.astype(BF16)
        got_a = col_swap(third[:half], 1).astype(F32)
        got_b = col_swap(third[half:], 2).astype(F32)
        to_second = jnp.concatenate([second[:half] + got_a, second[half:]], 0).astype(BF16)
        to_first = jnp.concatenate([first[:half], first[half:] + got_b], 0).astype(BF16)
        return own + col_swap(to_first, 1).astype(F32) + col_swap(to_second, 2).astype(F32)
    bit = count // 2
    while bit:
        kept = partial_rows.shape[0] // 2
        got = col_swap(partial_rows[kept:].astype(BF16), bit).astype(F32)
        partial_rows = partial_rows[:kept] + got
        bit //= 2
    return partial_rows


def row_sums(first, second):
    return lax.psum((first, second), "row")


def normalize(values):
    total, squares = row_sums(
        jnp.sum(values, 1, keepdims=True), jnp.sum(values * values, 1, keepdims=True)
    )
    center = total / D
    spread = squares / D - center * center
    inverse = lax.rsqrt(spread + EPSILON)
    return ((values - center) * inverse, inverse)


def norm_back(upstream, gain, scaled, inverse):
    weighted = upstream * gain
    total, mixed = row_sums(
        jnp.sum(weighted, 1, keepdims=True), jnp.sum(weighted * scaled, 1, keepdims=True)
    )
    return inverse * (weighted - total / D - scaled * (mixed / D))


def dot(a, b, kind=F32):
    return jnp.dot(a, b, preferred_element_type=F32).astype(kind)


def dot_t(a, b, kind=F32):
    return lax.dot_general(a, b, (((1,), (1,)), ((), ())), preferred_element_type=F32).astype(kind)


def t_dot(a, b, kind=F32):
    return lax.dot_general(a, b, (((0,), (0,)), ((), ())), preferred_element_type=F32).astype(kind)


def line_kernel(pieces, kinds, *refs):
    count = len(kinds)
    own, out = refs[:count], refs[count : 2 * count]
    inwards, part, across = (refs[(2 + k) * count : (3 + k) * count] for k in range(3))
    sent_in, got_in, got_across, sent_out, got_out = refs[5 * count :]
    size = lax.axis_size("dp")
    me = lax.axis_index("dp")
    half = size // 2
    low = me < half
    inner = jnp.where(low, me + 1, me - 1)
    outer = jnp.where(low, jnp.maximum(me - 1, 0), jnp.minimum(me + 1, size - 1))
    end = (me == 0) | (me == size - 1)
    middle = (me == half - 1) | (me == half)

    barrier = pltpu.get_barrier_semaphore()
    pl.semaphore_signal(
        barrier, inc=1, device_id={"dp": inner}, device_id_type=pl.DeviceIdType.MESH
    )

    @pl.when(jnp.logical_not(end))
    def _():
        pl.semaphore_signal(
            barrier, inc=1, device_id={"dp": outer}, device_id_type=pl.DeviceIdType.MESH
        )
        pl.semaphore_wait(barrier, 2)

    @pl.when(end)
    def _():
        pl.semaphore_wait(barrier, 1)

    def copy(source, target, sent, got, to):
        return pltpu.make_async_remote_copy(
            src_ref=source,
            dst_ref=target,
            send_sem=sent,
            recv_sem=got,
            device_id={"dp": to},
            device_id_type=pl.DeviceIdType.MESH,
        )

    def to_inner(k):
        a, start, rows = pieces[k]
        at = pl.ds(start, rows)
        return copy(own[a].at[at], inwards[a].at[at], sent_in.at[k], got_in.at[k], inner)

    def part_to_inner(k):
        a, start, rows = pieces[k]
        at = pl.ds(start, rows)
        return copy(part[a].at[at], inwards[a].at[at], sent_in.at[k], got_in.at[k], inner)

    def part_across(k):
        a, start, rows = pieces[k]
        at = pl.ds(start, rows)
        return copy(part[a].at[at], across[a].at[at], sent_in.at[k], got_across.at[k], inner)

    def to_outer(k):
        a, start, rows = pieces[k]
        at = pl.ds(start, rows)
        return copy(out[a].at[at], out[a].at[at], sent_out.at[k], got_out.at[k], outer)

    def add(first, second, target, k):
        a, start, rows = pieces[k]
        at = pl.ds(start, rows)
        target[a][at] = (
            first[a][at].astype(F32) + second[a][at].astype(F32)
        ).astype(kinds[a])

    def inward(k):
        @pl.when(end)
        def _():
            if half > 1:
                to_inner(k).start()

        @pl.when(jnp.logical_not(end))
        def _():
            to_inner(k).wait_recv()
            add(own, inwards, part, k)

            @pl.when(middle)
            def _():
                part_across(k).start()

            @pl.when(jnp.logical_not(middle))
            def _():
                part_to_inner(k).start()

    def outward(k):
        @pl.when(middle)
        def _():
            part_across(k).wait_recv()
            add(part, across, out, k)
            to_outer(k).start()

        @pl.when(jnp.logical_not(middle))
        def _():
            to_outer(k).wait_recv()

            @pl.when(jnp.logical_not(end))
            def _():
                to_outer(k).start()

    total = len(pieces)
    for k in range(total + 1):
        if k < total:
            inward(k)
        if k:
            outward(k - 1)
    for k in range(total):
        part_across(k).wait_send()

        @pl.when(jnp.logical_not(end))
        def _():
            to_outer(k).wait_send()


def line_sum(arrays, splits):
    pieces = []
    for a, (array, split) in enumerate(zip(arrays, splits)):
        rows = array.shape[0] // split
        pieces += [(a, i * rows, rows) for i in range(split)]
    kinds = [array.dtype for array in arrays]
    vmem = pl.BlockSpec(memory_space=pltpu.VMEM)
    scratch = [pltpu.VMEM(array.shape, array.dtype) for array in arrays]
    sems = [pltpu.SemaphoreType.DMA((len(pieces),)) for _ in range(5)]
    return pl.pallas_call(
        functools.partial(line_kernel, pieces, kinds),
        out_shape=[jax.ShapeDtypeStruct(array.shape, array.dtype) for array in arrays],
        in_specs=[vmem] * len(arrays),
        out_specs=[vmem] * len(arrays),
        scratch_shapes=scratch * 3 + sems,
        compiler_params=pltpu.CompilerParams(
            collective_id=1, has_side_effects=True, vmem_limit_bytes=60 << 20
        ),
        name="line_sum",
    )(*arrays)


def rotary_tables(positions, head_size):
    half = head_size // 8
    lane = jnp.arange(2 * head_size) % head_size
    freq = jnp.exp((lane % half).astype(F32) * (-math.log(10000.0) / half))
    theta = positions.reshape(-1).astype(jnp.float32)[:, None] * freq
    first, second = lane < half, (lane >= half) & (lane < 2 * half)
    sine = jnp.sin(theta)
    return [
        jnp.where(first | second, jnp.cos(theta), 1.0),
        jnp.where(first, -sine, 0.0),
        jnp.where(second, sine, 0.0),
    ]


def scores_of(queries, keys, allowed):
    scores = lax.dot_general(
        queries, keys, (((1,), (1,)), ((), ())), preferred_element_type=F32
    ) * (1.0 / math.sqrt(HD))
    return jnp.where(allowed, scores, MASKED)


def allowed_of(seg_q, order_q, seg_k, order_k):
    return (seg_q[...] == seg_k[0]) & (order_k[0] <= order_q[...])


def attend_kernel(
    q_in, k_in, v_in, q_bias, k_bias, v_bias, same, above, below, seg_q, order_q, seg_k, order_k,
    q_out, k_out, v_out, attended_out, total_out,
):
    step = HD // 8
    wide = q_in.shape[1]

    def rotate(values):
        return (
            values * same[...]
            + pltpu.roll(values, wide - step, 1) * above[...]
            + pltpu.roll(values, step, 1) * below[...]
        )

    queries = rotate(q_in[...] + q_bias[...]).astype(BF16)
    keys = rotate(k_in[...] + k_bias[...]).astype(BF16)
    values = (v_in[...] + v_bias[...]).astype(BF16)
    q_out[...] = queries
    k_out[...] = keys
    v_out[...] = values
    allowed = allowed_of(seg_q, order_q, seg_k, order_k)
    results, totals = [], []
    for h in range(wide // HD):
        at = slice(h * HD, (h + 1) * HD)
        scores = scores_of(queries[:, at], keys[:, at], allowed)
        peak = jnp.max(scores, -1, keepdims=True)
        raised = jnp.exp(scores - peak)
        denominator = jnp.sum(raised, -1, keepdims=True)
        probs = (raised / denominator).astype(BF16)
        results.append(jnp.dot(probs, values[:, at], preferred_element_type=F32))
        totals.append(peak + jnp.log(denominator))
    attended_out[...] = jnp.concatenate(results, 1).astype(BF16)
    total_out[0] = jnp.concatenate(totals, 1)


def attend_back_kernel(
    q_in, k_in, v_in, attended_in, grad_in, total_in, same, above, below,
    seg_q, order_q, seg_k, order_k, q_out, k_out, v_out,
):
    step = HD // 8
    wide = q_in.shape[1]

    def rotate_back(grads):
        return (
            grads * same[...]
            + pltpu.roll(grads * above[...], step, 1)
            + pltpu.roll(grads * below[...], wide - step, 1)
        )

    allowed = allowed_of(seg_q, order_q, seg_k, order_k)
    products = grad_in[...].astype(F32) * attended_in[...].astype(F32)
    q_grads, k_grads, v_grads = [], [], []
    for h in range(wide // HD):
        at = slice(h * HD, (h + 1) * HD)
        queries, keys, values = q_in[:, at], k_in[:, at], v_in[:, at]
        grad = grad_in[:, at]
        recovered = jnp.exp(scores_of(queries, keys, allowed) - total_in[0][:, h : h + 1])
        prob_grad = lax.dot_general(
            grad, values, (((1,), (1,)), ((), ())), preferred_element_type=F32
        )
        row_dot = jnp.sum(products[:, at], 1, keepdims=True)
        score_grad = (recovered * (prob_grad - row_dot) * (1.0 / math.sqrt(HD))).astype(BF16)
        q_grads.append(jnp.dot(score_grad, keys, preferred_element_type=F32))
        k_grads.append(t_dot(score_grad, queries))
        v_grads.append(t_dot(recovered.astype(BF16), grad))
    q_out[...] = rotate_back(jnp.concatenate(q_grads, 1)).astype(BF16)
    k_out[...] = rotate_back(jnp.concatenate(k_grads, 1)).astype(BF16)
    v_out[...] = jnp.concatenate(v_grads, 1).astype(BF16)


def attention_specs(tables, seq_len, wide):
    block = pl.BlockSpec((seq_len, wide), lambda s, p: (s, p))
    table = pl.BlockSpec((seq_len, wide), lambda s, p: (s, 0))
    tall = pl.BlockSpec((seq_len, 1), lambda s, p: (s, 0))
    flat = pl.BlockSpec((1, 1, seq_len), lambda s, p: (s, 0, 0))
    total = pl.BlockSpec((1, seq_len, wide // HD), lambda s, p: (p, s, 0))
    return block, [table] * 3 + [tall] * 2 + [flat] * 2, total


def attend(projected, bias, tables, seq_here, seq_len):
    tokens, piece = projected.shape[0], projected.shape[1] // 3
    wide = 2 * HD
    pairs = piece // wide
    block, extra, total = attention_specs(tables, seq_len, wide)
    shifted = [
        pl.BlockSpec((seq_len, wide), functools.partial(lambda k, s, p: (s, p + k * pairs), k))
        for k in range(3)
    ]
    biases = [
        pl.BlockSpec((1, wide), functools.partial(lambda k, s, p: (0, p + k * pairs), k))
        for k in range(3)
    ]
    whole = jax.ShapeDtypeStruct((tokens, piece), BF16)
    return pl.pallas_call(
        attend_kernel,
        grid=(seq_here, pairs),
        in_specs=shifted + biases + extra,
        out_specs=[block] * 4 + [total],
        out_shape=[whole] * 4 + [jax.ShapeDtypeStruct((pairs, tokens, wide // HD), F32)],
        cost_estimate=pl.CostEstimate(
            flops=4 * tokens * seq_len * piece, bytes_accessed=20 * tokens * piece,
            transcendentals=tokens * seq_len * piece // HD,
        ),
        name="attend",
    )(projected, projected, projected, bias, bias, bias, *tables)


def attend_back(queries, keys, values, attended, grad, total_log, tables, seq_here, seq_len):
    tokens, piece = queries.shape
    wide = 2 * HD
    pairs = piece // wide
    block, extra, total = attention_specs(tables, seq_len, wide)
    whole = jax.ShapeDtypeStruct((tokens, piece), BF16)
    return pl.pallas_call(
        attend_back_kernel,
        grid=(seq_here, pairs),
        in_specs=[block] * 5 + [total] + extra,
        out_specs=[block] * 3,
        out_shape=[whole] * 3,
        cost_estimate=pl.CostEstimate(
            flops=10 * tokens * seq_len * piece, bytes_accessed=20 * tokens * piece,
            transcendentals=tokens * seq_len * piece // HD,
        ),
        name="attend_back",
    )(queries, keys, values, attended, grad, total_log, *tables)


def local(
    block_input,
    segment_ids,
    positions,
    attention_gain,
    attention_shift,
    projection_weight,
    projection_bias,
    mixing_weight,
    feedforward_gain,
    feedforward_shift,
    gating_weight,
    lowering_weight,
    cotangent,
):
    own_tokens, local_width = block_input.shape
    seq_here, seq_len = segment_ids.shape
    tokens = seq_here * seq_len
    row = lax.axis_index("row")
    col = lax.axis_index("col")
    cols = lax.axis_size("col")
    tie = lax.optimization_barrier

    def mine(values, axis):
        size = values.shape[axis] // 2
        return lax.dynamic_slice_in_dim(values, row * size, size, axis)

    def theirs(values, axis):
        size = values.shape[axis] // 2
        return lax.dynamic_slice_in_dim(values, (1 - row) * size, size, axis)

    def both(values, axis):
        other = row_swap(values)
        return jnp.concatenate(
            [jnp.where(row == 0, values, other), jnp.where(row == 0, other, values)], axis
        )

    def reorder(table):
        blocks = table.reshape(cols, own_tokens)
        return jnp.take(blocks, col ^ jnp.arange(cols), axis=0).reshape(-1)

    order = reorder(jnp.tile(jnp.arange(seq_len), seq_here))
    segments = reorder(segment_ids)
    tables = rotary_tables(reorder(positions), HD) + [
        segments[:, None],
        order[:, None],
        segments.reshape(seq_here, 1, seq_len),
        order.reshape(seq_here, 1, seq_len),
    ]

    residual = block_input.astype(jnp.float32)
    scaled_one, inverse_one = normalize(residual)
    normed_one = (scaled_one * attention_gain + attention_shift).astype(jnp.bfloat16)
    normed_full = gather_tokens(normed_one)
    weights_mine = mine(projection_weight, 2).reshape(local_width, -1)
    weights_theirs = theirs(projection_weight, 2).reshape(local_width, -1)
    gating_pair = jnp.swapaxes(gating_weight, 0, 1)
    bias = mine(projection_bias, 1).reshape(1, -1)
    normed_full, weights_mine, weights_theirs, gating_pair, tables, bias, cotangent = tie(
        (normed_full, weights_mine, weights_theirs, gating_pair, tables, bias, cotangent)
    )
    gate_weight, up_weight = gating_pair[0], gating_pair[1]
    sent = row_swap(dot(normed_full, weights_theirs))
    projected = dot(normed_full, weights_mine) + sent
    queries, keys, values, attended, total_log = attend(
        projected, bias, tables, seq_here, seq_len
    )
    attended_full = both(attended, 1)
    upstream_full = gather_tokens(cotangent)
    attended_full, upstream_full = tie((attended_full, upstream_full))
    mixed = sum_tokens(dot(attended_full, mixing_weight))
    hidden_sent = row_swap(dot_t(theirs(upstream_full, 0), lowering_weight, BF16))
    hidden_grad = dot_t(mine(upstream_full, 0), lowering_weight) + hidden_sent.astype(F32)
    mixed, hidden_grad = tie((mixed, hidden_grad))
    middle = residual + mixed
    scaled_two, inverse_two = normalize(middle)
    normed_two = (scaled_two * feedforward_gain + feedforward_shift).astype(jnp.bfloat16)
    normed_two_full = gather_tokens(normed_two)

    outward = theirs(normed_two_full, 0)
    inward = mine(normed_two_full, 0)
    gate_sent = row_swap(dot(outward, gate_weight, BF16))
    up_sent = row_swap(dot(outward, up_weight, BF16))
    gate_value = dot(inward, gate_weight) + gate_sent.astype(F32)
    up_value = dot(inward, up_weight) + up_sent.astype(F32)
    sigmoid_gate = jax.nn.sigmoid(gate_value)
    hidden = (gate_value * sigmoid_gate * up_value).astype(jnp.bfloat16)
    gate_grad = hidden_grad * up_value * sigmoid_gate * (1.0 + gate_value * (1.0 - sigmoid_gate))
    up_grad = hidden_grad * gate_value * sigmoid_gate
    gate_back = both(gate_grad.astype(BF16), 0)
    up_back = both(up_grad.astype(BF16), 0)
    early = local_width * 3 // 4
    gate_wgrad = t_dot(normed_two_full, gate_back, BF16)
    up_wgrad = t_dot(normed_two_full, up_back, BF16)
    gate_back, up_back, gate_wgrad, up_wgrad = tie((gate_back, up_back, gate_wgrad, up_wgrad))
    gating_early = lax.psum((gate_wgrad[:early], up_wgrad[:early]), "dp")
    hidden_full = both(hidden, 0)

    normed_two_grad = sum_tokens(dot_t(gate_back, gate_weight) + dot_t(up_back, up_weight))
    middle_grad = cotangent.astype(jnp.float32) + norm_back(
        normed_two_grad, feedforward_gain, scaled_two, inverse_two
    )
    middle_wire = middle_grad.astype(jnp.bfloat16)
    middle_full = gather_tokens(middle_wire)
    attended_sent = row_swap(dot_t(middle_full, theirs(mixing_weight, 0), BF16))
    attended_grad = dot_t(middle_full, mine(mixing_weight, 0)) + attended_sent.astype(F32)
    grads = attend_back(
        queries, keys, values, attended, attended_grad.astype(BF16), total_log, tables,
        seq_here, seq_len,
    )
    backs = [both(grad, 1) for grad in grads]
    projection_bgrad = jnp.concatenate([jnp.sum(back, 0, dtype=F32) for back in backs])
    normed_one_grad = sum_tokens(
        sum(dot_t(back, projection_weight[:, i]) for i, back in enumerate(backs))
    )
    input_grad = (
        middle_grad + norm_back(normed_one_grad, attention_gain, scaled_one, inverse_one)
    ).astype(jnp.bfloat16)
    block_output = (middle + sum_tokens(dot(hidden_full, lowering_weight))).astype(jnp.bfloat16)

    sums = jnp.concatenate(
        [
            jnp.sum(normed_one_grad * scaled_one, 0),
            jnp.sum(normed_one_grad, 0),
            jnp.sum(normed_two_grad * scaled_two, 0),
            jnp.sum(normed_two_grad, 0),
        ]
    )
    bit = 1
    while bit < cols:
        sums = sums + col_swap(sums, bit)
        bit *= 2
    small = jnp.concatenate([sums, projection_bgrad])
    lanes = 128
    unit = 8 * lanes
    small = jnp.pad(small, (0, -small.shape[0] % unit)).reshape(-1, lanes)

    totals = line_sum(
        [
            t_dot(hidden_full, upstream_full, BF16),
            t_dot(attended_full, middle_full, BF16),
            *(t_dot(normed_full, back, BF16) for back in backs),
            gate_wgrad[early:],
            up_wgrad[early:],
            small,
        ],
        [4, 2, 2, 2, 2, 1, 1, 1],
    )
    lowering_wgrad, mixing_wgrad = totals[0], totals[1]
    sums = totals[7].reshape(-1)
    projection_bgrad = sums[4 * local_width : 4 * local_width + projection_bgrad.shape[0]]
    return (
        block_output,
        input_grad,
        sums[:local_width],
        sums[local_width : 2 * local_width],
        jnp.stack(totals[2:5], 1).astype(F32),
        projection_bgrad.reshape(3, -1),
        mixing_wgrad.astype(F32),
        sums[2 * local_width : 3 * local_width],
        sums[3 * local_width : 4 * local_width],
        jnp.stack(
            [jnp.concatenate([gating_early[k], totals[5 + k]]) for k in range(2)], 1
        ).astype(F32),
        lowering_wgrad.astype(F32),
    )


def solution(mesh):
    return jax.shard_map(
        local,
        mesh=mesh,
        in_specs=(
            P(("dp", "col"), "row"),
            P("dp", None),
            P("dp", None),
            P("row"),
            P("row"),
            P("row", None, "col"),
            P(None, "col"),
            P("col", "row"),
            P("row"),
            P("row"),
            P("row", None, "col"),
            P("col", "row"),
            P(("dp", "col"), "row"),
        ),
        out_specs=(
            P(("dp", "col"), "row"),
            P(("dp", "col"), "row"),
            P("row"),
            P("row"),
            P("row", None, "col"),
            P(None, "col"),
            P("col", "row"),
            P("row"),
            P("row"),
            P("row", None, "col"),
            P("col", "row"),
        ),
        check_vma=False,
    )
```

```python
import functools
import math

import jax
import jax.numpy as jnp
from jax import lax
from jax.experimental import pallas as pl
from jax.experimental.pallas import tpu as pltpu
from jax.sharding import PartitionSpec as P

D = 2048
HD = 64


EPSILON = 1e-05
MASKED = -1e30
WINDOW = 2
LANES = 128
BF16 = jnp.bfloat16
F32 = jnp.float32


def col_swap(values, bit):
    count = lax.axis_size("col")
    return lax.ppermute(values, "col", [(i, i ^ bit) for i in range(count)])


def row_swap(values):
    return lax.ppermute(values, "row", [(0, 1), (1, 0)])


def gather_tokens(values):
    count = lax.axis_size("col")
    if count == 4:
        half = values.shape[0] // 2
        first = col_swap(values, 1)
        second = col_swap(values, 2)
        third_a = col_swap(second[:half], 1)
        third_b = col_swap(first[half:], 2)
        return jnp.concatenate([values, first, second, third_a, third_b], 0)
    bit = 1
    while bit < count:
        values = jnp.concatenate([values, col_swap(values, bit)], 0)
        bit *= 2
    return values


def sum_tokens(partial_rows):
    count = lax.axis_size("col")
    size = partial_rows.shape[0] // count
    if count == 4:
        half = size // 2
        own, first, second, third = (partial_rows[i * size : (i + 1) * size] for i in range(4))
        third = third.astype(BF16)
        got_a = col_swap(third[:half], 1).astype(F32)
        got_b = col_swap(third[half:], 2).astype(F32)
        to_second = jnp.concatenate([second[:half] + got_a, second[half:]], 0).astype(BF16)
        to_first = jnp.concatenate([first[:half], first[half:] + got_b], 0).astype(BF16)
        return own + col_swap(to_first, 1).astype(F32) + col_swap(to_second, 2).astype(F32)
    bit = count // 2
    while bit:
        kept = partial_rows.shape[0] // 2
        got = col_swap(partial_rows[kept:].astype(BF16), bit).astype(F32)
        partial_rows = partial_rows[:kept] + got
        bit //= 2
    return partial_rows


def row_sums(first, second):
    return lax.psum((first, second), "row")


def normalize(values):
    total, squares = row_sums(
        jnp.sum(values, 1, keepdims=True), jnp.sum(values * values, 1, keepdims=True)
    )
    center = total / D
    spread = squares / D - center * center
    inverse = lax.rsqrt(spread + EPSILON)
    return ((values - center) * inverse, inverse)


def norm_back(upstream, gain, scaled, inverse):
    weighted = upstream * gain
    total, mixed = row_sums(
        jnp.sum(weighted, 1, keepdims=True), jnp.sum(weighted * scaled, 1, keepdims=True)
    )
    return inverse * (weighted - total / D - scaled * (mixed / D))


def dot(a, b, kind=F32):
    return jnp.dot(a, b, preferred_element_type=F32).astype(kind)


def dot_t(a, b, kind=F32):
    return lax.dot_general(a, b, (((1,), (1,)), ((), ())), preferred_element_type=F32).astype(kind)


def t_dot(a, b, kind=F32):
    return lax.dot_general(a, b, (((0,), (0,)), ((), ())), preferred_element_type=F32).astype(kind)


def line_kernel(pieces, kinds, *refs):
    count = len(kinds)
    own, out = refs[:count], refs[count : 2 * count]
    inwards, part, across = (refs[(2 + k) * count : (3 + k) * count] for k in range(3))
    sent_in, got_in, got_across, sent_out, got_out = refs[5 * count :]
    size = lax.axis_size("dp")
    me = lax.axis_index("dp")
    half = size // 2
    low = me < half
    inner = jnp.where(low, me + 1, me - 1)
    outer = jnp.where(low, jnp.maximum(me - 1, 0), jnp.minimum(me + 1, size - 1))
    end = (me == 0) | (me == size - 1)
    middle = (me == half - 1) | (me == half)

    barrier = pltpu.get_barrier_semaphore()
    pl.semaphore_signal(
        barrier, inc=1, device_id={"dp": inner}, device_id_type=pl.DeviceIdType.MESH
    )

    @pl.when(jnp.logical_not(end))
    def _():
        pl.semaphore_signal(
            barrier, inc=1, device_id={"dp": outer}, device_id_type=pl.DeviceIdType.MESH
        )
        pl.semaphore_wait(barrier, 2)

    @pl.when(end)
    def _():
        pl.semaphore_wait(barrier, 1)

    def copy(source, target, sent, got, to):
        return pltpu.make_async_remote_copy(
            src_ref=source,
            dst_ref=target,
            send_sem=sent,
            recv_sem=got,
            device_id={"dp": to},
            device_id_type=pl.DeviceIdType.MESH,
        )

    def to_inner(k):
        a, start, rows = pieces[k]
        at = pl.ds(start, rows)
        return copy(own[a].at[at], inwards[a].at[at], sent_in.at[k], got_in.at[k], inner)

    def part_to_inner(k):
        a, start, rows = pieces[k]
        at = pl.ds(start, rows)
        return copy(part[a].at[at], inwards[a].at[at], sent_in.at[k], got_in.at[k], inner)

    def part_across(k):
        a, start, rows = pieces[k]
        at = pl.ds(start, rows)
        return copy(part[a].at[at], across[a].at[at], sent_in.at[k], got_across.at[k], inner)

    def to_outer(k):
        a, start, rows = pieces[k]
        at = pl.ds(start, rows)
        return copy(out[a].at[at], out[a].at[at], sent_out.at[k], got_out.at[k], outer)

    def add(first, second, target, k):
        a, start, rows = pieces[k]
        at = pl.ds(start, rows)
        target[a][at] = (
            first[a][at].astype(F32) + second[a][at].astype(F32)
        ).astype(kinds[a])

    total = len(pieces)

    @pl.when(end)
    def _():
        for k in range(total):
            if k >= WINDOW:
                to_inner(k - WINDOW).wait_send()
            to_inner(k).start()
        for k in range(max(total - WINDOW, 0), total):
            to_inner(k).wait_send()
        for k in range(total):
            to_outer(k).wait_recv()

    def inward(k):
        to_inner(k).wait_recv()
        add(own, inwards, part, k)

        @pl.when(middle)
        def _():
            part_across(k).start()

        @pl.when(jnp.logical_not(middle))
        def _():
            part_to_inner(k).start()

    def outward(k):
        @pl.when(middle)
        def _():
            part_across(k).wait_recv()
            add(part, across, out, k)
            to_outer(k).start()

        @pl.when(jnp.logical_not(middle))
        def _():
            to_outer(k).wait_recv()
            to_outer(k).start()

    @pl.when(jnp.logical_not(end))
    def _():
        for k in range(total + 1):
            if k < total:
                inward(k)
            if k:
                outward(k - 1)
        for k in range(total):
            part_across(k).wait_send()
            to_outer(k).wait_send()


def line_sum(arrays, splits):
    pieces = []
    for a, (array, split) in enumerate(zip(arrays, splits)):
        rows = array.shape[0] // split
        pieces += [(a, i * rows, rows) for i in range(split)]
    kinds = [array.dtype for array in arrays]
    vmem = pl.BlockSpec(memory_space=pltpu.VMEM)
    scratch = [pltpu.VMEM(array.shape, array.dtype) for array in arrays]
    sems = [pltpu.SemaphoreType.DMA((len(pieces),)) for _ in range(5)]
    return pl.pallas_call(
        functools.partial(line_kernel, pieces, kinds),
        out_shape=[jax.ShapeDtypeStruct(array.shape, array.dtype) for array in arrays],
        in_specs=[vmem] * len(arrays),
        out_specs=[vmem] * len(arrays),
        scratch_shapes=scratch * 3 + sems,
        compiler_params=pltpu.CompilerParams(
            collective_id=1, has_side_effects=True, vmem_limit_bytes=60 << 20
        ),
        name="line_sum",
    )(*arrays)


def rotary_tables(positions, head_size):
    half = head_size // 8
    lane = jnp.arange(2 * head_size) % head_size
    freq = jnp.exp((lane % half).astype(F32) * (-math.log(10000.0) / half))
    theta = positions.reshape(-1).astype(jnp.float32)[:, None] * freq
    first, second = lane < half, (lane >= half) & (lane < 2 * half)
    sine = jnp.sin(theta)
    return [
        jnp.where(first | second, jnp.cos(theta), 1.0),
        jnp.where(first, -sine, 0.0),
        jnp.where(second, sine, 0.0),
    ]


def scores_of(queries, keys, allowed):
    scores = lax.dot_general(
        queries, keys, (((1,), (1,)), ((), ())), preferred_element_type=F32
    ) * (1.0 / math.sqrt(HD))
    return jnp.where(allowed, scores, MASKED)


def allowed_of(seg_q, order_q, seg_k, order_k):
    return (seg_q[...] == seg_k[0]) & (order_k[0] <= order_q[...])


def attend_kernel(
    q_in, k_in, v_in, q_bias, k_bias, v_bias, same, above, below, seg_q, order_q, seg_k, order_k,
    q_out, k_out, v_out, attended_out, total_out,
):
    step = HD // 8
    wide = q_in.shape[1]

    def rotate(values):
        return (
            values * same[...]
            + pltpu.roll(values, wide - step, 1) * above[...]
            + pltpu.roll(values, step, 1) * below[...]
        )

    queries = rotate(q_in[...] + q_bias[...]).astype(BF16)
    keys = rotate(k_in[...] + k_bias[...]).astype(BF16)
    values = (v_in[...] + v_bias[...]).astype(BF16)
    q_out[...] = queries
    k_out[...] = keys
    v_out[...] = values
    allowed = allowed_of(seg_q, order_q, seg_k, order_k)
    results, totals = [], []
    for h in range(wide // HD):
        at = slice(h * HD, (h + 1) * HD)
        scores = scores_of(queries[:, at], keys[:, at], allowed)
        peak = jnp.max(scores, -1, keepdims=True)
        raised = jnp.exp(scores - peak)
        denominator = jnp.sum(raised, -1, keepdims=True)
        probs = (raised / denominator).astype(BF16)
        results.append(jnp.dot(probs, values[:, at], preferred_element_type=F32))
        totals.append(peak + jnp.log(denominator))
    attended_out[...] = jnp.concatenate(results, 1).astype(BF16)
    total_out[0] = jnp.concatenate(totals, 1)


def attend_back_kernel(
    q_in, k_in, v_in, attended_in, grad_in, total_in, same, above, below,
    seg_q, order_q, seg_k, order_k, q_out, k_out, v_out,
):
    step = HD // 8
    wide = q_in.shape[1]

    def rotate_back(grads):
        return (
            grads * same[...]
            + pltpu.roll(grads * above[...], step, 1)
            + pltpu.roll(grads * below[...], wide - step, 1)
        )

    allowed = allowed_of(seg_q, order_q, seg_k, order_k)
    products = grad_in[...].astype(F32) * attended_in[...].astype(F32)
    q_grads, k_grads, v_grads = [], [], []
    for h in range(wide // HD):
        at = slice(h * HD, (h + 1) * HD)
        queries, keys, values = q_in[:, at], k_in[:, at], v_in[:, at]
        grad = grad_in[:, at]
        recovered = jnp.exp(scores_of(queries, keys, allowed) - total_in[0][:, h : h + 1])
        prob_grad = lax.dot_general(
            grad, values, (((1,), (1,)), ((), ())), preferred_element_type=F32
        )
        row_dot = jnp.sum(products[:, at], 1, keepdims=True)
        score_grad = (recovered * (prob_grad - row_dot) * (1.0 / math.sqrt(HD))).astype(BF16)
        q_grads.append(jnp.dot(score_grad, keys, preferred_element_type=F32))
        k_grads.append(t_dot(score_grad, queries))
        v_grads.append(t_dot(recovered.astype(BF16), grad))
    q_out[...] = rotate_back(jnp.concatenate(q_grads, 1)).astype(BF16)
    k_out[...] = rotate_back(jnp.concatenate(k_grads, 1)).astype(BF16)
    v_out[...] = jnp.concatenate(v_grads, 1).astype(BF16)


def attention_specs(tables, seq_len, wide):
    block = pl.BlockSpec((seq_len, wide), lambda s, p: (s, p))
    table = pl.BlockSpec((seq_len, wide), lambda s, p: (s, 0))
    tall = pl.BlockSpec((seq_len, 1), lambda s, p: (s, 0))
    flat = pl.BlockSpec((1, 1, seq_len), lambda s, p: (s, 0, 0))
    total = pl.BlockSpec((1, seq_len, wide // HD), lambda s, p: (p, s, 0))
    return block, [table] * 3 + [tall] * 2 + [flat] * 2, total


def attend(projected, bias, tables, seq_here, seq_len):
    tokens, piece = projected.shape[0], projected.shape[1] // 3
    wide = 2 * HD
    pairs = piece // wide
    block, extra, total = attention_specs(tables, seq_len, wide)
    shifted = [
        pl.BlockSpec((seq_len, wide), functools.partial(lambda k, s, p: (s, p + k * pairs), k))
        for k in range(3)
    ]
    biases = [
        pl.BlockSpec((1, wide), functools.partial(lambda k, s, p: (0, p + k * pairs), k))
        for k in range(3)
    ]
    whole = jax.ShapeDtypeStruct((tokens, piece), BF16)
    return pl.pallas_call(
        attend_kernel,
        grid=(seq_here, pairs),
        in_specs=shifted + biases + extra,
        out_specs=[block] * 4 + [total],
        out_shape=[whole] * 4 + [jax.ShapeDtypeStruct((pairs, tokens, wide // HD), F32)],
        cost_estimate=pl.CostEstimate(
            flops=4 * tokens * seq_len * piece, bytes_accessed=20 * tokens * piece,
            transcendentals=tokens * seq_len * piece // HD,
        ),
        name="attend",
    )(projected, projected, projected, bias, bias, bias, *tables)


def attend_back(queries, keys, values, attended, grad, total_log, tables, seq_here, seq_len):
    tokens, piece = queries.shape
    wide = 2 * HD
    pairs = piece // wide
    block, extra, total = attention_specs(tables, seq_len, wide)
    whole = jax.ShapeDtypeStruct((tokens, piece), BF16)
    return pl.pallas_call(
        attend_back_kernel,
        grid=(seq_here, pairs),
        in_specs=[block] * 5 + [total] + extra,
        out_specs=[block] * 3,
        out_shape=[whole] * 3,
        cost_estimate=pl.CostEstimate(
            flops=10 * tokens * seq_len * piece, bytes_accessed=20 * tokens * piece,
            transcendentals=tokens * seq_len * piece // HD,
        ),
        name="attend_back",
    )(queries, keys, values, attended, grad, total_log, *tables)


MESH = pl.DeviceIdType.MESH


def partners():
    col = lax.axis_index("col")
    cols = lax.axis_size("col")
    across = lax.rem(col + cols // 2, cols)
    return {"col": col + 1 - 2 * lax.rem(col, 2)}, {"col": across}, {"row": 1 - lax.axis_index("row")}


def meet(devices):
    barrier = pltpu.get_barrier_semaphore()
    for device in devices:
        pl.semaphore_signal(barrier, inc=1, device_id=device, device_id_type=MESH)
    pl.semaphore_wait(barrier, len(devices))


def remote(source, target, sems, k, device):
    return pltpu.make_async_remote_copy(
        src_ref=source,
        dst_ref=target,
        send_sem=sems.at[0, k],
        recv_sem=sems.at[1, k],
        device_id=device,
        device_id_type=MESH,
    )


def remote_sems(count):
    return pltpu.SemaphoreType.DMA((2, count))


def sum_scratch(size, width):
    half = size // 2
    return [
        pltpu.VMEM((3, size, width), BF16),
        pltpu.VMEM((2, half, width), BF16),
        pltpu.VMEM((2, size, width), BF16),
        pltpu.VMEM((2, half, width), F32),
        remote_sems(6),
    ]


def block_sum(part_of, filler, sent, passed, got, kept, sems):
    near, far, _ = partners()
    size = sent.shape[1]
    half = size // 2
    low, high = pl.ds(0, half), pl.ds(half, half)
    copies = [
        remote(sent.at[2, low], passed.at[0], sems, 0, near),
        remote(sent.at[2, high], passed.at[1], sems, 1, far),
        remote(sent.at[0, low], got.at[0, low], sems, 2, near),
        remote(sent.at[1, high], got.at[1, high], sems, 3, far),
        remote(sent.at[1, low], got.at[1, low], sems, 4, far),
        remote(sent.at[0, high], got.at[0, high], sems, 5, near),
    ]
    sent[2] = part_of(3).astype(BF16)
    copies[0].start()
    copies[1].start()
    part = part_of(1)
    sent[0, low] = part[:half].astype(BF16)
    copies[2].start()
    kept[0] = part[half:]
    part = part_of(2)
    sent[1, high] = part[half:].astype(BF16)
    copies[3].start()
    kept[1] = part[:half]
    copies[0].wait_recv()
    sent[1, low] = (kept[1] + passed[0].astype(F32)).astype(BF16)
    copies[4].start()
    copies[1].wait_recv()
    sent[0, high] = (kept[0] + passed[1].astype(F32)).astype(BF16)
    copies[5].start()
    own = part_of(0)
    filler()
    for copy in copies[2:]:
        copy.wait_recv()
    own = own + got[0].astype(F32) + got[1].astype(F32)
    for copy in copies:
        copy.wait_send()
    return own


def block_gather(blocks, use, sems):
    near, far, _ = partners()
    size = blocks.shape[0] // 4
    half = size // 2
    copies = [
        remote(blocks.at[pl.ds(0, size)], blocks.at[pl.ds(size, size)], sems, 0, near),
        remote(blocks.at[pl.ds(0, size)], blocks.at[pl.ds(2 * size, size)], sems, 1, far),
        remote(
            blocks.at[pl.ds(2 * size, half)], blocks.at[pl.ds(3 * size, half)], sems, 2, near
        ),
        remote(
            blocks.at[pl.ds(size + half, half)],
            blocks.at[pl.ds(3 * size + half, half)],
            sems,
            3,
            far,
        ),
    ]
    copies[0].start()
    copies[1].start()
    use(0)
    copies[1].wait_recv()
    copies[2].start()
    copies[0].wait_recv()
    copies[3].start()
    use(1)
    use(2)
    copies[2].wait_recv()
    copies[3].wait_recv()
    use(3)
    for copy in copies:
        copy.wait_send()


def pair_sums(first, second, stats, sems, k):
    _, _, other = partners()
    lane = lax.broadcasted_iota(jnp.int32, stats.shape[1:], 1)
    stats[0] = jnp.where(lane == 0, first, jnp.where(lane == 1, second, 0.0))
    copy = remote(stats.at[0], stats.at[1], sems, k, other)
    copy.start()
    copy.wait()
    both = stats[0] + stats[1]
    return both[:, 0:1], both[:, 1:2]


def scale_rows(values, stats, sems, k):
    total, squares = pair_sums(
        jnp.sum(values, 1, keepdims=True), jnp.sum(values * values, 1, keepdims=True), stats, sems, k
    )
    center = total / D
    inverse = lax.rsqrt(squares / D - center * center + EPSILON)
    return (values - center) * inverse, inverse


def project_kernel(
    x_in, gain, shift, weight, full_out, proj_out, scaled_out, inverse_out,
    loaded, sent, got, stats, load_sem, gather_sems, sems,
):
    near, far, other = partners()
    row = lax.axis_index("row")
    size = x_in.shape[0]
    kinds, _, width = weight.shape
    half = width // 2
    load = pltpu.make_async_copy(weight, loaded, load_sem)
    load.start()
    meet((near, far, other))
    scaled, inverse = scale_rows(x_in[...].astype(F32), stats, sems, 0)
    scaled_out[...] = scaled
    inverse_out[...] = jnp.broadcast_to(inverse, inverse_out.shape)
    full_out[pl.ds(0, size)] = (scaled * gain[...] + shift[...]).astype(BF16)
    mine = pl.ds(pl.multiple_of(row * half, half), half)
    theirs = pl.ds(pl.multiple_of((1 - row) * half, half), half)
    swaps = [
        remote(
            sent.at[pl.ds(b * size, size)], got.at[pl.ds(b * size, size)], sems, 1 + b, other
        )
        for b in range(4)
    ]

    def finish(b):
        at = pl.ds(b * size, size)
        swaps[b].wait_recv()
        proj_out[at] += got[at]

    def use(b):
        at = pl.ds(b * size, size)
        if b == 0:
            load.wait()
        values = full_out[at]
        for k in range(kinds):
            sent[at, k * half : (k + 1) * half] = dot(values, loaded[k, :, theirs])
        swaps[b].start()
        for k in range(kinds):
            proj_out[at, k * half : (k + 1) * half] = dot(values, loaded[k, :, mine])
        if b == 3:
            for done in range(4):
                finish(done)

    block_gather(full_out, use, gather_sems)
    for swap in swaps:
        swap.wait_send()


def project(x, gain, shift, weight):
    size, width = x.shape
    kinds, _, columns = weight.shape
    piece = kinds * columns // 2
    vmem = pl.BlockSpec(memory_space=pltpu.VMEM)
    return pl.pallas_call(
        project_kernel,
        in_specs=[vmem, vmem, vmem, pl.BlockSpec(memory_space=pl.ANY)],
        out_specs=[vmem] * 4,
        out_shape=[
            jax.ShapeDtypeStruct((4 * size, width), BF16),
            jax.ShapeDtypeStruct((4 * size, piece), F32),
            jax.ShapeDtypeStruct((size, width), F32),
            jax.ShapeDtypeStruct((size, LANES), F32),
        ],
        scratch_shapes=[
            pltpu.VMEM(weight.shape, BF16),
            pltpu.VMEM((4 * size, piece), F32),
            pltpu.VMEM((4 * size, piece), F32),
            pltpu.VMEM((2, size, LANES), F32),
            pltpu.SemaphoreType.DMA,
            remote_sems(4),
            remote_sems(5),
        ],
        compiler_params=pltpu.CompilerParams(
            collective_id=2, has_side_effects=True, vmem_limit_bytes=60 << 20
        ),
        name="project",
    )(x, gain, shift, weight)


def hidden_kernel(
    attended, mixing, x_in, gain, shift, gate_hbm, up_hbm, upstream_hbm, lowering_hbm,
    middle_out, scaled_out, inverse_out, full_out, hidden_out, gate_out, up_out,
    gate_w, up_w, upstream, lowering, attended_got, back_sent, back_got, back, stats,
    gates_sent, gates_got, gates_kept,
    s_sent, s_passed, s_got, s_kept, s_sems, load_sems, gather_sems, sems,
):
    near, far, other = partners()
    row = lax.axis_index("row")
    size = x_in.shape[0]
    part = size // 2
    depth = attended.shape[1]
    units = gate_w.shape[1]
    loads = [
        pltpu.make_async_copy(source, target, load_sems.at[k])
        for k, (source, target) in enumerate(
            ((upstream_hbm, upstream), (lowering_hbm, lowering), (gate_hbm, gate_w), (up_hbm, up_w))
        )
    ]
    for load in loads:
        load.start()
    meet((near, far, other))
    swap = remote(attended, attended_got, sems, 0, other)
    swap.start()

    def rows_of(b, whose):
        return pl.ds(pl.multiple_of(b * size + whose * part, part), part)

    loads[0].wait()
    loads[1].wait()
    for b in range(4):
        back_sent[pl.ds(b * part, part)] = dot_t(
            upstream[rows_of(b, 1 - row)], lowering[...], BF16
        )
    back_swap = remote(back_sent, back_got, sems, 1, other)
    back_swap.start()
    swap.wait_recv()
    mine = pl.ds(pl.multiple_of(row * depth, depth), depth)
    theirs = pl.ds(pl.multiple_of((1 - row) * depth, depth), depth)

    def part_of(b):
        at = pl.ds(b * size, size)
        return dot(attended[at], mixing[mine]) + dot(attended_got[at], mixing[theirs])

    def filler():
        back_swap.wait_recv()
        for b in range(4):
            at = pl.ds(b * part, part)
            back[at] = dot_t(upstream[rows_of(b, row)], lowering[...]) + back_got[at].astype(F32)
        loads[2].wait()
        loads[3].wait()

    middle = x_in[...].astype(F32) + block_sum(
        part_of, filler, s_sent, s_passed, s_got, s_kept, s_sems
    )
    middle_out[...] = middle
    scaled, inverse = scale_rows(middle, stats, sems, 2)
    scaled_out[...] = scaled
    inverse_out[...] = jnp.broadcast_to(inverse, inverse_out.shape)
    full_out[pl.ds(0, size)] = (scaled * gain[...] + shift[...]).astype(BF16)
    gate_swaps = [remote(gates_sent.at[b], gates_got.at[b], sems, 3 + b, other) for b in range(4)]

    def returns(b):
        at = rows_of(b, row)
        return [
            remote(ref.at[at], ref.at[at], sems, 7 + 3 * b + k, other)
            for k, ref in enumerate((gate_out, up_out, hidden_out))
        ]

    def finish(b):
        gate_swaps[b].wait_recv()
        gate = gates_kept[b % 2, :, :units] + gates_got[b, :, :units].astype(F32)
        up = gates_kept[b % 2, :, units:] + gates_got[b, :, units:].astype(F32)
        grad = back[pl.ds(b * part, part)]
        sigmoid = jax.nn.sigmoid(gate)
        at = rows_of(b, row)
        gate_out[at] = (grad * up * sigmoid * (1.0 + gate * (1.0 - sigmoid))).astype(BF16)
        up_out[at] = (grad * gate * sigmoid).astype(BF16)
        hidden_out[at] = (gate * sigmoid * up).astype(BF16)
        for copy in returns(b):
            copy.start()

    def use(b):
        values = full_out[rows_of(b, 1 - row)]
        gates_sent[b, :, :units] = dot(values, gate_w[...], BF16)
        gates_sent[b, :, units:] = dot(values, up_w[...], BF16)
        gate_swaps[b].start()
        values = full_out[rows_of(b, row)]
        gates_kept[b % 2, :, :units] = dot(values, gate_w[...])
        gates_kept[b % 2, :, units:] = dot(values, up_w[...])
        finish(b)

    block_gather(full_out, use, gather_sems)
    swap.wait_send()
    back_swap.wait_send()
    for b in range(4):
        gate_swaps[b].wait_send()
        at = rows_of(b, 1 - row)
        for copy in returns(b):
            copy.wait_send()
        for k, ref in enumerate((gate_out, up_out, hidden_out)):
            remote(ref.at[at], ref.at[at], sems, 7 + 3 * b + k, other).wait_recv()


def hidden_units(attended, mixing, x, gain, shift, gate_w, up_w, upstream, lowering):
    size, width = x.shape
    tokens = 4 * size
    units = gate_w.shape[1]
    part = size // 2
    vmem = pl.BlockSpec(memory_space=pltpu.VMEM)
    anywhere = pl.BlockSpec(memory_space=pl.ANY)
    return pl.pallas_call(
        hidden_kernel,
        in_specs=[vmem] * 5 + [anywhere] * 4,
        out_specs=[vmem] * 7,
        out_shape=[
            jax.ShapeDtypeStruct((size, width), F32),
            jax.ShapeDtypeStruct((size, width), F32),
            jax.ShapeDtypeStruct((size, LANES), F32),
            jax.ShapeDtypeStruct((tokens, width), BF16),
        ]
        + [jax.ShapeDtypeStruct((tokens, units), BF16)] * 3,
        scratch_shapes=[
            pltpu.VMEM(gate_w.shape, BF16),
            pltpu.VMEM(up_w.shape, BF16),
            pltpu.VMEM(upstream.shape, BF16),
            pltpu.VMEM(lowering.shape, BF16),
            pltpu.VMEM(attended.shape, BF16),
            pltpu.VMEM((tokens // 2, units), BF16),
            pltpu.VMEM((tokens // 2, units), BF16),
            pltpu.VMEM((tokens // 2, units), F32),
            pltpu.VMEM((2, size, LANES), F32),
            pltpu.VMEM((4, part, 2 * units), BF16),
            pltpu.VMEM((4, part, 2 * units), BF16),
            pltpu.VMEM((2, part, 2 * units), F32),
            *sum_scratch(size, width),
            pltpu.SemaphoreType.DMA((4,)),
            remote_sems(4),
            remote_sems(19),
        ],
        compiler_params=pltpu.CompilerParams(
            collective_id=3, has_side_effects=True, vmem_limit_bytes=61 << 20
        ),
        name="hidden_units",
    )(attended, mixing, x, gain, shift, gate_w, up_w, upstream, lowering)


def local(
    block_input,
    segment_ids,
    positions,
    attention_gain,
    attention_shift,
    projection_weight,
    projection_bias,
    mixing_weight,
    feedforward_gain,
    feedforward_shift,
    gating_weight,
    lowering_weight,
    cotangent,
):
    own_tokens, local_width = block_input.shape
    seq_here, seq_len = segment_ids.shape
    tokens = seq_here * seq_len
    row = lax.axis_index("row")
    col = lax.axis_index("col")
    cols = lax.axis_size("col")
    tie = lax.optimization_barrier

    def mine(values, axis):
        size = values.shape[axis] // 2
        return lax.dynamic_slice_in_dim(values, row * size, size, axis)

    def theirs(values, axis):
        size = values.shape[axis] // 2
        return lax.dynamic_slice_in_dim(values, (1 - row) * size, size, axis)

    def both(values, axis):
        other = row_swap(values)
        return jnp.concatenate(
            [jnp.where(row == 0, values, other), jnp.where(row == 0, other, values)], axis
        )

    def reorder(table):
        blocks = table.reshape(cols, own_tokens)
        return jnp.take(blocks, col ^ jnp.arange(cols), axis=0).reshape(-1)

    order = reorder(jnp.tile(jnp.arange(seq_len), seq_here))
    segments = reorder(segment_ids)
    tables = rotary_tables(reorder(positions), HD) + [
        segments[:, None],
        order[:, None],
        segments.reshape(seq_here, 1, seq_len),
        order.reshape(seq_here, 1, seq_len),
    ]

    gating_pair = jnp.swapaxes(gating_weight, 0, 1)
    bias = mine(projection_bias, 1).reshape(1, -1)
    normed_full, projected, scaled_one, inverse_one = project(
        block_input,
        attention_gain[None],
        attention_shift[None],
        jnp.swapaxes(projection_weight, 0, 1),
    )
    inverse_one = inverse_one[:, :1]
    normed_full, cotangent = tie((normed_full, cotangent))
    gate_weight, up_weight = gating_pair[0], gating_pair[1]
    queries, keys, values, attended, total_log = attend(
        projected, bias, tables, seq_here, seq_len
    )
    upstream_full = gather_tokens(cotangent)
    middle, scaled_two, inverse_two, normed_two_full, hidden_full, gate_back, up_back = (
        hidden_units(
            attended,
            mixing_weight,
            block_input,
            feedforward_gain[None],
            feedforward_shift[None],
            gate_weight,
            up_weight,
            upstream_full,
            lowering_weight,
        )
    )
    inverse_two = inverse_two[:, :1]
    attended_full = both(attended, 1)

    early = local_width * 3 // 4
    gate_wgrad = t_dot(normed_two_full, gate_back, BF16)
    up_wgrad = t_dot(normed_two_full, up_back, BF16)
    gate_back, up_back, gate_wgrad, up_wgrad = tie((gate_back, up_back, gate_wgrad, up_wgrad))
    gating_early = lax.psum((gate_wgrad[:early], up_wgrad[:early]), "dp")

    normed_two_grad = sum_tokens(dot_t(gate_back, gate_weight) + dot_t(up_back, up_weight))
    middle_grad = cotangent.astype(jnp.float32) + norm_back(
        normed_two_grad, feedforward_gain, scaled_two, inverse_two
    )
    middle_wire = middle_grad.astype(jnp.bfloat16)
    middle_full = gather_tokens(middle_wire)
    attended_sent = row_swap(dot_t(middle_full, theirs(mixing_weight, 0), BF16))
    attended_grad = dot_t(middle_full, mine(mixing_weight, 0)) + attended_sent.astype(F32)
    grads = attend_back(
        queries, keys, values, attended, attended_grad.astype(BF16), total_log, tables,
        seq_here, seq_len,
    )
    backs = [both(grad, 1) for grad in grads]
    projection_bgrad = jnp.concatenate([jnp.sum(back, 0, dtype=F32) for back in backs])
    normed_one_grad = sum_tokens(
        sum(dot_t(back, projection_weight[:, i]) for i, back in enumerate(backs))
    )
    input_grad = (
        middle_grad + norm_back(normed_one_grad, attention_gain, scaled_one, inverse_one)
    ).astype(jnp.bfloat16)
    block_output = (middle + sum_tokens(dot(hidden_full, lowering_weight))).astype(jnp.bfloat16)

    sums = jnp.concatenate(
        [
            jnp.sum(normed_one_grad * scaled_one, 0),
            jnp.sum(normed_one_grad, 0),
            jnp.sum(normed_two_grad * scaled_two, 0),
            jnp.sum(normed_two_grad, 0),
        ]
    )
    bit = 1
    while bit < cols:
        sums = sums + col_swap(sums, bit)
        bit *= 2
    small = jnp.concatenate([sums, projection_bgrad])
    lanes = 128
    unit = 8 * lanes
    small = jnp.pad(small, (0, -small.shape[0] % unit)).reshape(-1, lanes)

    totals = line_sum(
        [
            t_dot(hidden_full, upstream_full, BF16),
            t_dot(attended_full, middle_full, BF16),
            *(t_dot(normed_full, back, BF16) for back in backs),
            gate_wgrad[early:],
            up_wgrad[early:],
            small,
        ],
        [4, 2, 2, 2, 2, 1, 1, 1],
    )
    lowering_wgrad, mixing_wgrad = totals[0], totals[1]
    sums = totals[7].reshape(-1)
    projection_bgrad = sums[4 * local_width : 4 * local_width + projection_bgrad.shape[0]]
    return (
        block_output,
        input_grad,
        sums[:local_width],
        sums[local_width : 2 * local_width],
        jnp.stack(totals[2:5], 1).astype(F32),
        projection_bgrad.reshape(3, -1),
        mixing_wgrad.astype(F32),
        sums[2 * local_width : 3 * local_width],
        sums[3 * local_width : 4 * local_width],
        jnp.stack(
            [jnp.concatenate([gating_early[k], totals[5 + k]]) for k in range(2)], 1
        ).astype(F32),
        lowering_wgrad.astype(F32),
    )


def solution(mesh):
    return jax.shard_map(
        local,
        mesh=mesh,
        in_specs=(
            P(("dp", "col"), "row"),
            P("dp", None),
            P("dp", None),
            P("row"),
            P("row"),
            P("row", None, "col"),
            P(None, "col"),
            P("col", "row"),
            P("row"),
            P("row"),
            P("row", None, "col"),
            P("col", "row"),
            P(("dp", "col"), "row"),
        ),
        out_specs=(
            P(("dp", "col"), "row"),
            P(("dp", "col"), "row"),
            P("row"),
            P("row"),
            P("row", None, "col"),
            P(None, "col"),
            P("col", "row"),
            P("row"),
            P("row"),
            P("row", None, "col"),
            P("col", "row"),
        ),
        check_vma=False,
    )
```

```python
import functools
import math

import jax
import jax.numpy as jnp
from jax import lax
from jax.experimental import pallas as pl
from jax.experimental.pallas import tpu as pltpu
from jax.sharding import PartitionSpec as P

D = 2048
HD = 64


EPSILON = 1e-05
MASKED = -1e30
WINDOW = 2
LANES = 128
BF16 = jnp.bfloat16
F32 = jnp.float32


def col_swap(values, bit):
    count = lax.axis_size("col")
    return lax.ppermute(values, "col", [(i, i ^ bit) for i in range(count)])


def row_swap(values):
    return lax.ppermute(values, "row", [(0, 1), (1, 0)])


def gather_tokens(values):
    count = lax.axis_size("col")
    if count == 4:
        half = values.shape[0] // 2
        first = col_swap(values, 1)
        second = col_swap(values, 2)
        third_a = col_swap(second[:half], 1)
        third_b = col_swap(first[half:], 2)
        return jnp.concatenate([values, first, second, third_a, third_b], 0)
    bit = 1
    while bit < count:
        values = jnp.concatenate([values, col_swap(values, bit)], 0)
        bit *= 2
    return values


def sum_tokens(partial_rows):
    count = lax.axis_size("col")
    size = partial_rows.shape[0] // count
    if count == 4:
        half = size // 2
        own, first, second, third = (partial_rows[i * size : (i + 1) * size] for i in range(4))
        third = third.astype(BF16)
        got_a = col_swap(third[:half], 1).astype(F32)
        got_b = col_swap(third[half:], 2).astype(F32)
        to_second = jnp.concatenate([second[:half] + got_a, second[half:]], 0).astype(BF16)
        to_first = jnp.concatenate([first[:half], first[half:] + got_b], 0).astype(BF16)
        return own + col_swap(to_first, 1).astype(F32) + col_swap(to_second, 2).astype(F32)
    bit = count // 2
    while bit:
        kept = partial_rows.shape[0] // 2
        got = col_swap(partial_rows[kept:].astype(BF16), bit).astype(F32)
        partial_rows = partial_rows[:kept] + got
        bit //= 2
    return partial_rows


def row_sums(first, second):
    return lax.psum((first, second), "row")


def normalize(values):
    total, squares = row_sums(
        jnp.sum(values, 1, keepdims=True), jnp.sum(values * values, 1, keepdims=True)
    )
    center = total / D
    spread = squares / D - center * center
    inverse = lax.rsqrt(spread + EPSILON)
    return ((values - center) * inverse, inverse)


def norm_back(upstream, gain, scaled, inverse):
    weighted = upstream * gain
    total, mixed = row_sums(
        jnp.sum(weighted, 1, keepdims=True), jnp.sum(weighted * scaled, 1, keepdims=True)
    )
    return inverse * (weighted - total / D - scaled * (mixed / D))


def dot(a, b, kind=F32):
    return jnp.dot(a, b, preferred_element_type=F32).astype(kind)


def dot_t(a, b, kind=F32):
    return lax.dot_general(a, b, (((1,), (1,)), ((), ())), preferred_element_type=F32).astype(kind)


def t_dot(a, b, kind=F32):
    return lax.dot_general(a, b, (((0,), (0,)), ((), ())), preferred_element_type=F32).astype(kind)


def line_kernel(pieces, kinds, *refs):
    count = len(kinds)
    own, out = refs[:count], refs[count : 2 * count]
    inwards, part, across = (refs[(2 + k) * count : (3 + k) * count] for k in range(3))
    sent_in, got_in, got_across, sent_out, got_out = refs[5 * count :]
    size = lax.axis_size("dp")
    me = lax.axis_index("dp")
    half = size // 2
    low = me < half
    inner = jnp.where(low, me + 1, me - 1)
    outer = jnp.where(low, jnp.maximum(me - 1, 0), jnp.minimum(me + 1, size - 1))
    end = (me == 0) | (me == size - 1)
    middle = (me == half - 1) | (me == half)

    barrier = pltpu.get_barrier_semaphore()
    pl.semaphore_signal(
        barrier, inc=1, device_id={"dp": inner}, device_id_type=pl.DeviceIdType.MESH
    )

    @pl.when(jnp.logical_not(end))
    def _():
        pl.semaphore_signal(
            barrier, inc=1, device_id={"dp": outer}, device_id_type=pl.DeviceIdType.MESH
        )
        pl.semaphore_wait(barrier, 2)

    @pl.when(end)
    def _():
        pl.semaphore_wait(barrier, 1)

    def copy(source, target, sent, got, to):
        return pltpu.make_async_remote_copy(
            src_ref=source,
            dst_ref=target,
            send_sem=sent,
            recv_sem=got,
            device_id={"dp": to},
            device_id_type=pl.DeviceIdType.MESH,
        )

    def to_inner(k):
        a, start, rows = pieces[k]
        at = pl.ds(start, rows)
        return copy(own[a].at[at], inwards[a].at[at], sent_in.at[k], got_in.at[k], inner)

    def part_to_inner(k):
        a, start, rows = pieces[k]
        at = pl.ds(start, rows)
        return copy(part[a].at[at], inwards[a].at[at], sent_in.at[k], got_in.at[k], inner)

    def part_across(k):
        a, start, rows = pieces[k]
        at = pl.ds(start, rows)
        return copy(part[a].at[at], across[a].at[at], sent_in.at[k], got_across.at[k], inner)

    def to_outer(k):
        a, start, rows = pieces[k]
        at = pl.ds(start, rows)
        return copy(out[a].at[at], out[a].at[at], sent_out.at[k], got_out.at[k], outer)

    def add(first, second, target, k):
        a, start, rows = pieces[k]
        at = pl.ds(start, rows)
        target[a][at] = (
            first[a][at].astype(F32) + second[a][at].astype(F32)
        ).astype(kinds[a])

    total = len(pieces)

    @pl.when(end)
    def _():
        for k in range(total):
            if k >= WINDOW:
                to_inner(k - WINDOW).wait_send()
            to_inner(k).start()
        for k in range(max(total - WINDOW, 0), total):
            to_inner(k).wait_send()
        for k in range(total):
            to_outer(k).wait_recv()

    def inward(k):
        to_inner(k).wait_recv()
        add(own, inwards, part, k)

        @pl.when(middle)
        def _():
            part_across(k).start()

        @pl.when(jnp.logical_not(middle))
        def _():
            part_to_inner(k).start()

    def outward(k):
        @pl.when(middle)
        def _():
            part_across(k).wait_recv()
            add(part, across, out, k)
            to_outer(k).start()

        @pl.when(jnp.logical_not(middle))
        def _():
            to_outer(k).wait_recv()
            to_outer(k).start()

    @pl.when(jnp.logical_not(end))
    def _():
        for k in range(total + 1):
            if k < total:
                inward(k)
            if k:
                outward(k - 1)
        for k in range(total):
            part_across(k).wait_send()
            to_outer(k).wait_send()


def line_sum(arrays, splits):
    pieces = []
    for a, (array, split) in enumerate(zip(arrays, splits)):
        rows = array.shape[0] // split
        pieces += [(a, i * rows, rows) for i in range(split)]
    kinds = [array.dtype for array in arrays]
    vmem = pl.BlockSpec(memory_space=pltpu.VMEM)
    scratch = [pltpu.VMEM(array.shape, array.dtype) for array in arrays]
    sems = [pltpu.SemaphoreType.DMA((len(pieces),)) for _ in range(5)]
    return pl.pallas_call(
        functools.partial(line_kernel, pieces, kinds),
        out_shape=[jax.ShapeDtypeStruct(array.shape, array.dtype) for array in arrays],
        in_specs=[vmem] * len(arrays),
        out_specs=[vmem] * len(arrays),
        scratch_shapes=scratch * 3 + sems,
        compiler_params=pltpu.CompilerParams(
            collective_id=1, has_side_effects=True, vmem_limit_bytes=60 << 20
        ),
        name="line_sum",
    )(*arrays)


def rotary_tables(positions, head_size):
    half = head_size // 8
    lane = jnp.arange(2 * head_size) % head_size
    freq = jnp.exp((lane % half).astype(F32) * (-math.log(10000.0) / half))
    theta = positions.reshape(-1).astype(jnp.float32)[:, None] * freq
    first, second = lane < half, (lane >= half) & (lane < 2 * half)
    sine = jnp.sin(theta)
    return [
        jnp.where(first | second, jnp.cos(theta), 1.0),
        jnp.where(first, -sine, 0.0),
        jnp.where(second, sine, 0.0),
    ]


def scores_of(queries, keys, allowed):
    scores = lax.dot_general(
        queries, keys, (((1,), (1,)), ((), ())), preferred_element_type=F32
    ) * (1.0 / math.sqrt(HD))
    return jnp.where(allowed, scores, MASKED)


def allowed_of(seg_q, order_q, seg_k, order_k):
    return (seg_q[...] == seg_k[0]) & (order_k[0] <= order_q[...])


def attend_kernel(
    q_in, k_in, v_in, q_bias, k_bias, v_bias, same, above, below, seg_q, order_q, seg_k, order_k,
    q_out, k_out, v_out, attended_out, total_out,
):
    step = HD // 8
    wide = q_in.shape[1]

    def rotate(values):
        return (
            values * same[...]
            + pltpu.roll(values, wide - step, 1) * above[...]
            + pltpu.roll(values, step, 1) * below[...]
        )

    queries = rotate(q_in[...] + q_bias[...]).astype(BF16)
    keys = rotate(k_in[...] + k_bias[...]).astype(BF16)
    values = (v_in[...] + v_bias[...]).astype(BF16)
    q_out[...] = queries
    k_out[...] = keys
    v_out[...] = values
    allowed = allowed_of(seg_q, order_q, seg_k, order_k)
    results, totals = [], []
    for h in range(wide // HD):
        at = slice(h * HD, (h + 1) * HD)
        scores = scores_of(queries[:, at], keys[:, at], allowed)
        peak = jnp.max(scores, -1, keepdims=True)
        raised = jnp.exp(scores - peak)
        denominator = jnp.sum(raised, -1, keepdims=True)
        probs = (raised / denominator).astype(BF16)
        results.append(jnp.dot(probs, values[:, at], preferred_element_type=F32))
        totals.append(peak + jnp.log(denominator))
    attended_out[...] = jnp.concatenate(results, 1).astype(BF16)
    total_out[0] = jnp.concatenate(totals, 1)


def attend_back_kernel(
    q_in, k_in, v_in, attended_in, grad_in, total_in, same, above, below,
    seg_q, order_q, seg_k, order_k, q_out, k_out, v_out,
):
    step = HD // 8
    wide = q_in.shape[1]

    def rotate_back(grads):
        return (
            grads * same[...]
            + pltpu.roll(grads * above[...], step, 1)
            + pltpu.roll(grads * below[...], wide - step, 1)
        )

    allowed = allowed_of(seg_q, order_q, seg_k, order_k)
    products = grad_in[...].astype(F32) * attended_in[...].astype(F32)
    q_grads, k_grads, v_grads = [], [], []
    for h in range(wide // HD):
        at = slice(h * HD, (h + 1) * HD)
        queries, keys, values = q_in[:, at], k_in[:, at], v_in[:, at]
        grad = grad_in[:, at]
        recovered = jnp.exp(scores_of(queries, keys, allowed) - total_in[0][:, h : h + 1])
        prob_grad = lax.dot_general(
            grad, values, (((1,), (1,)), ((), ())), preferred_element_type=F32
        )
        row_dot = jnp.sum(products[:, at], 1, keepdims=True)
        score_grad = (recovered * (prob_grad - row_dot) * (1.0 / math.sqrt(HD))).astype(BF16)
        q_grads.append(jnp.dot(score_grad, keys, preferred_element_type=F32))
        k_grads.append(t_dot(score_grad, queries))
        v_grads.append(t_dot(recovered.astype(BF16), grad))
    q_out[...] = rotate_back(jnp.concatenate(q_grads, 1)).astype(BF16)
    k_out[...] = rotate_back(jnp.concatenate(k_grads, 1)).astype(BF16)
    v_out[...] = jnp.concatenate(v_grads, 1).astype(BF16)


def attention_specs(tables, seq_len, wide):
    block = pl.BlockSpec((seq_len, wide), lambda s, p: (s, p))
    table = pl.BlockSpec((seq_len, wide), lambda s, p: (s, 0))
    tall = pl.BlockSpec((seq_len, 1), lambda s, p: (s, 0))
    flat = pl.BlockSpec((1, 1, seq_len), lambda s, p: (s, 0, 0))
    total = pl.BlockSpec((1, seq_len, wide // HD), lambda s, p: (p, s, 0))
    return block, [table] * 3 + [tall] * 2 + [flat] * 2, total


def attend(projected, bias, tables, seq_here, seq_len):
    tokens, piece = projected.shape[0], projected.shape[1] // 3
    wide = 2 * HD
    pairs = piece // wide
    block, extra, total = attention_specs(tables, seq_len, wide)
    shifted = [
        pl.BlockSpec((seq_len, wide), functools.partial(lambda k, s, p: (s, p + k * pairs), k))
        for k in range(3)
    ]
    biases = [
        pl.BlockSpec((1, wide), functools.partial(lambda k, s, p: (0, p + k * pairs), k))
        for k in range(3)
    ]
    whole = jax.ShapeDtypeStruct((tokens, piece), BF16)
    return pl.pallas_call(
        attend_kernel,
        grid=(seq_here, pairs),
        in_specs=shifted + biases + extra,
        out_specs=[block] * 4 + [total],
        out_shape=[whole] * 4 + [jax.ShapeDtypeStruct((pairs, tokens, wide // HD), F32)],
        cost_estimate=pl.CostEstimate(
            flops=4 * tokens * seq_len * piece, bytes_accessed=20 * tokens * piece,
            transcendentals=tokens * seq_len * piece // HD,
        ),
        name="attend",
    )(projected, projected, projected, bias, bias, bias, *tables)


def attend_back(queries, keys, values, attended, grad, total_log, tables, seq_here, seq_len):
    tokens, piece = queries.shape
    wide = 2 * HD
    pairs = piece // wide
    block, extra, total = attention_specs(tables, seq_len, wide)
    whole = jax.ShapeDtypeStruct((tokens, piece), BF16)
    return pl.pallas_call(
        attend_back_kernel,
        grid=(seq_here, pairs),
        in_specs=[block] * 5 + [total] + extra,
        out_specs=[block] * 3,
        out_shape=[whole] * 3,
        cost_estimate=pl.CostEstimate(
            flops=10 * tokens * seq_len * piece, bytes_accessed=20 * tokens * piece,
            transcendentals=tokens * seq_len * piece // HD,
        ),
        name="attend_back",
    )(queries, keys, values, attended, grad, total_log, *tables)


MESH = pl.DeviceIdType.MESH


def partners():
    col = lax.axis_index("col")
    cols = lax.axis_size("col")
    across = lax.rem(col + cols // 2, cols)
    return {"col": col + 1 - 2 * lax.rem(col, 2)}, {"col": across}, {"row": 1 - lax.axis_index("row")}


def meet(devices):
    barrier = pltpu.get_barrier_semaphore()
    for device in devices:
        pl.semaphore_signal(barrier, inc=1, device_id=device, device_id_type=MESH)
    pl.semaphore_wait(barrier, len(devices))


def remote(source, target, sems, k, device):
    return pltpu.make_async_remote_copy(
        src_ref=source,
        dst_ref=target,
        send_sem=sems.at[0, k],
        recv_sem=sems.at[1, k],
        device_id=device,
        device_id_type=MESH,
    )


def remote_sems(count):
    return pltpu.SemaphoreType.DMA((2, count))


def sum_scratch(size, width):
    half = size // 2
    return [
        pltpu.VMEM((3, size, width), BF16),
        pltpu.VMEM((2, half, width), BF16),
        pltpu.VMEM((2, size, width), BF16),
        pltpu.VMEM((2, half, width), F32),
        remote_sems(6),
    ]


def block_sum(part_of, filler, sent, passed, got, kept, sems):
    near, far, _ = partners()
    size = sent.shape[1]
    half = size // 2
    low, high = pl.ds(0, half), pl.ds(half, half)
    copies = [
        remote(sent.at[2, low], passed.at[0], sems, 0, near),
        remote(sent.at[2, high], passed.at[1], sems, 1, far),
        remote(sent.at[0, low], got.at[0, low], sems, 2, near),
        remote(sent.at[1, high], got.at[1, high], sems, 3, far),
        remote(sent.at[1, low], got.at[1, low], sems, 4, far),
        remote(sent.at[0, high], got.at[0, high], sems, 5, near),
    ]
    sent[2] = part_of(3).astype(BF16)
    copies[0].start()
    copies[1].start()
    part = part_of(1)
    sent[0, low] = part[:half].astype(BF16)
    copies[2].start()
    kept[0] = part[half:]
    part = part_of(2)
    sent[1, high] = part[half:].astype(BF16)
    copies[3].start()
    kept[1] = part[:half]
    copies[0].wait_recv()
    sent[1, low] = (kept[1] + passed[0].astype(F32)).astype(BF16)
    copies[4].start()
    copies[1].wait_recv()
    sent[0, high] = (kept[0] + passed[1].astype(F32)).astype(BF16)
    copies[5].start()
    own = part_of(0)
    filler()
    for copy in copies[2:]:
        copy.wait_recv()
    own = own + got[0].astype(F32) + got[1].astype(F32)
    for copy in copies:
        copy.wait_send()
    return own


def block_gather(blocks, use, sems):
    near, far, _ = partners()
    size = blocks.shape[0] // 4
    half = size // 2
    copies = [
        remote(blocks.at[pl.ds(0, size)], blocks.at[pl.ds(size, size)], sems, 0, near),
        remote(blocks.at[pl.ds(0, size)], blocks.at[pl.ds(2 * size, size)], sems, 1, far),
        remote(
            blocks.at[pl.ds(2 * size, half)], blocks.at[pl.ds(3 * size, half)], sems, 2, near
        ),
        remote(
            blocks.at[pl.ds(size + half, half)],
            blocks.at[pl.ds(3 * size + half, half)],
            sems,
            3,
            far,
        ),
    ]
    copies[0].start()
    copies[1].start()
    use(0)
    copies[1].wait_recv()
    copies[2].start()
    copies[0].wait_recv()
    copies[3].start()
    use(1)
    use(2)
    copies[2].wait_recv()
    copies[3].wait_recv()
    use(3)
    for copy in copies:
        copy.wait_send()


def pair_sums(first, second, stats, sems, k):
    _, _, other = partners()
    lane = lax.broadcasted_iota(jnp.int32, stats.shape[1:], 1)
    stats[0] = jnp.where(lane == 0, first, jnp.where(lane == 1, second, 0.0))
    copy = remote(stats.at[0], stats.at[1], sems, k, other)
    copy.start()
    copy.wait()
    both = stats[0] + stats[1]
    return both[:, 0:1], both[:, 1:2]


def scale_rows(values, stats, sems, k):
    total, squares = pair_sums(
        jnp.sum(values, 1, keepdims=True), jnp.sum(values * values, 1, keepdims=True), stats, sems, k
    )
    center = total / D
    inverse = lax.rsqrt(squares / D - center * center + EPSILON)
    return (values - center) * inverse, inverse


def project_kernel(
    x_in, gain, shift, weight, full_out, proj_out, scaled_out, inverse_out,
    loaded, sent, got, stats, load_sem, gather_sems, sems,
):
    near, far, other = partners()
    row = lax.axis_index("row")
    size = x_in.shape[0]
    kinds, _, width = weight.shape
    half = width // 2
    load = pltpu.make_async_copy(weight, loaded, load_sem)
    load.start()
    meet((near, far, other))
    scaled, inverse = scale_rows(x_in[...].astype(F32), stats, sems, 0)
    scaled_out[...] = scaled
    inverse_out[...] = jnp.broadcast_to(inverse, inverse_out.shape)
    full_out[pl.ds(0, size)] = (scaled * gain[...] + shift[...]).astype(BF16)
    mine = pl.ds(pl.multiple_of(row * half, half), half)
    theirs = pl.ds(pl.multiple_of((1 - row) * half, half), half)
    swaps = [
        remote(
            sent.at[pl.ds(b * size, size)], got.at[pl.ds(b * size, size)], sems, 1 + b, other
        )
        for b in range(4)
    ]

    def finish(b):
        at = pl.ds(b * size, size)
        swaps[b].wait_recv()
        proj_out[at] += got[at]

    def use(b):
        at = pl.ds(b * size, size)
        if b == 0:
            load.wait()
        values = full_out[at]
        for k in range(kinds):
            sent[at, k * half : (k + 1) * half] = dot(values, loaded[k, :, theirs])
        swaps[b].start()
        for k in range(kinds):
            proj_out[at, k * half : (k + 1) * half] = dot(values, loaded[k, :, mine])
        if b == 3:
            for done in range(4):
                finish(done)

    block_gather(full_out, use, gather_sems)
    for swap in swaps:
        swap.wait_send()


def project(x, gain, shift, weight):
    size, width = x.shape
    kinds, _, columns = weight.shape
    piece = kinds * columns // 2
    vmem = pl.BlockSpec(memory_space=pltpu.VMEM)
    return pl.pallas_call(
        project_kernel,
        in_specs=[vmem, vmem, vmem, pl.BlockSpec(memory_space=pl.ANY)],
        out_specs=[vmem] * 4,
        out_shape=[
            jax.ShapeDtypeStruct((4 * size, width), BF16),
            jax.ShapeDtypeStruct((4 * size, piece), F32),
            jax.ShapeDtypeStruct((size, width), F32),
            jax.ShapeDtypeStruct((size, LANES), F32),
        ],
        scratch_shapes=[
            pltpu.VMEM(weight.shape, BF16),
            pltpu.VMEM((4 * size, piece), F32),
            pltpu.VMEM((4 * size, piece), F32),
            pltpu.VMEM((2, size, LANES), F32),
            pltpu.SemaphoreType.DMA,
            remote_sems(4),
            remote_sems(5),
        ],
        compiler_params=pltpu.CompilerParams(
            collective_id=2, has_side_effects=True, vmem_limit_bytes=60 << 20
        ),
        name="project",
    )(x, gain, shift, weight)


def hidden_kernel(
    attended, mixing, x_in, gain, shift, gate_hbm, up_hbm, upstream_hbm, lowering_hbm,
    middle_out, scaled_out, inverse_out, full_out, hidden_out, gate_out, up_out,
    gate_w, up_w, upstream, lowering, attended_got, back_sent, back_got, back, stats,
    gates_sent, gates_got, gates_kept,
    s_sent, s_passed, s_got, s_kept, s_sems, load_sems, gather_sems, sems,
):
    near, far, other = partners()
    row = lax.axis_index("row")
    size = x_in.shape[0]
    part = size // 2
    depth = attended.shape[1]
    units = gate_w.shape[1]
    loads = [
        pltpu.make_async_copy(source, target, load_sems.at[k])
        for k, (source, target) in enumerate(
            ((upstream_hbm, upstream), (lowering_hbm, lowering), (gate_hbm, gate_w), (up_hbm, up_w))
        )
    ]
    for load in loads:
        load.start()
    meet((near, far, other))
    swap = remote(attended, attended_got, sems, 0, other)
    swap.start()

    def rows_of(b, whose):
        return pl.ds(pl.multiple_of(b * size + whose * part, part), part)

    loads[0].wait()
    loads[1].wait()
    for b in range(4):
        back_sent[pl.ds(b * part, part)] = dot_t(
            upstream[rows_of(b, 1 - row)], lowering[...], BF16
        )
    back_swap = remote(back_sent, back_got, sems, 1, other)
    back_swap.start()
    swap.wait_recv()
    mine = pl.ds(pl.multiple_of(row * depth, depth), depth)
    theirs = pl.ds(pl.multiple_of((1 - row) * depth, depth), depth)

    def part_of(b):
        at = pl.ds(b * size, size)
        return dot(attended[at], mixing[mine]) + dot(attended_got[at], mixing[theirs])

    def filler():
        back_swap.wait_recv()
        for b in range(4):
            at = pl.ds(b * part, part)
            back[at] = dot_t(upstream[rows_of(b, row)], lowering[...]) + back_got[at].astype(F32)
        loads[2].wait()
        loads[3].wait()

    middle = x_in[...].astype(F32) + block_sum(
        part_of, filler, s_sent, s_passed, s_got, s_kept, s_sems
    )
    middle_out[...] = middle
    scaled, inverse = scale_rows(middle, stats, sems, 2)
    scaled_out[...] = scaled
    inverse_out[...] = jnp.broadcast_to(inverse, inverse_out.shape)
    full_out[pl.ds(0, size)] = (scaled * gain[...] + shift[...]).astype(BF16)
    gate_swaps = [remote(gates_sent.at[b], gates_got.at[b], sems, 3 + b, other) for b in range(4)]

    def returns(b):
        at = rows_of(b, row)
        return [
            remote(ref.at[at], ref.at[at], sems, 7 + 3 * b + k, other)
            for k, ref in enumerate((gate_out, up_out, hidden_out))
        ]

    def finish(b):
        gate_swaps[b].wait_recv()
        gate = gates_kept[b % 2, :, :units] + gates_got[b, :, :units].astype(F32)
        up = gates_kept[b % 2, :, units:] + gates_got[b, :, units:].astype(F32)
        grad = back[pl.ds(b * part, part)]
        sigmoid = jax.nn.sigmoid(gate)
        at = rows_of(b, row)
        gate_out[at] = (grad * up * sigmoid * (1.0 + gate * (1.0 - sigmoid))).astype(BF16)
        up_out[at] = (grad * gate * sigmoid).astype(BF16)
        hidden_out[at] = (gate * sigmoid * up).astype(BF16)
        for copy in returns(b):
            copy.start()

    def use(b):
        values = full_out[rows_of(b, 1 - row)]
        gates_sent[b, :, :units] = dot(values, gate_w[...], BF16)
        gates_sent[b, :, units:] = dot(values, up_w[...], BF16)
        gate_swaps[b].start()
        values = full_out[rows_of(b, row)]
        gates_kept[b % 2, :, :units] = dot(values, gate_w[...])
        gates_kept[b % 2, :, units:] = dot(values, up_w[...])
        finish(b)

    block_gather(full_out, use, gather_sems)
    swap.wait_send()
    back_swap.wait_send()
    for b in range(4):
        gate_swaps[b].wait_send()
        at = rows_of(b, 1 - row)
        for copy in returns(b):
            copy.wait_send()
        for k, ref in enumerate((gate_out, up_out, hidden_out)):
            remote(ref.at[at], ref.at[at], sems, 7 + 3 * b + k, other).wait_recv()


def hidden_units(attended, mixing, x, gain, shift, gate_w, up_w, upstream, lowering):
    size, width = x.shape
    tokens = 4 * size
    units = gate_w.shape[1]
    part = size // 2
    vmem = pl.BlockSpec(memory_space=pltpu.VMEM)
    anywhere = pl.BlockSpec(memory_space=pl.ANY)
    return pl.pallas_call(
        hidden_kernel,
        in_specs=[vmem] * 5 + [anywhere] * 4,
        out_specs=[vmem] * 7,
        out_shape=[
            jax.ShapeDtypeStruct((size, width), F32),
            jax.ShapeDtypeStruct((size, width), F32),
            jax.ShapeDtypeStruct((size, LANES), F32),
            jax.ShapeDtypeStruct((tokens, width), BF16),
        ]
        + [jax.ShapeDtypeStruct((tokens, units), BF16)] * 3,
        scratch_shapes=[
            pltpu.VMEM(gate_w.shape, BF16),
            pltpu.VMEM(up_w.shape, BF16),
            pltpu.VMEM(upstream.shape, BF16),
            pltpu.VMEM(lowering.shape, BF16),
            pltpu.VMEM(attended.shape, BF16),
            pltpu.VMEM((tokens // 2, units), BF16),
            pltpu.VMEM((tokens // 2, units), BF16),
            pltpu.VMEM((tokens // 2, units), F32),
            pltpu.VMEM((2, size, LANES), F32),
            pltpu.VMEM((4, part, 2 * units), BF16),
            pltpu.VMEM((4, part, 2 * units), BF16),
            pltpu.VMEM((2, part, 2 * units), F32),
            *sum_scratch(size, width),
            pltpu.SemaphoreType.DMA((4,)),
            remote_sems(4),
            remote_sems(19),
        ],
        compiler_params=pltpu.CompilerParams(
            collective_id=3, has_side_effects=True, vmem_limit_bytes=61 << 20
        ),
        name="hidden_units",
    )(attended, mixing, x, gain, shift, gate_w, up_w, upstream, lowering)


def local(
    block_input,
    segment_ids,
    positions,
    attention_gain,
    attention_shift,
    projection_weight,
    projection_bias,
    mixing_weight,
    feedforward_gain,
    feedforward_shift,
    gating_weight,
    lowering_weight,
    cotangent,
):
    own_tokens, local_width = block_input.shape
    seq_here, seq_len = segment_ids.shape
    tokens = seq_here * seq_len
    row = lax.axis_index("row")
    col = lax.axis_index("col")
    cols = lax.axis_size("col")
    tie = lax.optimization_barrier

    def mine(values, axis):
        size = values.shape[axis] // 2
        return lax.dynamic_slice_in_dim(values, row * size, size, axis)

    def theirs(values, axis):
        size = values.shape[axis] // 2
        return lax.dynamic_slice_in_dim(values, (1 - row) * size, size, axis)

    def both(values, axis):
        other = row_swap(values)
        return jnp.concatenate(
            [jnp.where(row == 0, values, other), jnp.where(row == 0, other, values)], axis
        )

    def reorder(table):
        blocks = table.reshape(cols, own_tokens)
        return jnp.take(blocks, col ^ jnp.arange(cols), axis=0).reshape(-1)

    order = reorder(jnp.tile(jnp.arange(seq_len), seq_here))
    segments = reorder(segment_ids)
    tables = rotary_tables(reorder(positions), HD) + [
        segments[:, None],
        order[:, None],
        segments.reshape(seq_here, 1, seq_len),
        order.reshape(seq_here, 1, seq_len),
    ]

    gating_pair = jnp.swapaxes(gating_weight, 0, 1)
    bias = mine(projection_bias, 1).reshape(1, -1)
    normed_full, projected, scaled_one, inverse_one = project(
        block_input,
        attention_gain[None],
        attention_shift[None],
        jnp.swapaxes(projection_weight, 0, 1),
    )
    inverse_one = inverse_one[:, :1]
    normed_full, cotangent = tie((normed_full, cotangent))
    gate_weight, up_weight = gating_pair[0], gating_pair[1]
    queries, keys, values, attended, total_log = attend(
        projected, bias, tables, seq_here, seq_len
    )
    upstream_full = gather_tokens(cotangent)
    middle, scaled_two, inverse_two, normed_two_full, hidden_full, gate_back, up_back = (
        hidden_units(
            attended,
            mixing_weight,
            block_input,
            feedforward_gain[None],
            feedforward_shift[None],
            gate_weight,
            up_weight,
            upstream_full,
            lowering_weight,
        )
    )
    inverse_two = inverse_two[:, :1]
    attended_full = both(attended, 1)

    early = local_width * 3 // 4
    first_rows, last_rows = normed_two_full[:, :early], normed_two_full[:, early:]
    parts = (t_dot(first_rows, gate_back, BF16), t_dot(first_rows, up_back, BF16))
    gate_back, up_back, parts = tie((gate_back, up_back, parts))
    gating_early = lax.psum(parts, "dp")

    normed_two_grad = sum_tokens(dot_t(gate_back, gate_weight) + dot_t(up_back, up_weight))
    middle_grad = cotangent.astype(jnp.float32) + norm_back(
        normed_two_grad, feedforward_gain, scaled_two, inverse_two
    )
    middle_wire = middle_grad.astype(jnp.bfloat16)
    middle_full = gather_tokens(middle_wire)
    attended_sent = row_swap(dot_t(middle_full, theirs(mixing_weight, 0), BF16))
    attended_grad = dot_t(middle_full, mine(mixing_weight, 0)) + attended_sent.astype(F32)
    grads = attend_back(
        queries, keys, values, attended, attended_grad.astype(BF16), total_log, tables,
        seq_here, seq_len,
    )
    backs = [both(grad, 1) for grad in grads]
    projection_bgrad = jnp.concatenate([jnp.sum(back, 0, dtype=F32) for back in backs])
    normed_one_grad = sum_tokens(
        sum(dot_t(back, projection_weight[:, i]) for i, back in enumerate(backs))
    )
    input_grad = (
        middle_grad + norm_back(normed_one_grad, attention_gain, scaled_one, inverse_one)
    ).astype(jnp.bfloat16)
    block_output = (middle + sum_tokens(dot(hidden_full, lowering_weight))).astype(jnp.bfloat16)

    sums = jnp.concatenate(
        [
            jnp.sum(normed_one_grad * scaled_one, 0),
            jnp.sum(normed_one_grad, 0),
            jnp.sum(normed_two_grad * scaled_two, 0),
            jnp.sum(normed_two_grad, 0),
        ]
    )
    bit = 1
    while bit < cols:
        sums = sums + col_swap(sums, bit)
        bit *= 2
    small = jnp.concatenate([sums, projection_bgrad])
    lanes = 128
    unit = 8 * lanes
    small = jnp.pad(small, (0, -small.shape[0] % unit)).reshape(-1, lanes)

    totals = line_sum(
        [
            t_dot(hidden_full, upstream_full, BF16),
            t_dot(attended_full, middle_full, BF16),
            *(t_dot(normed_full, back, BF16) for back in backs),
            t_dot(last_rows, gate_back, BF16),
            t_dot(last_rows, up_back, BF16),
            small,
        ],
        [8, 4, 4, 4, 4, 2, 2, 1],
    )
    lowering_wgrad, mixing_wgrad = totals[0], totals[1]
    sums = totals[7].reshape(-1)
    projection_bgrad = sums[4 * local_width : 4 * local_width + projection_bgrad.shape[0]]
    return (
        block_output,
        input_grad,
        sums[:local_width],
        sums[local_width : 2 * local_width],
        jnp.stack(totals[2:5], 1).astype(F32),
        projection_bgrad.reshape(3, -1),
        mixing_wgrad.astype(F32),
        sums[2 * local_width : 3 * local_width],
        sums[3 * local_width : 4 * local_width],
        jnp.stack(
            [jnp.concatenate([gating_early[k], totals[5 + k]]) for k in range(2)], 1
        ).astype(F32),
        lowering_wgrad.astype(F32),
    )


def solution(mesh):
    return jax.shard_map(
        local,
        mesh=mesh,
        in_specs=(
            P(("dp", "col"), "row"),
            P("dp", None),
            P("dp", None),
            P("row"),
            P("row"),
            P("row", None, "col"),
            P(None, "col"),
            P("col", "row"),
            P("row"),
            P("row"),
            P("row", None, "col"),
            P("col", "row"),
            P(("dp", "col"), "row"),
        ),
        out_specs=(
            P(("dp", "col"), "row"),
            P(("dp", "col"), "row"),
            P("row"),
            P("row"),
            P("row", None, "col"),
            P(None, "col"),
            P("col", "row"),
            P("row"),
            P("row"),
            P("row", None, "col"),
            P("col", "row"),
        ),
        check_vma=False,
    )
```

```python
import functools
import math

import jax
import jax.numpy as jnp
from jax import lax
from jax.experimental import pallas as pl
from jax.experimental.pallas import tpu as pltpu
from jax.sharding import PartitionSpec as P

D = 2048
HD = 64


EPSILON = 1e-05
MASKED = -1e30
WINDOW = 2
LANES = 128
BF16 = jnp.bfloat16
F32 = jnp.float32


def col_swap(values, bit):
    count = lax.axis_size("col")
    return lax.ppermute(values, "col", [(i, i ^ bit) for i in range(count)])


def row_swap(values):
    return lax.ppermute(values, "row", [(0, 1), (1, 0)])


def gather_tokens(values):
    count = lax.axis_size("col")
    if count == 4:
        half = values.shape[0] // 2
        first = col_swap(values, 1)
        second = col_swap(values, 2)
        third_a = col_swap(second[:half], 1)
        third_b = col_swap(first[half:], 2)
        return jnp.concatenate([values, first, second, third_a, third_b], 0)
    bit = 1
    while bit < count:
        values = jnp.concatenate([values, col_swap(values, bit)], 0)
        bit *= 2
    return values


def sum_tokens(partial_rows):
    count = lax.axis_size("col")
    size = partial_rows.shape[0] // count
    if count == 4:
        half = size // 2
        own, first, second, third = (partial_rows[i * size : (i + 1) * size] for i in range(4))
        third = third.astype(BF16)
        got_a = col_swap(third[:half], 1).astype(F32)
        got_b = col_swap(third[half:], 2).astype(F32)
        to_second = jnp.concatenate([second[:half] + got_a, second[half:]], 0).astype(BF16)
        to_first = jnp.concatenate([first[:half], first[half:] + got_b], 0).astype(BF16)
        return own + col_swap(to_first, 1).astype(F32) + col_swap(to_second, 2).astype(F32)
    bit = count // 2
    while bit:
        kept = partial_rows.shape[0] // 2
        got = col_swap(partial_rows[kept:].astype(BF16), bit).astype(F32)
        partial_rows = partial_rows[:kept] + got
        bit //= 2
    return partial_rows


def row_sums(first, second):
    return lax.psum((first, second), "row")


def normalize(values):
    total, squares = row_sums(
        jnp.sum(values, 1, keepdims=True), jnp.sum(values * values, 1, keepdims=True)
    )
    center = total / D
    spread = squares / D - center * center
    inverse = lax.rsqrt(spread + EPSILON)
    return ((values - center) * inverse, inverse)


def norm_back(upstream, gain, scaled, inverse):
    weighted = upstream * gain
    total, mixed = row_sums(
        jnp.sum(weighted, 1, keepdims=True), jnp.sum(weighted * scaled, 1, keepdims=True)
    )
    return inverse * (weighted - total / D - scaled * (mixed / D))


def dot(a, b, kind=F32):
    return jnp.dot(a, b, preferred_element_type=F32).astype(kind)


def dot_t(a, b, kind=F32):
    return lax.dot_general(a, b, (((1,), (1,)), ((), ())), preferred_element_type=F32).astype(kind)


def t_dot(a, b, kind=F32):
    return lax.dot_general(a, b, (((0,), (0,)), ((), ())), preferred_element_type=F32).astype(kind)


def line_kernel(pieces, kinds, *refs):
    count = len(kinds)
    own, out = refs[:count], refs[count : 2 * count]
    inwards, part, across = (refs[(2 + k) * count : (3 + k) * count] for k in range(3))
    sent_in, got_in, got_across, sent_out, got_out = refs[5 * count :]
    size = lax.axis_size("dp")
    me = lax.axis_index("dp")
    half = size // 2
    low = me < half
    inner = jnp.where(low, me + 1, me - 1)
    outer = jnp.where(low, jnp.maximum(me - 1, 0), jnp.minimum(me + 1, size - 1))
    end = (me == 0) | (me == size - 1)
    middle = (me == half - 1) | (me == half)

    barrier = pltpu.get_barrier_semaphore()
    pl.semaphore_signal(
        barrier, inc=1, device_id={"dp": inner}, device_id_type=pl.DeviceIdType.MESH
    )

    @pl.when(jnp.logical_not(end))
    def _():
        pl.semaphore_signal(
            barrier, inc=1, device_id={"dp": outer}, device_id_type=pl.DeviceIdType.MESH
        )
        pl.semaphore_wait(barrier, 2)

    @pl.when(end)
    def _():
        pl.semaphore_wait(barrier, 1)

    def copy(source, target, sent, got, to):
        return pltpu.make_async_remote_copy(
            src_ref=source,
            dst_ref=target,
            send_sem=sent,
            recv_sem=got,
            device_id={"dp": to},
            device_id_type=pl.DeviceIdType.MESH,
        )

    def to_inner(k):
        a, start, rows = pieces[k]
        at = pl.ds(start, rows)
        return copy(own[a].at[at], inwards[a].at[at], sent_in.at[k], got_in.at[k], inner)

    def part_to_inner(k):
        a, start, rows = pieces[k]
        at = pl.ds(start, rows)
        return copy(part[a].at[at], inwards[a].at[at], sent_in.at[k], got_in.at[k], inner)

    def part_across(k):
        a, start, rows = pieces[k]
        at = pl.ds(start, rows)
        return copy(part[a].at[at], across[a].at[at], sent_in.at[k], got_across.at[k], inner)

    def to_outer(k):
        a, start, rows = pieces[k]
        at = pl.ds(start, rows)
        return copy(out[a].at[at], out[a].at[at], sent_out.at[k], got_out.at[k], outer)

    def add(first, second, target, k):
        a, start, rows = pieces[k]
        at = pl.ds(start, rows)
        target[a][at] = (
            first[a][at].astype(F32) + second[a][at].astype(F32)
        ).astype(kinds[a])

    total = len(pieces)

    @pl.when(end)
    def _():
        for k in range(total):
            if k >= WINDOW:
                to_inner(k - WINDOW).wait_send()
            to_inner(k).start()
        for k in range(max(total - WINDOW, 0), total):
            to_inner(k).wait_send()
        for k in range(total):
            to_outer(k).wait_recv()

    def inward(k):
        to_inner(k).wait_recv()
        add(own, inwards, part, k)

        @pl.when(middle)
        def _():
            part_across(k).start()

        @pl.when(jnp.logical_not(middle))
        def _():
            part_to_inner(k).start()

    def outward(k):
        @pl.when(middle)
        def _():
            part_across(k).wait_recv()
            add(part, across, out, k)
            to_outer(k).start()

        @pl.when(jnp.logical_not(middle))
        def _():
            to_outer(k).wait_recv()
            to_outer(k).start()

    @pl.when(jnp.logical_not(end))
    def _():
        for k in range(total + 1):
            if k < total:
                inward(k)
            if k:
                outward(k - 1)
        for k in range(total):
            part_across(k).wait_send()
            to_outer(k).wait_send()


def line_sum(arrays, splits):
    pieces = []
    for a, (array, split) in enumerate(zip(arrays, splits)):
        rows = array.shape[0] // split
        pieces += [(a, i * rows, rows) for i in range(split)]
    kinds = [array.dtype for array in arrays]
    vmem = pl.BlockSpec(memory_space=pltpu.VMEM)
    scratch = [pltpu.VMEM(array.shape, array.dtype) for array in arrays]
    sems = [pltpu.SemaphoreType.DMA((len(pieces),)) for _ in range(5)]
    return pl.pallas_call(
        functools.partial(line_kernel, pieces, kinds),
        out_shape=[jax.ShapeDtypeStruct(array.shape, array.dtype) for array in arrays],
        in_specs=[vmem] * len(arrays),
        out_specs=[vmem] * len(arrays),
        scratch_shapes=scratch * 3 + sems,
        compiler_params=pltpu.CompilerParams(
            collective_id=1, has_side_effects=True, vmem_limit_bytes=60 << 20
        ),
        name="line_sum",
    )(*arrays)


def rotary_tables(positions, head_size):
    half = head_size // 8
    lane = jnp.arange(2 * head_size) % head_size
    freq = jnp.exp((lane % half).astype(F32) * (-math.log(10000.0) / half))
    theta = positions.reshape(-1).astype(jnp.float32)[:, None] * freq
    first, second = lane < half, (lane >= half) & (lane < 2 * half)
    sine = jnp.sin(theta)
    return [
        jnp.where(first | second, jnp.cos(theta), 1.0),
        jnp.where(first, -sine, 0.0),
        jnp.where(second, sine, 0.0),
    ]


def scores_of(queries, keys, allowed):
    scores = lax.dot_general(
        queries, keys, (((1,), (1,)), ((), ())), preferred_element_type=F32
    ) * (1.0 / math.sqrt(HD))
    return jnp.where(allowed, scores, MASKED)


def allowed_of(position):
    length = position.shape[0]
    cols = lax.axis_size("col")
    col = lax.axis_index("col")
    own = length * pl.num_programs(0) // cols

    def order_of(axis):
        shape = (length, 1) if axis == 0 else (1, length)
        index = lax.broadcasted_iota(jnp.int32, shape, axis)
        order = jnp.zeros(shape, jnp.int32)
        for k in range(length // own):
            block = pl.program_id(0) * (length // own) + k
            block = 2 * lax.rem(lax.div(col, 2) + lax.div(block, 2), 2) + lax.rem(col + block, 2)
            start = lax.rem(block * own, length)
            order = jnp.where(index >= k * own, start + index - k * own, order)
        return order

    order_q, order_k = order_of(0), order_of(1)
    return (order_k <= order_q) & (order_k >= order_q - position[...])


def attend_kernel(
    q_in, k_in, v_in, q_bias, k_bias, v_bias, same, above, below, position, own_hbm,
    q_out, k_out, v_out, attended_out, total_out, blocks_out, blocks, load_sem, sems,
):
    step = HD // 8
    wide = q_in.shape[1]

    near, far, _ = partners()
    size = blocks.shape[0] // 4
    part = size // 2
    first, second = pl.ds(size, size), pl.ds(2 * size, size)
    copies = [
        remote(blocks.at[pl.ds(0, size)], blocks.at[first], sems, 0, near),
        remote(blocks.at[pl.ds(0, size)], blocks.at[second], sems, 1, far),
        remote(blocks.at[pl.ds(2 * size, part)], blocks.at[pl.ds(3 * size, part)], sems, 2, near),
        remote(
            blocks.at[pl.ds(size + part, part)],
            blocks.at[pl.ds(3 * size + part, part)],
            sems,
            3,
            far,
        ),
    ]
    at_end = (pl.program_id(0) == pl.num_programs(0) - 1) & (
        pl.program_id(1) == pl.num_programs(1) - 1
    )

    @pl.when((pl.program_id(0) == 0) & (pl.program_id(1) == 0))
    def _():
        load = pltpu.make_async_copy(own_hbm, blocks.at[pl.ds(0, size)], load_sem)
        load.start()
        meet((near, far))
        load.wait()
        copies[0].start()
        copies[1].start()

    @pl.when(at_end)
    def _():
        copies[1].wait_recv()
        copies[2].start()
        copies[0].wait_recv()
        copies[3].start()

    def rotate(values):
        return (
            values * same[...]
            + pltpu.roll(values, wide - step, 1) * above[...]
            + pltpu.roll(values, step, 1) * below[...]
        )

    queries = rotate(q_in[...] + q_bias[...]).astype(BF16)
    keys = rotate(k_in[...] + k_bias[...]).astype(BF16)
    values = (v_in[...] + v_bias[...]).astype(BF16)
    q_out[...] = queries
    k_out[...] = keys
    v_out[...] = values
    allowed = allowed_of(position)
    results, totals = [], []
    for h in range(wide // HD):
        at = slice(h * HD, (h + 1) * HD)
        scores = scores_of(queries[:, at], keys[:, at], allowed)
        peak = jnp.max(scores, -1, keepdims=True)
        raised = jnp.exp(scores - peak)
        denominator = jnp.sum(raised, -1, keepdims=True)
        probs = (raised / denominator).astype(BF16)
        results.append(jnp.dot(probs, values[:, at], preferred_element_type=F32))
        totals.append(peak + jnp.log(denominator))
    attended_out[...] = jnp.concatenate(results, 1).astype(BF16)
    total_out[0] = jnp.concatenate(totals, 1)

    @pl.when(at_end)
    def _():
        copies[2].wait_recv()
        copies[3].wait_recv()
        for copy in copies:
            copy.wait_send()
        blocks_out[...] = blocks[...]


def attend_back_kernel(
    q_in, k_in, v_in, attended_in, grad_in, total_in, same, above, below, position, q_out, k_out, v_out,
):
    step = HD // 8
    wide = q_in.shape[1]

    def rotate_back(grads):
        return (
            grads * same[...]
            + pltpu.roll(grads * above[...], step, 1)
            + pltpu.roll(grads * below[...], wide - step, 1)
        )

    allowed = allowed_of(position)
    products = grad_in[...].astype(F32) * attended_in[...].astype(F32)
    q_grads, k_grads, v_grads = [], [], []
    for h in range(wide // HD):
        at = slice(h * HD, (h + 1) * HD)
        queries, keys, values = q_in[:, at], k_in[:, at], v_in[:, at]
        grad = grad_in[:, at]
        recovered = jnp.exp(scores_of(queries, keys, allowed) - total_in[0][:, h : h + 1])
        prob_grad = lax.dot_general(
            grad, values, (((1,), (1,)), ((), ())), preferred_element_type=F32
        )
        row_dot = jnp.sum(products[:, at], 1, keepdims=True)
        score_grad = (recovered * (prob_grad - row_dot) * (1.0 / math.sqrt(HD))).astype(BF16)
        q_grads.append(jnp.dot(score_grad, keys, preferred_element_type=F32))
        k_grads.append(t_dot(score_grad, queries))
        v_grads.append(t_dot(recovered.astype(BF16), grad))
    q_out[...] = rotate_back(jnp.concatenate(q_grads, 1)).astype(BF16)
    k_out[...] = rotate_back(jnp.concatenate(k_grads, 1)).astype(BF16)
    v_out[...] = jnp.concatenate(v_grads, 1).astype(BF16)


def attention_specs(tables, seq_len, wide):
    block = pl.BlockSpec((seq_len, wide), lambda s, p: (s, p))
    table = pl.BlockSpec((seq_len, wide), lambda s, p: (s, 0))
    tall = pl.BlockSpec((seq_len, 1), lambda s, p: (s, 0))
    total = pl.BlockSpec((1, seq_len, wide // HD), lambda s, p: (p, s, 0))
    return block, [table] * 3 + [tall], total


def attend(projected, bias, tables, own, seq_here, seq_len):
    tokens, piece = projected.shape[0], projected.shape[1] // 3
    wide = 2 * HD
    pairs = piece // wide
    block, extra, total = attention_specs(tables, seq_len, wide)
    shifted = [
        pl.BlockSpec((seq_len, wide), functools.partial(lambda k, s, p: (s, p + k * pairs), k))
        for k in range(3)
    ]
    biases = [
        pl.BlockSpec((1, wide), functools.partial(lambda k, s, p: (0, p + k * pairs), k))
        for k in range(3)
    ]
    whole = jax.ShapeDtypeStruct((tokens, piece), BF16)
    return pl.pallas_call(
        attend_kernel,
        grid=(seq_here, pairs),
        in_specs=shifted + biases + extra + [pl.BlockSpec(memory_space=pl.ANY)],
        out_specs=[block] * 4 + [total, pl.BlockSpec((tokens, own.shape[1]), lambda s, p: (0, 0))],
        out_shape=[whole] * 4
        + [
            jax.ShapeDtypeStruct((pairs, tokens, wide // HD), F32),
            jax.ShapeDtypeStruct((tokens, own.shape[1]), BF16),
        ],
        scratch_shapes=[
            pltpu.VMEM((tokens, own.shape[1]), BF16),
            pltpu.SemaphoreType.DMA,
            remote_sems(4),
        ],
        compiler_params=pltpu.CompilerParams(
            collective_id=4, has_side_effects=True, vmem_limit_bytes=48 << 20
        ),
        cost_estimate=pl.CostEstimate(
            flops=4 * tokens * seq_len * piece, bytes_accessed=20 * tokens * piece,
            transcendentals=tokens * seq_len * piece // HD,
        ),
        name="attend",
    )(projected, projected, projected, bias, bias, bias, *tables, own)


def attend_back(queries, keys, values, attended, grad, total_log, tables, seq_here, seq_len):
    tokens, piece = queries.shape
    wide = 2 * HD
    pairs = piece // wide
    block, extra, total = attention_specs(tables, seq_len, wide)
    whole = jax.ShapeDtypeStruct((tokens, piece), BF16)
    return pl.pallas_call(
        attend_back_kernel,
        grid=(seq_here, pairs),
        in_specs=[block] * 5 + [total] + extra,
        out_specs=[block] * 3,
        out_shape=[whole] * 3,
        cost_estimate=pl.CostEstimate(
            flops=10 * tokens * seq_len * piece, bytes_accessed=20 * tokens * piece,
            transcendentals=tokens * seq_len * piece // HD,
        ),
        name="attend_back",
    )(queries, keys, values, attended, grad, total_log, *tables)


MESH = pl.DeviceIdType.MESH


def partners():
    col = lax.axis_index("col")
    cols = lax.axis_size("col")
    across = lax.rem(col + cols // 2, cols)
    return {"col": col + 1 - 2 * lax.rem(col, 2)}, {"col": across}, {"row": 1 - lax.axis_index("row")}


def meet(devices):
    barrier = pltpu.get_barrier_semaphore()
    for device in devices:
        pl.semaphore_signal(barrier, inc=1, device_id=device, device_id_type=MESH)
    pl.semaphore_wait(barrier, len(devices))


def remote(source, target, sems, k, device):
    return pltpu.make_async_remote_copy(
        src_ref=source,
        dst_ref=target,
        send_sem=sems.at[0, k],
        recv_sem=sems.at[1, k],
        device_id=device,
        device_id_type=MESH,
    )


def remote_sems(count):
    return pltpu.SemaphoreType.DMA((2, count))


def sum_scratch(size, width):
    half = size // 2
    return [
        pltpu.VMEM((3, size, width), BF16),
        pltpu.VMEM((2, half, width), BF16),
        pltpu.VMEM((2, size, width), BF16),
        pltpu.VMEM((2, half, width), F32),
        remote_sems(6),
    ]


def block_sum(part_of, filler, sent, passed, got, kept, sems):
    near, far, _ = partners()
    size = sent.shape[1]
    half = size // 2
    low, high = pl.ds(0, half), pl.ds(half, half)
    copies = [
        remote(sent.at[2, low], passed.at[0], sems, 0, near),
        remote(sent.at[2, high], passed.at[1], sems, 1, far),
        remote(sent.at[0, low], got.at[0, low], sems, 2, near),
        remote(sent.at[1, high], got.at[1, high], sems, 3, far),
        remote(sent.at[1, low], got.at[1, low], sems, 4, far),
        remote(sent.at[0, high], got.at[0, high], sems, 5, near),
    ]
    sent[2] = part_of(3).astype(BF16)
    copies[0].start()
    copies[1].start()
    part = part_of(1)
    sent[0, low] = part[:half].astype(BF16)
    copies[2].start()
    kept[0] = part[half:]
    part = part_of(2)
    sent[1, high] = part[half:].astype(BF16)
    copies[3].start()
    kept[1] = part[:half]
    copies[0].wait_recv()
    sent[1, low] = (kept[1] + passed[0].astype(F32)).astype(BF16)
    copies[4].start()
    copies[1].wait_recv()
    sent[0, high] = (kept[0] + passed[1].astype(F32)).astype(BF16)
    copies[5].start()
    own = part_of(0)
    filler()
    for copy in copies[2:]:
        copy.wait_recv()
    own = own + got[0].astype(F32) + got[1].astype(F32)
    for copy in copies:
        copy.wait_send()
    return own


def block_gather(blocks, use, sems):
    near, far, _ = partners()
    size = blocks.shape[0] // 4
    half = size // 2
    copies = [
        remote(blocks.at[pl.ds(0, size)], blocks.at[pl.ds(size, size)], sems, 0, near),
        remote(blocks.at[pl.ds(0, size)], blocks.at[pl.ds(2 * size, size)], sems, 1, far),
        remote(
            blocks.at[pl.ds(2 * size, half)], blocks.at[pl.ds(3 * size, half)], sems, 2, near
        ),
        remote(
            blocks.at[pl.ds(size + half, half)],
            blocks.at[pl.ds(3 * size + half, half)],
            sems,
            3,
            far,
        ),
    ]
    copies[0].start()
    copies[1].start()
    use(0)
    copies[1].wait_recv()
    copies[2].start()
    copies[0].wait_recv()
    copies[3].start()
    use(1)
    use(2)
    copies[2].wait_recv()
    copies[3].wait_recv()
    use(3)
    for copy in copies:
        copy.wait_send()


def pair_sums(first, second, stats, sems, k):
    _, _, other = partners()
    lane = lax.broadcasted_iota(jnp.int32, stats.shape[1:], 1)
    stats[0] = jnp.where(lane == 0, first, jnp.where(lane == 1, second, 0.0))
    copy = remote(stats.at[0], stats.at[1], sems, k, other)
    copy.start()
    copy.wait()
    both = stats[0] + stats[1]
    return both[:, 0:1], both[:, 1:2]


def scale_rows(values, stats, sems, k):
    total, squares = pair_sums(
        jnp.sum(values, 1, keepdims=True), jnp.sum(values * values, 1, keepdims=True), stats, sems, k
    )
    center = total / D
    inverse = lax.rsqrt(squares / D - center * center + EPSILON)
    return (values - center) * inverse, inverse


def project_kernel(
    x_in, gain, shift, weight, full_out, proj_out, scaled_out, inverse_out,
    loaded, sent, got, stats, load_sem, gather_sems, sems,
):
    near, far, other = partners()
    row = lax.axis_index("row")
    size = x_in.shape[0]
    kinds, _, width = weight.shape
    half = width // 2
    load = pltpu.make_async_copy(weight, loaded, load_sem)
    load.start()
    meet((near, far, other))
    scaled, inverse = scale_rows(x_in[...].astype(F32), stats, sems, 0)
    scaled_out[...] = scaled
    inverse_out[...] = jnp.broadcast_to(inverse, inverse_out.shape)
    full_out[pl.ds(0, size)] = (scaled * gain[...] + shift[...]).astype(BF16)
    mine = pl.ds(pl.multiple_of(row * half, half), half)
    theirs = pl.ds(pl.multiple_of((1 - row) * half, half), half)
    swaps = [
        remote(
            sent.at[pl.ds(b * size, size)], got.at[pl.ds(b * size, size)], sems, 1 + b, other
        )
        for b in range(4)
    ]

    def finish(b):
        at = pl.ds(b * size, size)
        swaps[b].wait_recv()
        proj_out[at] += got[at]

    def use(b):
        at = pl.ds(b * size, size)
        if b == 0:
            load.wait()
        values = full_out[at]
        for k in range(kinds):
            sent[at, k * half : (k + 1) * half] = dot(values, loaded[k, :, theirs])
        swaps[b].start()
        for k in range(kinds):
            proj_out[at, k * half : (k + 1) * half] = dot(values, loaded[k, :, mine])
        if b == 3:
            for done in range(4):
                finish(done)

    block_gather(full_out, use, gather_sems)
    for swap in swaps:
        swap.wait_send()


def project(x, gain, shift, weight):
    size, width = x.shape
    kinds, _, columns = weight.shape
    piece = kinds * columns // 2
    vmem = pl.BlockSpec(memory_space=pltpu.VMEM)
    return pl.pallas_call(
        project_kernel,
        in_specs=[vmem, vmem, vmem, pl.BlockSpec(memory_space=pl.ANY)],
        out_specs=[vmem] * 4,
        out_shape=[
            jax.ShapeDtypeStruct((4 * size, width), BF16),
            jax.ShapeDtypeStruct((4 * size, piece), F32),
            jax.ShapeDtypeStruct((size, width), F32),
            jax.ShapeDtypeStruct((size, LANES), F32),
        ],
        scratch_shapes=[
            pltpu.VMEM(weight.shape, BF16),
            pltpu.VMEM((4 * size, piece), F32),
            pltpu.VMEM((4 * size, piece), F32),
            pltpu.VMEM((2, size, LANES), F32),
            pltpu.SemaphoreType.DMA,
            remote_sems(4),
            remote_sems(5),
        ],
        compiler_params=pltpu.CompilerParams(
            collective_id=2, has_side_effects=True, vmem_limit_bytes=60 << 20
        ),
        name="project",
    )(x, gain, shift, weight)


def hidden_kernel(
    attended, mixing, x_in, gain, shift, gating_hbm, upstream_hbm, lowering_hbm,
    middle_out, scaled_out, inverse_out, full_out, hidden_out, gate_out, up_out,
    gate_w, up_w, upstream, lowering, attended_got, back_sent, back_got, back, stats,
    gates_sent, gates_got, gates_kept,
    s_sent, s_passed, s_got, s_kept, s_sems, load_sems, gather_sems, sems,
):
    near, far, other = partners()
    row = lax.axis_index("row")
    size = x_in.shape[0]
    part = size // 2
    depth = attended.shape[1]
    units = gate_w.shape[1]
    loads = [
        pltpu.make_async_copy(source, target, load_sems.at[k])
        for k, (source, target) in enumerate(
            (
                (upstream_hbm, upstream),
                (lowering_hbm, lowering),
                (gating_hbm.at[0], gate_w),
                (gating_hbm.at[1], up_w),
            )
        )
    ]
    for load in loads:
        load.start()
    meet((near, far, other))
    swap = remote(attended, attended_got, sems, 0, other)
    swap.start()

    def rows_of(b, whose):
        return pl.ds(pl.multiple_of(b * size + whose * part, part), part)

    back_swap = remote(back_sent, back_got, sems, 1, other)
    swap.wait_recv()
    mine = pl.ds(pl.multiple_of(row * depth, depth), depth)
    theirs = pl.ds(pl.multiple_of((1 - row) * depth, depth), depth)

    def part_of(b):
        at = pl.ds(b * size, size)
        return dot(attended[at], mixing[mine]) + dot(attended_got[at], mixing[theirs])

    def filler():
        loads[0].wait()
        loads[1].wait()
        for b in range(4):
            back_sent[pl.ds(b * part, part)] = dot_t(
                upstream[rows_of(b, 1 - row)], lowering[...], BF16
            )
        back_swap.start()
        back_swap.wait_recv()
        for b in range(4):
            at = pl.ds(b * part, part)
            back[at] = dot_t(upstream[rows_of(b, row)], lowering[...]) + back_got[at].astype(F32)
        loads[2].wait()
        loads[3].wait()

    middle = x_in[...].astype(F32) + block_sum(
        part_of, filler, s_sent, s_passed, s_got, s_kept, s_sems
    )
    middle_out[...] = middle
    scaled, inverse = scale_rows(middle, stats, sems, 2)
    scaled_out[...] = scaled
    inverse_out[...] = jnp.broadcast_to(inverse, inverse_out.shape)
    full_out[pl.ds(0, size)] = (scaled * gain[...] + shift[...]).astype(BF16)
    gate_swaps = [remote(gates_sent.at[b], gates_got.at[b], sems, 3 + b, other) for b in range(4)]

    def returns(b):
        at = rows_of(b, row)
        return [
            remote(ref.at[at], ref.at[at], sems, 7 + 3 * b + k, other)
            for k, ref in enumerate((gate_out, up_out, hidden_out))
        ]

    def finish(b):
        gate_swaps[b].wait_recv()
        gate = gates_kept[b % 2, :, :units] + gates_got[b, :, :units].astype(F32)
        up = gates_kept[b % 2, :, units:] + gates_got[b, :, units:].astype(F32)
        grad = back[pl.ds(b * part, part)]
        sigmoid = jax.nn.sigmoid(gate)
        at = rows_of(b, row)
        gate_out[at] = (grad * up * sigmoid * (1.0 + gate * (1.0 - sigmoid))).astype(BF16)
        up_out[at] = (grad * gate * sigmoid).astype(BF16)
        hidden_out[at] = (gate * sigmoid * up).astype(BF16)
        for copy in returns(b):
            copy.start()

    def use(b):
        values = full_out[rows_of(b, 1 - row)]
        gates_sent[b, :, :units] = dot(values, gate_w[...], BF16)
        gates_sent[b, :, units:] = dot(values, up_w[...], BF16)
        gate_swaps[b].start()
        values = full_out[rows_of(b, row)]
        gates_kept[b % 2, :, :units] = dot(values, gate_w[...])
        gates_kept[b % 2, :, units:] = dot(values, up_w[...])
        finish(b)

    block_gather(full_out, use, gather_sems)
    swap.wait_send()
    back_swap.wait_send()
    for b in range(4):
        gate_swaps[b].wait_send()
        at = rows_of(b, 1 - row)
        for copy in returns(b):
            copy.wait_send()
        for k, ref in enumerate((gate_out, up_out, hidden_out)):
            remote(ref.at[at], ref.at[at], sems, 7 + 3 * b + k, other).wait_recv()


def hidden_units(attended, mixing, x, gain, shift, gating, upstream, lowering):
    size, width = x.shape
    tokens = 4 * size
    units = gating.shape[2]
    part = size // 2
    vmem = pl.BlockSpec(memory_space=pltpu.VMEM)
    anywhere = pl.BlockSpec(memory_space=pl.ANY)
    return pl.pallas_call(
        hidden_kernel,
        in_specs=[vmem] * 5 + [anywhere] * 3,
        out_specs=[vmem] * 7,
        out_shape=[
            jax.ShapeDtypeStruct((size, width), F32),
            jax.ShapeDtypeStruct((size, width), F32),
            jax.ShapeDtypeStruct((size, LANES), F32),
            jax.ShapeDtypeStruct((tokens, width), BF16),
        ]
        + [jax.ShapeDtypeStruct((tokens, units), BF16)] * 3,
        scratch_shapes=[
            pltpu.VMEM(gating.shape[1:], BF16),
            pltpu.VMEM(gating.shape[1:], BF16),
            pltpu.VMEM(upstream.shape, BF16),
            pltpu.VMEM(lowering.shape, BF16),
            pltpu.VMEM(attended.shape, BF16),
            pltpu.VMEM((tokens // 2, units), BF16),
            pltpu.VMEM((tokens // 2, units), BF16),
            pltpu.VMEM((tokens // 2, units), F32),
            pltpu.VMEM((2, size, LANES), F32),
            pltpu.VMEM((4, part, 2 * units), BF16),
            pltpu.VMEM((4, part, 2 * units), BF16),
            pltpu.VMEM((2, part, 2 * units), F32),
            *sum_scratch(size, width),
            pltpu.SemaphoreType.DMA((4,)),
            remote_sems(4),
            remote_sems(19),
        ],
        compiler_params=pltpu.CompilerParams(
            collective_id=3, has_side_effects=True, vmem_limit_bytes=61 << 20
        ),
        name="hidden_units",
    )(attended, mixing, x, gain, shift, gating, upstream, lowering)


def local(
    block_input,
    segment_ids,
    positions,
    attention_gain,
    attention_shift,
    projection_weight,
    projection_bias,
    mixing_weight,
    feedforward_gain,
    feedforward_shift,
    gating_weight,
    lowering_weight,
    cotangent,
):
    own_tokens, local_width = block_input.shape
    seq_here, seq_len = segment_ids.shape
    tokens = seq_here * seq_len
    row = lax.axis_index("row")
    col = lax.axis_index("col")
    cols = lax.axis_size("col")
    tie = lax.optimization_barrier

    def mine(values, axis):
        size = values.shape[axis] // 2
        return lax.dynamic_slice_in_dim(values, row * size, size, axis)

    def theirs(values, axis):
        size = values.shape[axis] // 2
        return lax.dynamic_slice_in_dim(values, (1 - row) * size, size, axis)

    def both(values, axis):
        other = row_swap(values)
        return jnp.concatenate(
            [jnp.where(row == 0, values, other), jnp.where(row == 0, other, values)], axis
        )

    def reorder(table):
        blocks = table.reshape(cols, own_tokens)
        return jnp.take(blocks, col ^ jnp.arange(cols), axis=0).reshape(-1)

    position = reorder(positions)
    tables = rotary_tables(position, HD) + [position[:, None]]

    gating_pair = jnp.swapaxes(gating_weight, 0, 1)
    bias = mine(projection_bias, 1).reshape(1, -1)
    normed_full, projected, scaled_one, inverse_one = project(
        block_input,
        attention_gain[None],
        attention_shift[None],
        jnp.swapaxes(projection_weight, 0, 1),
    )
    inverse_one = inverse_one[:, :1]
    gate_weight, up_weight = gating_pair[0], gating_pair[1]
    queries, keys, values, attended, total_log, upstream_full = attend(
        projected, bias, tables, cotangent, seq_here, seq_len
    )
    middle, scaled_two, inverse_two, normed_two_full, hidden_full, gate_back, up_back = (
        hidden_units(
            attended,
            mixing_weight,
            block_input,
            feedforward_gain[None],
            feedforward_shift[None],
            gating_pair,
            upstream_full,
            lowering_weight,
        )
    )
    inverse_two = inverse_two[:, :1]
    attended_full = both(attended, 1)

    parts = (t_dot(normed_two_full, gate_back, BF16), t_dot(normed_two_full, up_back, BF16))
    gate_back, up_back, parts = tie((gate_back, up_back, parts))
    gating_sums = lax.psum(parts, "dp")

    normed_two_grad = sum_tokens(dot_t(gate_back, gate_weight) + dot_t(up_back, up_weight))
    middle_grad = cotangent.astype(jnp.float32) + norm_back(
        normed_two_grad, feedforward_gain, scaled_two, inverse_two
    )
    middle_wire = middle_grad.astype(jnp.bfloat16)
    middle_full = gather_tokens(middle_wire)
    attended_sent = row_swap(dot_t(middle_full, theirs(mixing_weight, 0), BF16))
    attended_grad = dot_t(middle_full, mine(mixing_weight, 0)) + attended_sent.astype(F32)
    grads = attend_back(
        queries, keys, values, attended, attended_grad.astype(BF16), total_log, tables,
        seq_here, seq_len,
    )
    backs = [both(grad, 1) for grad in grads]
    projection_bgrad = jnp.concatenate([jnp.sum(back, 0, dtype=F32) for back in backs])
    normed_one_grad = sum_tokens(
        sum(dot_t(back, projection_weight[:, i]) for i, back in enumerate(backs))
    )
    input_grad = (
        middle_grad + norm_back(normed_one_grad, attention_gain, scaled_one, inverse_one)
    ).astype(jnp.bfloat16)
    block_output = (middle + sum_tokens(dot(hidden_full, lowering_weight))).astype(jnp.bfloat16)

    sums = jnp.concatenate(
        [
            jnp.sum(normed_one_grad * scaled_one, 0),
            jnp.sum(normed_one_grad, 0),
            jnp.sum(normed_two_grad * scaled_two, 0),
            jnp.sum(normed_two_grad, 0),
        ]
    )
    bit = 1
    while bit < cols:
        sums = sums + col_swap(sums, bit)
        bit *= 2
    small = jnp.concatenate([sums, projection_bgrad])
    lanes = 128
    unit = 8 * lanes
    small = jnp.pad(small, (0, -small.shape[0] % unit)).reshape(-1, lanes)

    totals = line_sum(
        [
            t_dot(hidden_full, upstream_full, BF16),
            t_dot(attended_full, middle_full, BF16),
            *(t_dot(normed_full, back, BF16) for back in backs),
            small,
        ],
        [8, 4, 4, 4, 4, 1],
    )
    lowering_wgrad, mixing_wgrad = totals[0], totals[1]
    sums = totals[5].reshape(-1)
    projection_bgrad = sums[4 * local_width : 4 * local_width + projection_bgrad.shape[0]]
    return (
        block_output,
        input_grad,
        sums[:local_width],
        sums[local_width : 2 * local_width],
        jnp.stack(totals[2:5], 1).astype(F32),
        projection_bgrad.reshape(3, -1),
        mixing_wgrad.astype(F32),
        sums[2 * local_width : 3 * local_width],
        sums[3 * local_width : 4 * local_width],
        tie(jnp.stack(gating_sums, 1)).astype(F32),
        lowering_wgrad.astype(F32),
    )


def solution(mesh):
    return jax.shard_map(
        local,
        mesh=mesh,
        in_specs=(
            P(("dp", "col"), "row"),
            P("dp", None),
            P("dp", None),
            P("row"),
            P("row"),
            P("row", None, "col"),
            P(None, "col"),
            P("col", "row"),
            P("row"),
            P("row"),
            P("row", None, "col"),
            P("col", "row"),
            P(("dp", "col"), "row"),
        ),
        out_specs=(
            P(("dp", "col"), "row"),
            P(("dp", "col"), "row"),
            P("row"),
            P("row"),
            P("row", None, "col"),
            P(None, "col"),
            P("col", "row"),
            P("row"),
            P("row"),
            P("row", None, "col"),
            P("col", "row"),
        ),
        check_vma=False,
    )
```

```python
import functools
import math

import jax
import jax.numpy as jnp
from jax import lax
from jax.experimental import pallas as pl
from jax.experimental.pallas import tpu as pltpu
from jax.sharding import PartitionSpec as P

D = 2048
HD = 64


EPSILON = 1e-05
MASKED = -1e30
WINDOW = 2
LANES = 128
BF16 = jnp.bfloat16
F32 = jnp.float32


def col_swap(values, bit):
    count = lax.axis_size("col")
    return lax.ppermute(values, "col", [(i, i ^ bit) for i in range(count)])


def row_swap(values):
    return lax.ppermute(values, "row", [(0, 1), (1, 0)])


def gather_tokens(values):
    count = lax.axis_size("col")
    if count == 4:
        half = values.shape[0] // 2
        first = col_swap(values, 1)
        second = col_swap(values, 2)
        third_a = col_swap(second[:half], 1)
        third_b = col_swap(first[half:], 2)
        return jnp.concatenate([values, first, second, third_a, third_b], 0)
    bit = 1
    while bit < count:
        values = jnp.concatenate([values, col_swap(values, bit)], 0)
        bit *= 2
    return values


def sum_tokens(partial_rows):
    count = lax.axis_size("col")
    size = partial_rows.shape[0] // count
    if count == 4:
        half = size // 2
        own, first, second, third = (partial_rows[i * size : (i + 1) * size] for i in range(4))
        third = third.astype(BF16)
        got_a = col_swap(third[:half], 1).astype(F32)
        got_b = col_swap(third[half:], 2).astype(F32)
        to_second = jnp.concatenate([second[:half] + got_a, second[half:]], 0).astype(BF16)
        to_first = jnp.concatenate([first[:half], first[half:] + got_b], 0).astype(BF16)
        return own + col_swap(to_first, 1).astype(F32) + col_swap(to_second, 2).astype(F32)
    bit = count // 2
    while bit:
        kept = partial_rows.shape[0] // 2
        got = col_swap(partial_rows[kept:].astype(BF16), bit).astype(F32)
        partial_rows = partial_rows[:kept] + got
        bit //= 2
    return partial_rows


def row_sums(first, second):
    return lax.psum((first, second), "row")


def normalize(values):
    total, squares = row_sums(
        jnp.sum(values, 1, keepdims=True), jnp.sum(values * values, 1, keepdims=True)
    )
    center = total / D
    spread = squares / D - center * center
    inverse = lax.rsqrt(spread + EPSILON)
    return ((values - center) * inverse, inverse)


def norm_back(upstream, gain, scaled, inverse):
    weighted = upstream * gain
    total, mixed = row_sums(
        jnp.sum(weighted, 1, keepdims=True), jnp.sum(weighted * scaled, 1, keepdims=True)
    )
    return inverse * (weighted - total / D - scaled * (mixed / D))


def dot(a, b, kind=F32):
    return jnp.dot(a, b, preferred_element_type=F32).astype(kind)


def dot_t(a, b, kind=F32):
    return lax.dot_general(a, b, (((1,), (1,)), ((), ())), preferred_element_type=F32).astype(kind)


def t_dot(a, b, kind=F32):
    return lax.dot_general(a, b, (((0,), (0,)), ((), ())), preferred_element_type=F32).astype(kind)


def line_kernel(pieces, kinds, *refs):
    count = len(kinds)
    own, out = refs[:count], refs[count : 2 * count]
    inwards, part, across = (refs[(2 + k) * count : (3 + k) * count] for k in range(3))
    sent_in, got_in, got_across, sent_out, got_out = refs[5 * count :]
    size = lax.axis_size("dp")
    me = lax.axis_index("dp")
    half = size // 2
    low = me < half
    inner = jnp.where(low, me + 1, me - 1)
    outer = jnp.where(low, jnp.maximum(me - 1, 0), jnp.minimum(me + 1, size - 1))
    end = (me == 0) | (me == size - 1)
    middle = (me == half - 1) | (me == half)

    barrier = pltpu.get_barrier_semaphore()
    pl.semaphore_signal(
        barrier, inc=1, device_id={"dp": inner}, device_id_type=pl.DeviceIdType.MESH
    )

    @pl.when(jnp.logical_not(end))
    def _():
        pl.semaphore_signal(
            barrier, inc=1, device_id={"dp": outer}, device_id_type=pl.DeviceIdType.MESH
        )
        pl.semaphore_wait(barrier, 2)

    @pl.when(end)
    def _():
        pl.semaphore_wait(barrier, 1)

    def copy(source, target, sent, got, to):
        return pltpu.make_async_remote_copy(
            src_ref=source,
            dst_ref=target,
            send_sem=sent,
            recv_sem=got,
            device_id={"dp": to},
            device_id_type=pl.DeviceIdType.MESH,
        )

    def to_inner(k):
        a, start, rows = pieces[k]
        at = pl.ds(start, rows)
        return copy(own[a].at[at], inwards[a].at[at], sent_in.at[k], got_in.at[k], inner)

    def part_to_inner(k):
        a, start, rows = pieces[k]
        at = pl.ds(start, rows)
        return copy(part[a].at[at], inwards[a].at[at], sent_in.at[k], got_in.at[k], inner)

    def part_across(k):
        a, start, rows = pieces[k]
        at = pl.ds(start, rows)
        return copy(part[a].at[at], across[a].at[at], sent_in.at[k], got_across.at[k], inner)

    def to_outer(k):
        a, start, rows = pieces[k]
        at = pl.ds(start, rows)
        return copy(out[a].at[at], out[a].at[at], sent_out.at[k], got_out.at[k], outer)

    def add(first, second, target, k):
        a, start, rows = pieces[k]
        at = pl.ds(start, rows)
        target[a][at] = (
            first[a][at].astype(F32) + second[a][at].astype(F32)
        ).astype(kinds[a])

    total = len(pieces)

    @pl.when(end)
    def _():
        for k in range(total):
            if k >= WINDOW:
                to_inner(k - WINDOW).wait_send()
            to_inner(k).start()
        for k in range(max(total - WINDOW, 0), total):
            to_inner(k).wait_send()
        for k in range(total):
            to_outer(k).wait_recv()

    def inward(k):
        to_inner(k).wait_recv()
        add(own, inwards, part, k)

        @pl.when(middle)
        def _():
            part_across(k).start()

        @pl.when(jnp.logical_not(middle))
        def _():
            part_to_inner(k).start()

    def outward(k):
        @pl.when(middle)
        def _():
            part_across(k).wait_recv()
            add(part, across, out, k)
            to_outer(k).start()

        @pl.when(jnp.logical_not(middle))
        def _():
            to_outer(k).wait_recv()
            to_outer(k).start()

    @pl.when(jnp.logical_not(end))
    def _():
        for k in range(total + 1):
            if k < total:
                inward(k)
            if k:
                outward(k - 1)
        for k in range(total):
            part_across(k).wait_send()
            to_outer(k).wait_send()


def line_sum(arrays, splits):
    pieces = []
    for a, (array, split) in enumerate(zip(arrays, splits)):
        rows = array.shape[0] // split
        pieces += [(a, i * rows, rows) for i in range(split)]
    kinds = [array.dtype for array in arrays]
    vmem = pl.BlockSpec(memory_space=pltpu.VMEM)
    scratch = [pltpu.VMEM(array.shape, array.dtype) for array in arrays]
    sems = [pltpu.SemaphoreType.DMA((len(pieces),)) for _ in range(5)]
    return pl.pallas_call(
        functools.partial(line_kernel, pieces, kinds),
        out_shape=[jax.ShapeDtypeStruct(array.shape, array.dtype) for array in arrays],
        in_specs=[vmem] * len(arrays),
        out_specs=[vmem] * len(arrays),
        scratch_shapes=scratch * 3 + sems,
        compiler_params=pltpu.CompilerParams(
            collective_id=1, has_side_effects=True, vmem_limit_bytes=60 << 20
        ),
        name="line_sum",
    )(*arrays)


def rotary_tables(positions, head_size):
    half = head_size // 8
    lane = jnp.arange(2 * head_size) % head_size
    freq = jnp.exp((lane % half).astype(F32) * (-math.log(10000.0) / half))
    theta = positions.reshape(-1).astype(jnp.float32)[:, None] * freq
    first, second = lane < half, (lane >= half) & (lane < 2 * half)
    sine = jnp.sin(theta)
    return [
        jnp.where(first | second, jnp.cos(theta), 1.0),
        jnp.where(first, -sine, 0.0),
        jnp.where(second, sine, 0.0),
    ]


def scores_of(queries, keys, allowed):
    scores = lax.dot_general(
        queries, keys, (((1,), (1,)), ((), ())), preferred_element_type=F32
    ) * (1.0 / math.sqrt(HD))
    return jnp.where(allowed, scores, MASKED)


def allowed_of(position):
    length = position.shape[0]
    cols = lax.axis_size("col")
    col = lax.axis_index("col")
    own = length * pl.num_programs(0) // cols

    def order_of(axis):
        shape = (length, 1) if axis == 0 else (1, length)
        index = lax.broadcasted_iota(jnp.int32, shape, axis)
        order = jnp.zeros(shape, jnp.int32)
        for k in range(length // own):
            block = pl.program_id(0) * (length // own) + k
            block = 2 * lax.rem(lax.div(col, 2) + lax.div(block, 2), 2) + lax.rem(col + block, 2)
            start = lax.rem(block * own, length)
            order = jnp.where(index >= k * own, start + index - k * own, order)
        return order

    order_q, order_k = order_of(0), order_of(1)
    return (order_k <= order_q) & (order_k >= order_q - position[...])


def attend_kernel(
    q_in, k_in, v_in, q_bias, k_bias, v_bias, same, above, below, position, near_hbm,
    q_out, k_out, v_out, attended_out, total_out, blocks_out, blocks, load_sem, sems,
):
    step = HD // 8
    wide = q_in.shape[1]

    near, far, _ = partners()
    size = blocks.shape[0] // 4
    part = size // 2
    copies = [
        remote(blocks.at[pl.ds(2 * size, part)], blocks.at[pl.ds(3 * size, part)], sems, 0, near),
        remote(
            blocks.at[pl.ds(size + part, part)],
            blocks.at[pl.ds(3 * size + part, part)],
            sems,
            1,
            far,
        ),
    ]
    at_end = (pl.program_id(0) == pl.num_programs(0) - 1) & (
        pl.program_id(1) == pl.num_programs(1) - 1
    )

    @pl.when((pl.program_id(0) == 0) & (pl.program_id(1) == 0))
    def _():
        load = pltpu.make_async_copy(near_hbm, blocks.at[pl.ds(0, 3 * size)], load_sem)
        load.start()
        meet((near, far))
        load.wait()
        for copy in copies:
            copy.start()

    def rotate(values):
        return (
            values * same[...]
            + pltpu.roll(values, wide - step, 1) * above[...]
            + pltpu.roll(values, step, 1) * below[...]
        )

    queries = rotate(q_in[...] + q_bias[...]).astype(BF16)
    keys = rotate(k_in[...] + k_bias[...]).astype(BF16)
    values = (v_in[...] + v_bias[...]).astype(BF16)
    q_out[...] = queries
    k_out[...] = keys
    v_out[...] = values
    allowed = allowed_of(position)
    results, totals = [], []
    for h in range(wide // HD):
        at = slice(h * HD, (h + 1) * HD)
        scores = scores_of(queries[:, at], keys[:, at], allowed)
        peak = jnp.max(scores, -1, keepdims=True)
        raised = jnp.exp(scores - peak)
        denominator = jnp.sum(raised, -1, keepdims=True)
        probs = (raised / denominator).astype(BF16)
        results.append(jnp.dot(probs, values[:, at], preferred_element_type=F32))
        totals.append(peak + jnp.log(denominator))
    attended_out[...] = jnp.concatenate(results, 1).astype(BF16)
    total_out[0] = jnp.concatenate(totals, 1)

    @pl.when(at_end)
    def _():
        for copy in copies:
            copy.wait()
        blocks_out[...] = blocks[...]


def attend_back_kernel(
    q_in, k_in, v_in, attended_in, grad_in, total_in, same, above, below, position, q_out, k_out, v_out,
):
    step = HD // 8
    wide = q_in.shape[1]

    def rotate_back(grads):
        return (
            grads * same[...]
            + pltpu.roll(grads * above[...], step, 1)
            + pltpu.roll(grads * below[...], wide - step, 1)
        )

    allowed = allowed_of(position)
    products = grad_in[...].astype(F32) * attended_in[...].astype(F32)
    q_grads, k_grads, v_grads = [], [], []
    for h in range(wide // HD):
        at = slice(h * HD, (h + 1) * HD)
        queries, keys, values = q_in[:, at], k_in[:, at], v_in[:, at]
        grad = grad_in[:, at]
        recovered = jnp.exp(scores_of(queries, keys, allowed) - total_in[0][:, h : h + 1])
        prob_grad = lax.dot_general(
            grad, values, (((1,), (1,)), ((), ())), preferred_element_type=F32
        )
        row_dot = jnp.sum(products[:, at], 1, keepdims=True)
        score_grad = (recovered * (prob_grad - row_dot) * (1.0 / math.sqrt(HD))).astype(BF16)
        q_grads.append(jnp.dot(score_grad, keys, preferred_element_type=F32))
        k_grads.append(t_dot(score_grad, queries))
        v_grads.append(t_dot(recovered.astype(BF16), grad))
    q_out[...] = rotate_back(jnp.concatenate(q_grads, 1)).astype(BF16)
    k_out[...] = rotate_back(jnp.concatenate(k_grads, 1)).astype(BF16)
    v_out[...] = jnp.concatenate(v_grads, 1).astype(BF16)


def attention_specs(tables, seq_len, wide):
    block = pl.BlockSpec((seq_len, wide), lambda s, p: (s, p))
    table = pl.BlockSpec((seq_len, wide), lambda s, p: (s, 0))
    tall = pl.BlockSpec((seq_len, 1), lambda s, p: (s, 0))
    total = pl.BlockSpec((1, seq_len, wide // HD), lambda s, p: (p, s, 0))
    return block, [table] * 3 + [tall], total


def attend(projected, bias, tables, nearby, seq_here, seq_len):
    tokens, piece = projected.shape[0], projected.shape[1] // 3
    wide = 2 * HD
    pairs = piece // wide
    block, extra, total = attention_specs(tables, seq_len, wide)
    shifted = [
        pl.BlockSpec((seq_len, wide), functools.partial(lambda k, s, p: (s, p + k * pairs), k))
        for k in range(3)
    ]
    biases = [
        pl.BlockSpec((1, wide), functools.partial(lambda k, s, p: (0, p + k * pairs), k))
        for k in range(3)
    ]
    whole = jax.ShapeDtypeStruct((tokens, piece), BF16)
    return pl.pallas_call(
        attend_kernel,
        grid=(seq_here, pairs),
        in_specs=shifted + biases + extra + [pl.BlockSpec(memory_space=pl.ANY)],
        out_specs=[block] * 4 + [total, pl.BlockSpec((tokens, nearby.shape[1]), lambda s, p: (0, 0))],
        out_shape=[whole] * 4
        + [
            jax.ShapeDtypeStruct((pairs, tokens, wide // HD), F32),
            jax.ShapeDtypeStruct((tokens, nearby.shape[1]), BF16),
        ],
        scratch_shapes=[
            pltpu.VMEM((tokens, nearby.shape[1]), BF16),
            pltpu.SemaphoreType.DMA,
            remote_sems(2),
        ],
        compiler_params=pltpu.CompilerParams(
            collective_id=4, has_side_effects=True, vmem_limit_bytes=61 << 20
        ),
        cost_estimate=pl.CostEstimate(
            flops=4 * tokens * seq_len * piece, bytes_accessed=20 * tokens * piece,
            transcendentals=tokens * seq_len * piece // HD,
        ),
        name="attend",
    )(projected, projected, projected, bias, bias, bias, *tables, nearby)


def attend_back(queries, keys, values, attended, grad, total_log, tables, seq_here, seq_len):
    tokens, piece = queries.shape
    wide = 2 * HD
    pairs = piece // wide
    block, extra, total = attention_specs(tables, seq_len, wide)
    whole = jax.ShapeDtypeStruct((tokens, piece), BF16)
    return pl.pallas_call(
        attend_back_kernel,
        grid=(seq_here, pairs),
        in_specs=[block] * 5 + [total] + extra,
        out_specs=[block] * 3,
        out_shape=[whole] * 3,
        cost_estimate=pl.CostEstimate(
            flops=10 * tokens * seq_len * piece, bytes_accessed=20 * tokens * piece,
            transcendentals=tokens * seq_len * piece // HD,
        ),
        name="attend_back",
    )(queries, keys, values, attended, grad, total_log, *tables)


MESH = pl.DeviceIdType.MESH


def partners():
    col = lax.axis_index("col")
    cols = lax.axis_size("col")
    across = lax.rem(col + cols // 2, cols)
    return {"col": col + 1 - 2 * lax.rem(col, 2)}, {"col": across}, {"row": 1 - lax.axis_index("row")}


def meet(devices):
    barrier = pltpu.get_barrier_semaphore()
    for device in devices:
        pl.semaphore_signal(barrier, inc=1, device_id=device, device_id_type=MESH)
    pl.semaphore_wait(barrier, len(devices))


def remote(source, target, sems, k, device):
    return pltpu.make_async_remote_copy(
        src_ref=source,
        dst_ref=target,
        send_sem=sems.at[0, k],
        recv_sem=sems.at[1, k],
        device_id=device,
        device_id_type=MESH,
    )


def remote_sems(count):
    return pltpu.SemaphoreType.DMA((2, count))


def sum_scratch(size, width):
    half = size // 2
    return [
        pltpu.VMEM((3, size, width), BF16),
        pltpu.VMEM((2, half, width), BF16),
        pltpu.VMEM((2, size, width), BF16),
        pltpu.VMEM((2, half, width), F32),
        remote_sems(6),
    ]


def block_sum(part_of, filler, sent, passed, got, kept, sems):
    near, far, _ = partners()
    size = sent.shape[1]
    half = size // 2
    low, high = pl.ds(0, half), pl.ds(half, half)
    copies = [
        remote(sent.at[2, low], passed.at[0], sems, 0, near),
        remote(sent.at[2, high], passed.at[1], sems, 1, far),
        remote(sent.at[0, low], got.at[0, low], sems, 2, near),
        remote(sent.at[1, high], got.at[1, high], sems, 3, far),
        remote(sent.at[1, low], got.at[1, low], sems, 4, far),
        remote(sent.at[0, high], got.at[0, high], sems, 5, near),
    ]
    sent[2] = part_of(3).astype(BF16)
    copies[0].start()
    copies[1].start()
    part = part_of(1)
    sent[0, low] = part[:half].astype(BF16)
    copies[2].start()
    kept[0] = part[half:]
    part = part_of(2)
    sent[1, high] = part[half:].astype(BF16)
    copies[3].start()
    kept[1] = part[:half]
    copies[0].wait_recv()
    sent[1, low] = (kept[1] + passed[0].astype(F32)).astype(BF16)
    copies[4].start()
    copies[1].wait_recv()
    sent[0, high] = (kept[0] + passed[1].astype(F32)).astype(BF16)
    copies[5].start()
    own = part_of(0)
    filler()
    for copy in copies[2:]:
        copy.wait_recv()
    own = own + got[0].astype(F32) + got[1].astype(F32)
    for copy in copies:
        copy.wait_send()
    return own


def block_gather(blocks, use, sems):
    near, far, _ = partners()
    size = blocks.shape[0] // 4
    half = size // 2
    copies = [
        remote(blocks.at[pl.ds(0, size)], blocks.at[pl.ds(size, size)], sems, 0, near),
        remote(blocks.at[pl.ds(0, size)], blocks.at[pl.ds(2 * size, size)], sems, 1, far),
        remote(
            blocks.at[pl.ds(2 * size, half)], blocks.at[pl.ds(3 * size, half)], sems, 2, near
        ),
        remote(
            blocks.at[pl.ds(size + half, half)],
            blocks.at[pl.ds(3 * size + half, half)],
            sems,
            3,
            far,
        ),
    ]
    copies[0].start()
    copies[1].start()
    use(0)
    copies[1].wait_recv()
    copies[2].start()
    copies[0].wait_recv()
    copies[3].start()
    use(1)
    use(2)
    copies[2].wait_recv()
    copies[3].wait_recv()
    use(3)
    for copy in copies:
        copy.wait_send()


def pair_sums(first, second, stats, sems, k):
    _, _, other = partners()
    lane = lax.broadcasted_iota(jnp.int32, stats.shape[1:], 1)
    stats[0] = jnp.where(lane == 0, first, jnp.where(lane == 1, second, 0.0))
    copy = remote(stats.at[0], stats.at[1], sems, k, other)
    copy.start()
    copy.wait()
    both = stats[0] + stats[1]
    return both[:, 0:1], both[:, 1:2]


def scale_rows(values, stats, sems, k):
    total, squares = pair_sums(
        jnp.sum(values, 1, keepdims=True), jnp.sum(values * values, 1, keepdims=True), stats, sems, k
    )
    center = total / D
    inverse = lax.rsqrt(squares / D - center * center + EPSILON)
    return (values - center) * inverse, inverse


def project_kernel(
    x_in, gain, shift, weight, own_hbm, full_out, proj_out, scaled_out, inverse_out, near_out,
    loaded, sent, got, blocks, stats, load_sem, own_sem, gather_sems, sems,
):
    near, far, other = partners()
    row = lax.axis_index("row")
    size = x_in.shape[0]
    kinds, _, width = weight.shape
    half = width // 2
    load = pltpu.make_async_copy(weight, loaded, load_sem)
    load.start()
    own_at = pl.ds(0, size)
    own_load = pltpu.make_async_copy(own_hbm, blocks.at[own_at], own_sem)
    own_load.start()
    hops = [
        remote(blocks.at[own_at], blocks.at[pl.ds(size, size)], sems, 5, near),
        remote(blocks.at[own_at], blocks.at[pl.ds(2 * size, size)], sems, 6, far),
    ]
    meet((near, far, other))
    scaled, inverse = scale_rows(x_in[...].astype(F32), stats, sems, 0)
    scaled_out[...] = scaled
    inverse_out[...] = jnp.broadcast_to(inverse, inverse_out.shape)
    full_out[pl.ds(0, size)] = (scaled * gain[...] + shift[...]).astype(BF16)
    mine = pl.ds(pl.multiple_of(row * half, half), half)
    theirs = pl.ds(pl.multiple_of((1 - row) * half, half), half)
    swaps = [
        remote(
            sent.at[pl.ds(b * size, size)], got.at[pl.ds(b * size, size)], sems, 1 + b, other
        )
        for b in range(4)
    ]

    def finish(b):
        at = pl.ds(b * size, size)
        swaps[b].wait_recv()
        proj_out[at] += got[at]

    def use(b):
        at = pl.ds(b * size, size)
        if b == 0:
            load.wait()
        if b == 1:
            own_load.wait()
            for hop in hops:
                hop.start()
        values = full_out[at]
        for k in range(kinds):
            sent[at, k * half : (k + 1) * half] = dot(values, loaded[k, :, theirs])
        swaps[b].start()
        for k in range(kinds):
            proj_out[at, k * half : (k + 1) * half] = dot(values, loaded[k, :, mine])
        if b == 3:
            for done in range(4):
                finish(done)

    block_gather(full_out, use, gather_sems)
    for swap in swaps:
        swap.wait_send()
    for hop in hops:
        hop.wait()
    near_out[...] = blocks[...]


def project(x, gain, shift, weight, own):
    size, width = x.shape
    kinds, _, columns = weight.shape
    piece = kinds * columns // 2
    vmem = pl.BlockSpec(memory_space=pltpu.VMEM)
    return pl.pallas_call(
        project_kernel,
        in_specs=[vmem] * 3 + [pl.BlockSpec(memory_space=pl.ANY)] * 2,
        out_specs=[vmem] * 5,
        out_shape=[
            jax.ShapeDtypeStruct((4 * size, width), BF16),
            jax.ShapeDtypeStruct((4 * size, piece), F32),
            jax.ShapeDtypeStruct((size, width), F32),
            jax.ShapeDtypeStruct((size, LANES), F32),
            jax.ShapeDtypeStruct((3 * size, width), BF16),
        ],
        scratch_shapes=[
            pltpu.VMEM(weight.shape, BF16),
            pltpu.VMEM((4 * size, piece), F32),
            pltpu.VMEM((4 * size, piece), F32),
            pltpu.VMEM((3 * size, width), BF16),
            pltpu.VMEM((2, size, LANES), F32),
            pltpu.SemaphoreType.DMA,
            pltpu.SemaphoreType.DMA,
            remote_sems(4),
            remote_sems(7),
        ],
        compiler_params=pltpu.CompilerParams(
            collective_id=2, has_side_effects=True, vmem_limit_bytes=60 << 20
        ),
        name="project",
    )(x, gain, shift, weight, own)


def hidden_kernel(
    attended, mixing, x_in, gain, shift, gating_hbm, upstream_hbm, lowering_hbm,
    middle_out, scaled_out, inverse_out, full_out, hidden_out, gate_out, up_out,
    gate_w, up_w, upstream, lowering, attended_got, back_sent, back_got, back, stats,
    gates_sent, gates_got, gates_kept,
    s_sent, s_passed, s_got, s_kept, s_sems, load_sems, gather_sems, sems,
):
    near, far, other = partners()
    row = lax.axis_index("row")
    size = x_in.shape[0]
    part = size // 2
    depth = attended.shape[1]
    units = gate_w.shape[1]
    loads = [
        pltpu.make_async_copy(source, target, load_sems.at[k])
        for k, (source, target) in enumerate(
            (
                (upstream_hbm, upstream),
                (lowering_hbm, lowering),
                (gating_hbm.at[0], gate_w),
                (gating_hbm.at[1], up_w),
            )
        )
    ]
    for load in loads:
        load.start()
    meet((near, far, other))
    swap = remote(attended, attended_got, sems, 0, other)
    swap.start()

    def rows_of(b, whose):
        return pl.ds(pl.multiple_of(b * size + whose * part, part), part)

    back_swap = remote(back_sent, back_got, sems, 1, other)
    swap.wait_recv()
    mine = pl.ds(pl.multiple_of(row * depth, depth), depth)
    theirs = pl.ds(pl.multiple_of((1 - row) * depth, depth), depth)

    def part_of(b):
        at = pl.ds(b * size, size)
        return dot(attended[at], mixing[mine]) + dot(attended_got[at], mixing[theirs])

    def filler():
        loads[0].wait()
        loads[1].wait()
        for b in range(4):
            back_sent[pl.ds(b * part, part)] = dot_t(
                upstream[rows_of(b, 1 - row)], lowering[...], BF16
            )
        back_swap.start()
        back_swap.wait_recv()
        for b in range(4):
            at = pl.ds(b * part, part)
            back[at] = dot_t(upstream[rows_of(b, row)], lowering[...]) + back_got[at].astype(F32)
        loads[2].wait()
        loads[3].wait()

    middle = x_in[...].astype(F32) + block_sum(
        part_of, filler, s_sent, s_passed, s_got, s_kept, s_sems
    )
    middle_out[...] = middle
    scaled, inverse = scale_rows(middle, stats, sems, 2)
    scaled_out[...] = scaled
    inverse_out[...] = jnp.broadcast_to(inverse, inverse_out.shape)
    full_out[pl.ds(0, size)] = (scaled * gain[...] + shift[...]).astype(BF16)
    gate_swaps = [remote(gates_sent.at[b], gates_got.at[b], sems, 3 + b, other) for b in range(4)]

    def returns(b):
        at = rows_of(b, row)
        return [
            remote(ref.at[at], ref.at[at], sems, 7 + 3 * b + k, other)
            for k, ref in enumerate((gate_out, up_out, hidden_out))
        ]

    def finish(b):
        gate_swaps[b].wait_recv()
        gate = gates_kept[b % 2, :, :units] + gates_got[b, :, :units].astype(F32)
        up = gates_kept[b % 2, :, units:] + gates_got[b, :, units:].astype(F32)
        grad = back[pl.ds(b * part, part)]
        sigmoid = jax.nn.sigmoid(gate)
        at = rows_of(b, row)
        gate_out[at] = (grad * up * sigmoid * (1.0 + gate * (1.0 - sigmoid))).astype(BF16)
        up_out[at] = (grad * gate * sigmoid).astype(BF16)
        hidden_out[at] = (gate * sigmoid * up).astype(BF16)
        for copy in returns(b):
            copy.start()

    def use(b):
        values = full_out[rows_of(b, 1 - row)]
        gates_sent[b, :, :units] = dot(values, gate_w[...], BF16)
        gates_sent[b, :, units:] = dot(values, up_w[...], BF16)
        gate_swaps[b].start()
        values = full_out[rows_of(b, row)]
        gates_kept[b % 2, :, :units] = dot(values, gate_w[...])
        gates_kept[b % 2, :, units:] = dot(values, up_w[...])
        finish(b)

    block_gather(full_out, use, gather_sems)
    swap.wait_send()
    back_swap.wait_send()
    for b in range(4):
        gate_swaps[b].wait_send()
        at = rows_of(b, 1 - row)
        for copy in returns(b):
            copy.wait_send()
        for k, ref in enumerate((gate_out, up_out, hidden_out)):
            remote(ref.at[at], ref.at[at], sems, 7 + 3 * b + k, other).wait_recv()


def hidden_units(attended, mixing, x, gain, shift, gating, upstream, lowering):
    size, width = x.shape
    tokens = 4 * size
    units = gating.shape[2]
    part = size // 2
    vmem = pl.BlockSpec(memory_space=pltpu.VMEM)
    anywhere = pl.BlockSpec(memory_space=pl.ANY)
    return pl.pallas_call(
        hidden_kernel,
        in_specs=[vmem] * 5 + [anywhere] * 3,
        out_specs=[vmem] * 7,
        out_shape=[
            jax.ShapeDtypeStruct((size, width), F32),
            jax.ShapeDtypeStruct((size, width), F32),
            jax.ShapeDtypeStruct((size, LANES), F32),
            jax.ShapeDtypeStruct((tokens, width), BF16),
        ]
        + [jax.ShapeDtypeStruct((tokens, units), BF16)] * 3,
        scratch_shapes=[
            pltpu.VMEM(gating.shape[1:], BF16),
            pltpu.VMEM(gating.shape[1:], BF16),
            pltpu.VMEM(upstream.shape, BF16),
            pltpu.VMEM(lowering.shape, BF16),
            pltpu.VMEM(attended.shape, BF16),
            pltpu.VMEM((tokens // 2, units), BF16),
            pltpu.VMEM((tokens // 2, units), BF16),
            pltpu.VMEM((tokens // 2, units), F32),
            pltpu.VMEM((2, size, LANES), F32),
            pltpu.VMEM((4, part, 2 * units), BF16),
            pltpu.VMEM((4, part, 2 * units), BF16),
            pltpu.VMEM((2, part, 2 * units), F32),
            *sum_scratch(size, width),
            pltpu.SemaphoreType.DMA((4,)),
            remote_sems(4),
            remote_sems(19),
        ],
        compiler_params=pltpu.CompilerParams(
            collective_id=3, has_side_effects=True, vmem_limit_bytes=61 << 20
        ),
        name="hidden_units",
    )(attended, mixing, x, gain, shift, gating, upstream, lowering)


def local(
    block_input,
    segment_ids,
    positions,
    attention_gain,
    attention_shift,
    projection_weight,
    projection_bias,
    mixing_weight,
    feedforward_gain,
    feedforward_shift,
    gating_weight,
    lowering_weight,
    cotangent,
):
    own_tokens, local_width = block_input.shape
    seq_here, seq_len = segment_ids.shape
    tokens = seq_here * seq_len
    row = lax.axis_index("row")
    col = lax.axis_index("col")
    cols = lax.axis_size("col")
    tie = lax.optimization_barrier

    def mine(values, axis):
        size = values.shape[axis] // 2
        return lax.dynamic_slice_in_dim(values, row * size, size, axis)

    def theirs(values, axis):
        size = values.shape[axis] // 2
        return lax.dynamic_slice_in_dim(values, (1 - row) * size, size, axis)

    def both(values, axis):
        other = row_swap(values)
        return jnp.concatenate(
            [jnp.where(row == 0, values, other), jnp.where(row == 0, other, values)], axis
        )

    def reorder(table):
        blocks = table.reshape(cols, own_tokens)
        return jnp.take(blocks, col ^ jnp.arange(cols), axis=0).reshape(-1)

    position = reorder(positions)
    tables = rotary_tables(position, HD) + [position[:, None]]

    gating_pair = jnp.swapaxes(gating_weight, 0, 1)
    bias = mine(projection_bias, 1).reshape(1, -1)
    normed_full, projected, scaled_one, inverse_one, nearby = project(
        block_input,
        attention_gain[None],
        attention_shift[None],
        jnp.swapaxes(projection_weight, 0, 1),
        cotangent,
    )
    inverse_one = inverse_one[:, :1]
    gate_weight, up_weight = gating_pair[0], gating_pair[1]
    queries, keys, values, attended, total_log, upstream_full = attend(
        projected, bias, tables, nearby, seq_here, seq_len
    )
    middle, scaled_two, inverse_two, normed_two_full, hidden_full, gate_back, up_back = (
        hidden_units(
            attended,
            mixing_weight,
            block_input,
            feedforward_gain[None],
            feedforward_shift[None],
            gating_pair,
            upstream_full,
            lowering_weight,
        )
    )
    inverse_two = inverse_two[:, :1]
    attended_full = both(attended, 1)

    early = local_width * 11 // 16
    first_rows, last_rows = normed_two_full[:, :early], normed_two_full[:, early:]
    parts = (t_dot(first_rows, gate_back, BF16), t_dot(first_rows, up_back, BF16))
    gate_back, up_back, parts = tie((gate_back, up_back, parts))
    gating_sums = lax.psum(parts, "dp")

    normed_two_grad = sum_tokens(dot_t(gate_back, gate_weight) + dot_t(up_back, up_weight))
    middle_grad = cotangent.astype(jnp.float32) + norm_back(
        normed_two_grad, feedforward_gain, scaled_two, inverse_two
    )
    middle_wire = middle_grad.astype(jnp.bfloat16)
    middle_full = gather_tokens(middle_wire)
    attended_sent = row_swap(dot_t(middle_full, theirs(mixing_weight, 0), BF16))
    attended_grad = dot_t(middle_full, mine(mixing_weight, 0)) + attended_sent.astype(F32)
    grads = attend_back(
        queries, keys, values, attended, attended_grad.astype(BF16), total_log, tables,
        seq_here, seq_len,
    )
    backs = [both(grad, 1) for grad in grads]
    projection_bgrad = jnp.concatenate([jnp.sum(back, 0, dtype=F32) for back in backs])
    normed_one_grad = sum_tokens(
        sum(dot_t(back, projection_weight[:, i]) for i, back in enumerate(backs))
    )
    input_grad = (
        middle_grad + norm_back(normed_one_grad, attention_gain, scaled_one, inverse_one)
    ).astype(jnp.bfloat16)
    block_output = (middle + sum_tokens(dot(hidden_full, lowering_weight))).astype(jnp.bfloat16)

    sums = jnp.concatenate(
        [
            jnp.sum(normed_one_grad * scaled_one, 0),
            jnp.sum(normed_one_grad, 0),
            jnp.sum(normed_two_grad * scaled_two, 0),
            jnp.sum(normed_two_grad, 0),
        ]
    )
    bit = 1
    while bit < cols:
        sums = sums + col_swap(sums, bit)
        bit *= 2
    small = jnp.concatenate([sums, projection_bgrad])
    lanes = 128
    unit = 8 * lanes
    small = jnp.pad(small, (0, -small.shape[0] % unit)).reshape(-1, lanes)

    totals = line_sum(
        [
            t_dot(hidden_full, upstream_full, BF16),
            t_dot(attended_full, middle_full, BF16),
            *(t_dot(normed_full, back, BF16) for back in backs),
            t_dot(last_rows, gate_back, BF16),
            t_dot(last_rows, up_back, BF16),
            small,
        ],
        [11, 4, 4, 4, 4, 4, 4, 1],
    )
    lowering_wgrad, mixing_wgrad = totals[0], totals[1]
    sums = totals[7].reshape(-1)
    projection_bgrad = sums[4 * local_width : 4 * local_width + projection_bgrad.shape[0]]
    return (
        block_output,
        input_grad,
        sums[:local_width],
        sums[local_width : 2 * local_width],
        jnp.stack(totals[2:5], 1).astype(F32),
        projection_bgrad.reshape(3, -1),
        mixing_wgrad.astype(F32),
        sums[2 * local_width : 3 * local_width],
        sums[3 * local_width : 4 * local_width],
        tie(
            jnp.stack([jnp.concatenate([gating_sums[k], totals[5 + k]]) for k in range(2)], 1)
        ).astype(F32),
        lowering_wgrad.astype(F32),
    )


def solution(mesh):
    return jax.shard_map(
        local,
        mesh=mesh,
        in_specs=(
            P(("dp", "col"), "row"),
            P("dp", None),
            P("dp", None),
            P("row"),
            P("row"),
            P("row", None, "col"),
            P(None, "col"),
            P("col", "row"),
            P("row"),
            P("row"),
            P("row", None, "col"),
            P("col", "row"),
            P(("dp", "col"), "row"),
        ),
        out_specs=(
            P(("dp", "col"), "row"),
            P(("dp", "col"), "row"),
            P("row"),
            P("row"),
            P("row", None, "col"),
            P(None, "col"),
            P("col", "row"),
            P("row"),
            P("row"),
            P("row", None, "col"),
            P("col", "row"),
        ),
        check_vma=False,
    )
```

```python
import functools
import math

import jax
import jax.numpy as jnp
from jax import lax
from jax.experimental import pallas as pl
from jax.experimental.pallas import tpu as pltpu
from jax.sharding import PartitionSpec as P

D = 2048
HD = 64


EPSILON = 1e-05
MASKED = -1e30
WINDOW = 2
LANES = 128
BF16 = jnp.bfloat16
F32 = jnp.float32


def col_swap(values, bit):
    count = lax.axis_size("col")
    return lax.ppermute(values, "col", [(i, i ^ bit) for i in range(count)])


def row_swap(values):
    return lax.ppermute(values, "row", [(0, 1), (1, 0)])


def gather_tokens(values):
    count = lax.axis_size("col")
    if count == 4:
        half = values.shape[0] // 2
        first = col_swap(values, 1)
        second = col_swap(values, 2)
        third_a = col_swap(second[:half], 1)
        third_b = col_swap(first[half:], 2)
        return jnp.concatenate([values, first, second, third_a, third_b], 0)
    bit = 1
    while bit < count:
        values = jnp.concatenate([values, col_swap(values, bit)], 0)
        bit *= 2
    return values


def sum_tokens(partial_rows):
    count = lax.axis_size("col")
    size = partial_rows.shape[0] // count
    if count == 4:
        half = size // 2
        own, first, second, third = (partial_rows[i * size : (i + 1) * size] for i in range(4))
        third = third.astype(BF16)
        got_a = col_swap(third[:half], 1).astype(F32)
        got_b = col_swap(third[half:], 2).astype(F32)
        to_second = jnp.concatenate([second[:half] + got_a, second[half:]], 0).astype(BF16)
        to_first = jnp.concatenate([first[:half], first[half:] + got_b], 0).astype(BF16)
        return own + col_swap(to_first, 1).astype(F32) + col_swap(to_second, 2).astype(F32)
    bit = count // 2
    while bit:
        kept = partial_rows.shape[0] // 2
        got = col_swap(partial_rows[kept:].astype(BF16), bit).astype(F32)
        partial_rows = partial_rows[:kept] + got
        bit //= 2
    return partial_rows


def row_sums(first, second):
    return lax.psum((first, second), "row")


def normalize(values):
    total, squares = row_sums(
        jnp.sum(values, 1, keepdims=True), jnp.sum(values * values, 1, keepdims=True)
    )
    center = total / D
    spread = squares / D - center * center
    inverse = lax.rsqrt(spread + EPSILON)
    return ((values - center) * inverse, inverse)


def norm_back(upstream, gain, scaled, inverse):
    weighted = upstream * gain
    total, mixed = row_sums(
        jnp.sum(weighted, 1, keepdims=True), jnp.sum(weighted * scaled, 1, keepdims=True)
    )
    return inverse * (weighted - total / D - scaled * (mixed / D))


def dot(a, b, kind=F32):
    return jnp.dot(a, b, preferred_element_type=F32).astype(kind)


def dot_t(a, b, kind=F32):
    return lax.dot_general(a, b, (((1,), (1,)), ((), ())), preferred_element_type=F32).astype(kind)


def t_dot(a, b, kind=F32):
    return lax.dot_general(a, b, (((0,), (0,)), ((), ())), preferred_element_type=F32).astype(kind)


def line_kernel(pieces, kinds, *refs):
    count = len(kinds)
    own, out = refs[:count], refs[count : 2 * count]
    inwards, part, across = (refs[(2 + k) * count : (3 + k) * count] for k in range(3))
    sent_in, got_in, got_across, sent_out, got_out = refs[5 * count :]
    size = lax.axis_size("dp")
    me = lax.axis_index("dp")
    half = size // 2
    low = me < half
    inner = jnp.where(low, me + 1, me - 1)
    outer = jnp.where(low, jnp.maximum(me - 1, 0), jnp.minimum(me + 1, size - 1))
    end = (me == 0) | (me == size - 1)
    middle = (me == half - 1) | (me == half)

    barrier = pltpu.get_barrier_semaphore()
    pl.semaphore_signal(
        barrier, inc=1, device_id={"dp": inner}, device_id_type=pl.DeviceIdType.MESH
    )

    @pl.when(jnp.logical_not(end))
    def _():
        pl.semaphore_signal(
            barrier, inc=1, device_id={"dp": outer}, device_id_type=pl.DeviceIdType.MESH
        )
        pl.semaphore_wait(barrier, 2)

    @pl.when(end)
    def _():
        pl.semaphore_wait(barrier, 1)

    def copy(source, target, sent, got, to):
        return pltpu.make_async_remote_copy(
            src_ref=source,
            dst_ref=target,
            send_sem=sent,
            recv_sem=got,
            device_id={"dp": to},
            device_id_type=pl.DeviceIdType.MESH,
        )

    def to_inner(k):
        a, start, rows = pieces[k]
        at = pl.ds(start, rows)
        return copy(own[a].at[at], inwards[a].at[at], sent_in.at[k], got_in.at[k], inner)

    def part_to_inner(k):
        a, start, rows = pieces[k]
        at = pl.ds(start, rows)
        return copy(part[a].at[at], inwards[a].at[at], sent_in.at[k], got_in.at[k], inner)

    def part_across(k):
        a, start, rows = pieces[k]
        at = pl.ds(start, rows)
        return copy(part[a].at[at], across[a].at[at], sent_in.at[k], got_across.at[k], inner)

    def to_outer(k):
        a, start, rows = pieces[k]
        at = pl.ds(start, rows)
        return copy(out[a].at[at], out[a].at[at], sent_out.at[k], got_out.at[k], outer)

    def add(first, second, target, k):
        a, start, rows = pieces[k]
        at = pl.ds(start, rows)
        target[a][at] = (
            first[a][at].astype(F32) + second[a][at].astype(F32)
        ).astype(kinds[a])

    total = len(pieces)

    @pl.when(end)
    def _():
        for k in range(total):
            if k >= WINDOW:
                to_inner(k - WINDOW).wait_send()
            to_inner(k).start()
        for k in range(max(total - WINDOW, 0), total):
            to_inner(k).wait_send()
        for k in range(total):
            to_outer(k).wait_recv()

    def inward(k):
        to_inner(k).wait_recv()
        add(own, inwards, part, k)

        @pl.when(middle)
        def _():
            part_across(k).start()

        @pl.when(jnp.logical_not(middle))
        def _():
            part_to_inner(k).start()

    def outward(k):
        @pl.when(middle)
        def _():
            part_across(k).wait_recv()
            add(part, across, out, k)
            to_outer(k).start()

        @pl.when(jnp.logical_not(middle))
        def _():
            to_outer(k).wait_recv()
            to_outer(k).start()

    @pl.when(jnp.logical_not(end))
    def _():
        for k in range(total + 1):
            if k < total:
                inward(k)
            if k:
                outward(k - 1)
        for k in range(total):
            part_across(k).wait_send()
            to_outer(k).wait_send()


def line_sum(arrays, splits):
    pieces = []
    for a, (array, split) in enumerate(zip(arrays, splits)):
        rows = array.shape[0] // split
        pieces += [(a, i * rows, rows) for i in range(split)]
    kinds = [array.dtype for array in arrays]
    vmem = pl.BlockSpec(memory_space=pltpu.VMEM)
    scratch = [pltpu.VMEM(array.shape, array.dtype) for array in arrays]
    sems = [pltpu.SemaphoreType.DMA((len(pieces),)) for _ in range(5)]
    return pl.pallas_call(
        functools.partial(line_kernel, pieces, kinds),
        out_shape=[jax.ShapeDtypeStruct(array.shape, array.dtype) for array in arrays],
        in_specs=[vmem] * len(arrays),
        out_specs=[vmem] * len(arrays),
        scratch_shapes=scratch * 3 + sems,
        compiler_params=pltpu.CompilerParams(
            collective_id=1, has_side_effects=True, vmem_limit_bytes=60 << 20
        ),
        name="line_sum",
    )(*arrays)


def rotary_tables(positions, head_size):
    half = head_size // 8
    lane = jnp.arange(2 * head_size) % head_size
    freq = jnp.exp((lane % half).astype(F32) * (-math.log(10000.0) / half))
    theta = positions.reshape(-1).astype(jnp.float32)[:, None] * freq
    first, second = lane < half, (lane >= half) & (lane < 2 * half)
    sine = jnp.sin(theta)
    return [
        jnp.where(first | second, jnp.cos(theta), 1.0),
        jnp.where(first, -sine, 0.0),
        jnp.where(second, sine, 0.0),
    ]


def scores_of(queries, keys, allowed):
    scores = lax.dot_general(
        queries, keys, (((1,), (1,)), ((), ())), preferred_element_type=F32
    ) * (1.0 / math.sqrt(HD))
    return jnp.where(allowed, scores, MASKED)


def allowed_of(position):
    length = position.shape[0]
    cols = lax.axis_size("col")
    col = lax.axis_index("col")
    own = length * pl.num_programs(0) // cols

    def order_of(axis):
        shape = (length, 1) if axis == 0 else (1, length)
        index = lax.broadcasted_iota(jnp.int32, shape, axis)
        order = jnp.zeros(shape, jnp.int32)
        for k in range(length // own):
            block = pl.program_id(0) * (length // own) + k
            block = 2 * lax.rem(lax.div(col, 2) + lax.div(block, 2), 2) + lax.rem(col + block, 2)
            start = lax.rem(block * own, length)
            order = jnp.where(index >= k * own, start + index - k * own, order)
        return order

    order_q, order_k = order_of(0), order_of(1)
    return (order_k <= order_q) & (order_k >= order_q - position[...])


def attend_kernel(
    q_in, k_in, v_in, q_bias, k_bias, v_bias, same, above, below, position, near_hbm,
    q_out, k_out, v_out, attended_out, total_out, blocks_out, blocks, load_sem, sems,
):
    step = HD // 8
    wide = q_in.shape[1]

    near, far, _ = partners()
    size = blocks.shape[0] // 4
    part = size // 2
    copies = [
        remote(blocks.at[pl.ds(2 * size, part)], blocks.at[pl.ds(3 * size, part)], sems, 0, near),
        remote(
            blocks.at[pl.ds(size + part, part)],
            blocks.at[pl.ds(3 * size + part, part)],
            sems,
            1,
            far,
        ),
        remote(blocks.at[pl.ds(0, part)], blocks.at[pl.ds(size, part)], sems, 2, near),
        remote(blocks.at[pl.ds(part, part)], blocks.at[pl.ds(2 * size + part, part)], sems, 3, far),
    ]
    at_end = (pl.program_id(0) == pl.num_programs(0) - 1) & (
        pl.program_id(1) == pl.num_programs(1) - 1
    )

    @pl.when((pl.program_id(0) == 0) & (pl.program_id(1) == 0))
    def _():
        loads = [
            pltpu.make_async_copy(
                near_hbm.at[pl.ds(k * size, size)],
                blocks.at[pl.ds(k * (size + part), size)],
                load_sem.at[k],
            )
            for k in range(2)
        ]
        for load in loads:
            load.start()
        meet((near, far))
        for load in loads:
            load.wait()
        for copy in copies:
            copy.start()

    def rotate(values):
        return (
            values * same[...]
            + pltpu.roll(values, wide - step, 1) * above[...]
            + pltpu.roll(values, step, 1) * below[...]
        )

    queries = rotate(q_in[...] + q_bias[...]).astype(BF16)
    keys = rotate(k_in[...] + k_bias[...]).astype(BF16)
    values = (v_in[...] + v_bias[...]).astype(BF16)
    q_out[...] = queries
    k_out[...] = keys
    v_out[...] = values
    allowed = allowed_of(position)
    results, totals = [], []
    for h in range(wide // HD):
        at = slice(h * HD, (h + 1) * HD)
        scores = scores_of(queries[:, at], keys[:, at], allowed)
        peak = jnp.max(scores, -1, keepdims=True)
        raised = jnp.exp(scores - peak)
        denominator = jnp.sum(raised, -1, keepdims=True)
        probs = (raised / denominator).astype(BF16)
        results.append(jnp.dot(probs, values[:, at], preferred_element_type=F32))
        totals.append(peak + jnp.log(denominator))
    attended_out[...] = jnp.concatenate(results, 1).astype(BF16)
    total_out[0] = jnp.concatenate(totals, 1)

    @pl.when(at_end)
    def _():
        for copy in copies:
            copy.wait()
        blocks_out[...] = blocks[...]


def attend_back_kernel(
    q_in, k_in, v_in, attended_in, grad_in, total_in, same, above, below, position, q_out, k_out, v_out,
):
    step = HD // 8
    wide = q_in.shape[1]

    def rotate_back(grads):
        return (
            grads * same[...]
            + pltpu.roll(grads * above[...], step, 1)
            + pltpu.roll(grads * below[...], wide - step, 1)
        )

    allowed = allowed_of(position)
    products = grad_in[...].astype(F32) * attended_in[...].astype(F32)
    q_grads, k_grads, v_grads = [], [], []
    for h in range(wide // HD):
        at = slice(h * HD, (h + 1) * HD)
        queries, keys, values = q_in[:, at], k_in[:, at], v_in[:, at]
        grad = grad_in[:, at]
        recovered = jnp.exp(scores_of(queries, keys, allowed) - total_in[0][:, h : h + 1])
        prob_grad = lax.dot_general(
            grad, values, (((1,), (1,)), ((), ())), preferred_element_type=F32
        )
        row_dot = jnp.sum(products[:, at], 1, keepdims=True)
        score_grad = (recovered * (prob_grad - row_dot) * (1.0 / math.sqrt(HD))).astype(BF16)
        q_grads.append(jnp.dot(score_grad, keys, preferred_element_type=F32))
        k_grads.append(t_dot(score_grad, queries))
        v_grads.append(t_dot(recovered.astype(BF16), grad))
    q_out[...] = rotate_back(jnp.concatenate(q_grads, 1)).astype(BF16)
    k_out[...] = rotate_back(jnp.concatenate(k_grads, 1)).astype(BF16)
    v_out[...] = jnp.concatenate(v_grads, 1).astype(BF16)


def attention_specs(tables, seq_len, wide):
    block = pl.BlockSpec((seq_len, wide), lambda s, p: (s, p))
    table = pl.BlockSpec((seq_len, wide), lambda s, p: (s, 0))
    tall = pl.BlockSpec((seq_len, 1), lambda s, p: (s, 0))
    total = pl.BlockSpec((1, seq_len, wide // HD), lambda s, p: (p, s, 0))
    return block, [table] * 3 + [tall], total


def attend(projected, bias, tables, nearby, seq_here, seq_len):
    tokens, piece = projected.shape[0], projected.shape[1] // 3
    wide = 2 * HD
    pairs = piece // wide
    block, extra, total = attention_specs(tables, seq_len, wide)
    shifted = [
        pl.BlockSpec((seq_len, wide), functools.partial(lambda k, s, p: (s, p + k * pairs), k))
        for k in range(3)
    ]
    biases = [
        pl.BlockSpec((1, wide), functools.partial(lambda k, s, p: (0, p + k * pairs), k))
        for k in range(3)
    ]
    whole = jax.ShapeDtypeStruct((tokens, piece), BF16)
    return pl.pallas_call(
        attend_kernel,
        grid=(seq_here, pairs),
        in_specs=shifted + biases + extra + [pl.BlockSpec(memory_space=pl.ANY)],
        out_specs=[block] * 4 + [total, pl.BlockSpec((tokens, nearby.shape[1]), lambda s, p: (0, 0))],
        out_shape=[whole] * 4
        + [
            jax.ShapeDtypeStruct((pairs, tokens, wide // HD), F32),
            jax.ShapeDtypeStruct((tokens, nearby.shape[1]), BF16),
        ],
        scratch_shapes=[
            pltpu.VMEM((tokens, nearby.shape[1]), BF16),
            pltpu.SemaphoreType.DMA((2,)),
            remote_sems(4),
        ],
        compiler_params=pltpu.CompilerParams(
            collective_id=4, has_side_effects=True, vmem_limit_bytes=61 << 20
        ),
        cost_estimate=pl.CostEstimate(
            flops=4 * tokens * seq_len * piece, bytes_accessed=20 * tokens * piece,
            transcendentals=tokens * seq_len * piece // HD,
        ),
        name="attend",
    )(projected, projected, projected, bias, bias, bias, *tables, nearby)


def attend_back(queries, keys, values, attended, grad, total_log, tables, seq_here, seq_len):
    tokens, piece = queries.shape
    wide = 2 * HD
    pairs = piece // wide
    block, extra, total = attention_specs(tables, seq_len, wide)
    whole = jax.ShapeDtypeStruct((tokens, piece), BF16)
    return pl.pallas_call(
        attend_back_kernel,
        grid=(seq_here, pairs),
        in_specs=[block] * 5 + [total] + extra,
        out_specs=[block] * 3,
        out_shape=[whole] * 3,
        cost_estimate=pl.CostEstimate(
            flops=10 * tokens * seq_len * piece, bytes_accessed=20 * tokens * piece,
            transcendentals=tokens * seq_len * piece // HD,
        ),
        name="attend_back",
    )(queries, keys, values, attended, grad, total_log, *tables)


MESH = pl.DeviceIdType.MESH


def partners():
    col = lax.axis_index("col")
    cols = lax.axis_size("col")
    across = lax.rem(col + cols // 2, cols)
    return {"col": col + 1 - 2 * lax.rem(col, 2)}, {"col": across}, {"row": 1 - lax.axis_index("row")}


def meet(devices):
    barrier = pltpu.get_barrier_semaphore()
    for device in devices:
        pl.semaphore_signal(barrier, inc=1, device_id=device, device_id_type=MESH)
    pl.semaphore_wait(barrier, len(devices))


def remote(source, target, sems, k, device):
    return pltpu.make_async_remote_copy(
        src_ref=source,
        dst_ref=target,
        send_sem=sems.at[0, k],
        recv_sem=sems.at[1, k],
        device_id=device,
        device_id_type=MESH,
    )


def remote_sems(count):
    return pltpu.SemaphoreType.DMA((2, count))


def sum_scratch(size, width):
    half = size // 2
    return [
        pltpu.VMEM((3, size, width), BF16),
        pltpu.VMEM((2, half, width), BF16),
        pltpu.VMEM((2, size, width), BF16),
        pltpu.VMEM((2, half, width), F32),
        remote_sems(6),
    ]


def block_sum(part_of, filler, sent, passed, got, kept, sems):
    near, far, _ = partners()
    size = sent.shape[1]
    half = size // 2
    low, high = pl.ds(0, half), pl.ds(half, half)
    copies = [
        remote(sent.at[2, low], passed.at[0], sems, 0, near),
        remote(sent.at[2, high], passed.at[1], sems, 1, far),
        remote(sent.at[0, low], got.at[0, low], sems, 2, near),
        remote(sent.at[1, high], got.at[1, high], sems, 3, far),
        remote(sent.at[1, low], got.at[1, low], sems, 4, far),
        remote(sent.at[0, high], got.at[0, high], sems, 5, near),
    ]
    sent[2] = part_of(3).astype(BF16)
    copies[0].start()
    copies[1].start()
    part = part_of(1)
    sent[0, low] = part[:half].astype(BF16)
    copies[2].start()
    kept[0] = part[half:]
    part = part_of(2)
    sent[1, high] = part[half:].astype(BF16)
    copies[3].start()
    kept[1] = part[:half]
    copies[0].wait_recv()
    sent[1, low] = (kept[1] + passed[0].astype(F32)).astype(BF16)
    copies[4].start()
    copies[1].wait_recv()
    sent[0, high] = (kept[0] + passed[1].astype(F32)).astype(BF16)
    copies[5].start()
    own = part_of(0)
    filler()
    for copy in copies[2:]:
        copy.wait_recv()
    own = own + got[0].astype(F32) + got[1].astype(F32)
    for copy in copies:
        copy.wait_send()
    return own


def block_gather(blocks, use, sems):
    near, far, _ = partners()
    size = blocks.shape[0] // 4
    half = size // 2
    copies = [
        remote(blocks.at[pl.ds(0, size)], blocks.at[pl.ds(size, size)], sems, 0, near),
        remote(blocks.at[pl.ds(0, size)], blocks.at[pl.ds(2 * size, size)], sems, 1, far),
        remote(
            blocks.at[pl.ds(2 * size, half)], blocks.at[pl.ds(3 * size, half)], sems, 2, near
        ),
        remote(
            blocks.at[pl.ds(size + half, half)],
            blocks.at[pl.ds(3 * size + half, half)],
            sems,
            3,
            far,
        ),
    ]
    copies[0].start()
    copies[1].start()
    use(0)
    copies[1].wait_recv()
    copies[2].start()
    copies[0].wait_recv()
    copies[3].start()
    use(1)
    use(2)
    copies[2].wait_recv()
    copies[3].wait_recv()
    use(3)
    for copy in copies:
        copy.wait_send()


def pair_sums(first, second, stats, sems, k):
    _, _, other = partners()
    lane = lax.broadcasted_iota(jnp.int32, stats.shape[1:], 1)
    stats[0] = jnp.where(lane == 0, first, jnp.where(lane == 1, second, 0.0))
    copy = remote(stats.at[0], stats.at[1], sems, k, other)
    copy.start()
    copy.wait()
    both = stats[0] + stats[1]
    return both[:, 0:1], both[:, 1:2]


def scale_rows(values, stats, sems, k):
    total, squares = pair_sums(
        jnp.sum(values, 1, keepdims=True), jnp.sum(values * values, 1, keepdims=True), stats, sems, k
    )
    center = total / D
    inverse = lax.rsqrt(squares / D - center * center + EPSILON)
    return (values - center) * inverse, inverse


def project_kernel(
    x_in, gain, shift, weight, own_hbm, mixed_hbm,
    full_out, proj_out, scaled_out, inverse_out, near_out, pair_hbm,
    loaded, sent, got, blocks, mixed, pair, stats, load_sem, own_sem, pair_sems, gather_sems, sems,
):
    near, far, other = partners()
    row = lax.axis_index("row")
    size = x_in.shape[0]
    kinds, _, width = weight.shape
    half = width // 2
    load = pltpu.make_async_copy(weight, loaded, load_sem)
    load.start()
    pair_load = pltpu.make_async_copy(mixed_hbm, mixed, pair_sems.at[0])
    pair_load.start()
    pair_store = pltpu.make_async_copy(pair, pair_hbm, pair_sems.at[1])
    own_at = pl.ds(0, size)
    own_load = pltpu.make_async_copy(own_hbm, blocks.at[own_at], own_sem)
    own_load.start()
    part = size // 2
    hops = [
        remote(blocks.at[pl.ds(part, part)], blocks.at[pl.ds(size, part)], sems, 5, near),
        remote(blocks.at[pl.ds(0, part)], blocks.at[pl.ds(size + part, part)], sems, 6, far),
    ]
    meet((near, far, other))
    scaled, inverse = scale_rows(x_in[...].astype(F32), stats, sems, 0)
    scaled_out[...] = scaled
    inverse_out[...] = jnp.broadcast_to(inverse, inverse_out.shape)
    full_out[pl.ds(0, size)] = (scaled * gain[...] + shift[...]).astype(BF16)
    mine = pl.ds(pl.multiple_of(row * half, half), half)
    theirs = pl.ds(pl.multiple_of((1 - row) * half, half), half)
    swaps = [
        remote(
            sent.at[pl.ds(b * size, size)], got.at[pl.ds(b * size, size)], sems, 1 + b, other
        )
        for b in range(4)
    ]

    def finish(b):
        at = pl.ds(b * size, size)
        swaps[b].wait_recv()
        proj_out[at] += got[at]

    rows = 16
    steps = mixed.shape[0] // rows

    def split(first, last):
        def body(i, carry):
            at = pl.ds(pl.multiple_of(i * rows, rows), rows)
            values = mixed[at]
            pair[0, at] = values[:, 0]
            pair[1, at] = values[:, 1]
            return carry

        lax.fori_loop(first, last, body, 0)

    def use(b):
        at = pl.ds(b * size, size)
        if b == 0:
            load.wait()
            pair_load.wait()
            split(0, steps * 3 // 4)
        if b == 2:
            split(steps * 3 // 4, steps)
            pair_store.start()
        if b == 1:
            own_load.wait()
            for hop in hops:
                hop.start()
        values = full_out[at]
        for k in range(kinds):
            sent[at, k * half : (k + 1) * half] = dot(values, loaded[k, :, theirs])
        swaps[b].start()
        for k in range(kinds):
            proj_out[at, k * half : (k + 1) * half] = dot(values, loaded[k, :, mine])
        if b == 3:
            for done in range(4):
                finish(done)

    block_gather(full_out, use, gather_sems)
    for swap in swaps:
        swap.wait_send()
    for hop in hops:
        hop.wait()
    near_out[...] = blocks[...]
    pair_store.wait()


def project(x, gain, shift, weight, own, gating):
    size, width = x.shape
    kinds, _, columns = weight.shape
    piece = kinds * columns // 2
    vmem = pl.BlockSpec(memory_space=pltpu.VMEM)
    return pl.pallas_call(
        project_kernel,
        in_specs=[vmem] * 3 + [pl.BlockSpec(memory_space=pl.ANY)] * 3,
        out_specs=[vmem] * 5 + [pl.BlockSpec(memory_space=pl.ANY)],
        out_shape=[
            jax.ShapeDtypeStruct((4 * size, width), BF16),
            jax.ShapeDtypeStruct((4 * size, piece), F32),
            jax.ShapeDtypeStruct((size, width), F32),
            jax.ShapeDtypeStruct((size, LANES), F32),
            jax.ShapeDtypeStruct((2 * size, width), BF16),
            jax.ShapeDtypeStruct((2, gating.shape[0], gating.shape[2]), BF16),
        ],
        scratch_shapes=[
            pltpu.VMEM(weight.shape, BF16),
            pltpu.VMEM((4 * size, piece), F32),
            pltpu.VMEM((4 * size, piece), F32),
            pltpu.VMEM((2 * size, width), BF16),
            pltpu.VMEM(gating.shape, BF16),
            pltpu.VMEM((2, gating.shape[0], gating.shape[2]), BF16),
            pltpu.VMEM((2, size, LANES), F32),
            pltpu.SemaphoreType.DMA,
            pltpu.SemaphoreType.DMA,
            pltpu.SemaphoreType.DMA((2,)),
            remote_sems(4),
            remote_sems(7),
        ],
        compiler_params=pltpu.CompilerParams(
            collective_id=2, has_side_effects=True, vmem_limit_bytes=60 << 20
        ),
        name="project",
    )(x, gain, shift, weight, own, gating)


def hidden_kernel(
    attended, mixing, x_in, gain, shift, gating_hbm, upstream_hbm, lowering_hbm,
    middle_out, scaled_out, inverse_out, full_out, hidden_out, gate_out, up_out,
    gate_w, up_w, upstream, lowering, attended_got, back_sent, back_got, back, stats,
    gates_sent, gates_got, gates_kept,
    s_sent, s_passed, s_got, s_kept, s_sems, load_sems, gather_sems, sems,
):
    near, far, other = partners()
    row = lax.axis_index("row")
    size = x_in.shape[0]
    part = size // 2
    depth = attended.shape[1]
    units = gate_w.shape[1]
    loads = [
        pltpu.make_async_copy(source, target, load_sems.at[k])
        for k, (source, target) in enumerate(
            (
                (upstream_hbm, upstream),
                (lowering_hbm, lowering),
                (gating_hbm.at[0], gate_w),
                (gating_hbm.at[1], up_w),
            )
        )
    ]
    for load in loads:
        load.start()
    meet((near, far, other))
    swap = remote(attended, attended_got, sems, 0, other)
    swap.start()

    def rows_of(b, whose):
        return pl.ds(pl.multiple_of(b * size + whose * part, part), part)

    back_swap = remote(back_sent, back_got, sems, 1, other)
    swap.wait_recv()
    mine = pl.ds(pl.multiple_of(row * depth, depth), depth)
    theirs = pl.ds(pl.multiple_of((1 - row) * depth, depth), depth)

    def part_of(b):
        at = pl.ds(b * size, size)
        return dot(attended[at], mixing[mine]) + dot(attended_got[at], mixing[theirs])

    def filler():
        loads[0].wait()
        loads[1].wait()
        for b in range(4):
            back_sent[pl.ds(b * part, part)] = dot_t(
                upstream[rows_of(b, 1 - row)], lowering[...], BF16
            )
        back_swap.start()
        back_swap.wait_recv()
        for b in range(4):
            at = pl.ds(b * part, part)
            back[at] = dot_t(upstream[rows_of(b, row)], lowering[...]) + back_got[at].astype(F32)
        loads[2].wait()
        loads[3].wait()

    middle = x_in[...].astype(F32) + block_sum(
        part_of, filler, s_sent, s_passed, s_got, s_kept, s_sems
    )
    middle_out[...] = middle
    scaled, inverse = scale_rows(middle, stats, sems, 2)
    scaled_out[...] = scaled
    inverse_out[...] = jnp.broadcast_to(inverse, inverse_out.shape)
    full_out[pl.ds(0, size)] = (scaled * gain[...] + shift[...]).astype(BF16)
    gate_swaps = [remote(gates_sent.at[b], gates_got.at[b], sems, 3 + b, other) for b in range(4)]

    def returns(b):
        at = rows_of(b, row)
        return [
            remote(ref.at[at], ref.at[at], sems, 7 + 3 * b + k, other)
            for k, ref in enumerate((gate_out, up_out, hidden_out))
        ]

    def finish(b):
        gate_swaps[b].wait_recv()
        gate = gates_kept[b % 2, :, :units] + gates_got[b, :, :units].astype(F32)
        up = gates_kept[b % 2, :, units:] + gates_got[b, :, units:].astype(F32)
        grad = back[pl.ds(b * part, part)]
        sigmoid = jax.nn.sigmoid(gate)
        at = rows_of(b, row)
        gate_out[at] = (grad * up * sigmoid * (1.0 + gate * (1.0 - sigmoid))).astype(BF16)
        up_out[at] = (grad * gate * sigmoid).astype(BF16)
        hidden_out[at] = (gate * sigmoid * up).astype(BF16)
        for copy in returns(b):
            copy.start()

    def use(b):
        values = full_out[rows_of(b, 1 - row)]
        gates_sent[b, :, :units] = dot(values, gate_w[...], BF16)
        gates_sent[b, :, units:] = dot(values, up_w[...], BF16)
        gate_swaps[b].start()
        values = full_out[rows_of(b, row)]
        gates_kept[b % 2, :, :units] = dot(values, gate_w[...])
        gates_kept[b % 2, :, units:] = dot(values, up_w[...])
        finish(b)

    block_gather(full_out, use, gather_sems)
    swap.wait_send()
    back_swap.wait_send()
    for b in range(4):
        gate_swaps[b].wait_send()
        at = rows_of(b, 1 - row)
        for copy in returns(b):
            copy.wait_send()
        for k, ref in enumerate((gate_out, up_out, hidden_out)):
            remote(ref.at[at], ref.at[at], sems, 7 + 3 * b + k, other).wait_recv()


def hidden_units(attended, mixing, x, gain, shift, gating, upstream, lowering):
    size, width = x.shape
    tokens = 4 * size
    units = gating.shape[2]
    part = size // 2
    vmem = pl.BlockSpec(memory_space=pltpu.VMEM)
    anywhere = pl.BlockSpec(memory_space=pl.ANY)
    return pl.pallas_call(
        hidden_kernel,
        in_specs=[vmem] * 5 + [anywhere] * 3,
        out_specs=[vmem] * 7,
        out_shape=[
            jax.ShapeDtypeStruct((size, width), F32),
            jax.ShapeDtypeStruct((size, width), F32),
            jax.ShapeDtypeStruct((size, LANES), F32),
            jax.ShapeDtypeStruct((tokens, width), BF16),
        ]
        + [jax.ShapeDtypeStruct((tokens, units), BF16)] * 3,
        scratch_shapes=[
            pltpu.VMEM(gating.shape[1:], BF16),
            pltpu.VMEM(gating.shape[1:], BF16),
            pltpu.VMEM(upstream.shape, BF16),
            pltpu.VMEM(lowering.shape, BF16),
            pltpu.VMEM(attended.shape, BF16),
            pltpu.VMEM((tokens // 2, units), BF16),
            pltpu.VMEM((tokens // 2, units), BF16),
            pltpu.VMEM((tokens // 2, units), F32),
            pltpu.VMEM((2, size, LANES), F32),
            pltpu.VMEM((4, part, 2 * units), BF16),
            pltpu.VMEM((4, part, 2 * units), BF16),
            pltpu.VMEM((2, part, 2 * units), F32),
            *sum_scratch(size, width),
            pltpu.SemaphoreType.DMA((4,)),
            remote_sems(4),
            remote_sems(19),
        ],
        compiler_params=pltpu.CompilerParams(
            collective_id=3, has_side_effects=True, vmem_limit_bytes=61 << 20
        ),
        name="hidden_units",
    )(attended, mixing, x, gain, shift, gating, upstream, lowering)


def local(
    block_input,
    segment_ids,
    positions,
    attention_gain,
    attention_shift,
    projection_weight,
    projection_bias,
    mixing_weight,
    feedforward_gain,
    feedforward_shift,
    gating_weight,
    lowering_weight,
    cotangent,
):
    own_tokens, local_width = block_input.shape
    seq_here, seq_len = segment_ids.shape
    tokens = seq_here * seq_len
    row = lax.axis_index("row")
    col = lax.axis_index("col")
    cols = lax.axis_size("col")
    tie = lax.optimization_barrier

    def mine(values, axis):
        size = values.shape[axis] // 2
        return lax.dynamic_slice_in_dim(values, row * size, size, axis)

    def theirs(values, axis):
        size = values.shape[axis] // 2
        return lax.dynamic_slice_in_dim(values, (1 - row) * size, size, axis)

    def both(values, axis):
        other = row_swap(values)
        return jnp.concatenate(
            [jnp.where(row == 0, values, other), jnp.where(row == 0, other, values)], axis
        )

    def reorder(table):
        blocks = table.reshape(cols, own_tokens)
        return jnp.take(blocks, col ^ jnp.arange(cols), axis=0).reshape(-1)

    position = reorder(positions)
    tables = rotary_tables(position, HD) + [position[:, None]]

    bias = mine(projection_bias, 1).reshape(1, -1)
    normed_full, projected, scaled_one, inverse_one, nearby, gating_pair = project(
        block_input,
        attention_gain[None],
        attention_shift[None],
        jnp.swapaxes(projection_weight, 0, 1),
        cotangent,
        gating_weight,
    )
    inverse_one = inverse_one[:, :1]
    gate_weight, up_weight = gating_pair[0], gating_pair[1]
    queries, keys, values, attended, total_log, upstream_full = attend(
        projected, bias, tables, nearby, seq_here, seq_len
    )
    middle, scaled_two, inverse_two, normed_two_full, hidden_full, gate_back, up_back = (
        hidden_units(
            attended,
            mixing_weight,
            block_input,
            feedforward_gain[None],
            feedforward_shift[None],
            gating_pair,
            upstream_full,
            lowering_weight,
        )
    )
    inverse_two = inverse_two[:, :1]
    attended_full = both(attended, 1)

    early = local_width * 11 // 16
    first_rows, last_rows = normed_two_full[:, :early], normed_two_full[:, early:]
    parts = (t_dot(first_rows, gate_back, BF16), t_dot(first_rows, up_back, BF16))
    gate_back, up_back, parts = tie((gate_back, up_back, parts))
    gating_sums = lax.psum(parts, "dp")

    normed_two_grad = sum_tokens(dot_t(gate_back, gate_weight) + dot_t(up_back, up_weight))
    middle_grad = cotangent.astype(jnp.float32) + norm_back(
        normed_two_grad, feedforward_gain, scaled_two, inverse_two
    )
    middle_wire = middle_grad.astype(jnp.bfloat16)
    middle_full = gather_tokens(middle_wire)
    attended_sent = row_swap(dot_t(middle_full, theirs(mixing_weight, 0), BF16))
    attended_grad = dot_t(middle_full, mine(mixing_weight, 0)) + attended_sent.astype(F32)
    grads = attend_back(
        queries, keys, values, attended, attended_grad.astype(BF16), total_log, tables,
        seq_here, seq_len,
    )
    backs = [both(grad, 1) for grad in grads]
    projection_bgrad = jnp.concatenate([jnp.sum(back, 0, dtype=F32) for back in backs])
    normed_one_grad = sum_tokens(
        sum(dot_t(back, projection_weight[:, i]) for i, back in enumerate(backs))
    )
    input_grad = (
        middle_grad + norm_back(normed_one_grad, attention_gain, scaled_one, inverse_one)
    ).astype(jnp.bfloat16)
    block_output = (middle + sum_tokens(dot(hidden_full, lowering_weight))).astype(jnp.bfloat16)

    sums = jnp.concatenate(
        [
            jnp.sum(normed_one_grad * scaled_one, 0),
            jnp.sum(normed_one_grad, 0),
            jnp.sum(normed_two_grad * scaled_two, 0),
            jnp.sum(normed_two_grad, 0),
        ]
    )
    bit = 1
    while bit < cols:
        sums = sums + col_swap(sums, bit)
        bit *= 2
    small = jnp.concatenate([sums, projection_bgrad])
    lanes = 128
    unit = 8 * lanes
    small = jnp.pad(small, (0, -small.shape[0] % unit)).reshape(-1, lanes)

    totals = line_sum(
        [
            t_dot(hidden_full, upstream_full, BF16),
            t_dot(attended_full, middle_full, BF16),
            *(t_dot(normed_full, back, BF16) for back in backs),
            t_dot(last_rows, gate_back, BF16),
            t_dot(last_rows, up_back, BF16),
            small,
        ],
        [11, 4, 4, 4, 4, 4, 4, 1],
    )
    lowering_wgrad, mixing_wgrad = totals[0], totals[1]
    sums = totals[7].reshape(-1)
    projection_bgrad = sums[4 * local_width : 4 * local_width + projection_bgrad.shape[0]]
    return (
        block_output,
        input_grad,
        sums[:local_width],
        sums[local_width : 2 * local_width],
        jnp.stack(totals[2:5], 1).astype(F32),
        projection_bgrad.reshape(3, -1),
        mixing_wgrad.astype(F32),
        sums[2 * local_width : 3 * local_width],
        sums[3 * local_width : 4 * local_width],
        tie(
            jnp.stack([jnp.concatenate([gating_sums[k], totals[5 + k]]) for k in range(2)], 1)
        ).astype(F32),
        lowering_wgrad.astype(F32),
    )


def solution(mesh):
    return jax.shard_map(
        local,
        mesh=mesh,
        in_specs=(
            P(("dp", "col"), "row"),
            P("dp", None),
            P("dp", None),
            P("row"),
            P("row"),
            P("row", None, "col"),
            P(None, "col"),
            P("col", "row"),
            P("row"),
            P("row"),
            P("row", None, "col"),
            P("col", "row"),
            P(("dp", "col"), "row"),
        ),
        out_specs=(
            P(("dp", "col"), "row"),
            P(("dp", "col"), "row"),
            P("row"),
            P("row"),
            P("row", None, "col"),
            P(None, "col"),
            P("col", "row"),
            P("row"),
            P("row"),
            P("row", None, "col"),
            P("col", "row"),
        ),
        check_vma=False,
    )
```

```python
import functools
import math

import jax
import jax.numpy as jnp
from jax import lax
from jax.experimental import pallas as pl
from jax.experimental.pallas import tpu as pltpu
from jax.sharding import PartitionSpec as P

D = 2048
HD = 64


EPSILON = 1e-05
MASKED = -1e30
WINDOW = 2
LANES = 128
BF16 = jnp.bfloat16
F32 = jnp.float32


def col_swap(values, bit):
    count = lax.axis_size("col")
    return lax.ppermute(values, "col", [(i, i ^ bit) for i in range(count)])


def row_swap(values):
    return lax.ppermute(values, "row", [(0, 1), (1, 0)])


def gather_tokens(values):
    count = lax.axis_size("col")
    if count == 4:
        half = values.shape[0] // 2
        first = col_swap(values, 1)
        second = col_swap(values, 2)
        third_a = col_swap(second[:half], 1)
        third_b = col_swap(first[half:], 2)
        return jnp.concatenate([values, first, second, third_a, third_b], 0)
    bit = 1
    while bit < count:
        values = jnp.concatenate([values, col_swap(values, bit)], 0)
        bit *= 2
    return values


def sum_tokens(partial_rows):
    count = lax.axis_size("col")
    size = partial_rows.shape[0] // count
    if count == 4:
        half = size // 2
        own, first, second, third = (partial_rows[i * size : (i + 1) * size] for i in range(4))
        third = third.astype(BF16)
        got_a = col_swap(third[:half], 1).astype(F32)
        got_b = col_swap(third[half:], 2).astype(F32)
        to_second = jnp.concatenate([second[:half] + got_a, second[half:]], 0).astype(BF16)
        to_first = jnp.concatenate([first[:half], first[half:] + got_b], 0).astype(BF16)
        return own + col_swap(to_first, 1).astype(F32) + col_swap(to_second, 2).astype(F32)
    bit = count // 2
    while bit:
        kept = partial_rows.shape[0] // 2
        got = col_swap(partial_rows[kept:].astype(BF16), bit).astype(F32)
        partial_rows = partial_rows[:kept] + got
        bit //= 2
    return partial_rows


def row_sums(first, second):
    return lax.psum((first, second), "row")


def normalize(values):
    total, squares = row_sums(
        jnp.sum(values, 1, keepdims=True), jnp.sum(values * values, 1, keepdims=True)
    )
    center = total / D
    spread = squares / D - center * center
    inverse = lax.rsqrt(spread + EPSILON)
    return ((values - center) * inverse, inverse)


def norm_back(upstream, gain, scaled, inverse):
    weighted = upstream * gain
    total, mixed = row_sums(
        jnp.sum(weighted, 1, keepdims=True), jnp.sum(weighted * scaled, 1, keepdims=True)
    )
    return inverse * (weighted - total / D - scaled * (mixed / D))


def dot(a, b, kind=F32):
    return jnp.dot(a, b, preferred_element_type=F32).astype(kind)


def dot_t(a, b, kind=F32):
    return lax.dot_general(a, b, (((1,), (1,)), ((), ())), preferred_element_type=F32).astype(kind)


def t_dot(a, b, kind=F32):
    return lax.dot_general(a, b, (((0,), (0,)), ((), ())), preferred_element_type=F32).astype(kind)


def line_kernel(pieces, kinds, *refs):
    count = len(kinds)
    own, out = refs[:count], refs[count : 2 * count]
    inwards, part, across = (refs[(2 + k) * count : (3 + k) * count] for k in range(3))
    sent_in, got_in, got_across, sent_out, got_out = refs[5 * count :]
    size = lax.axis_size("dp")
    me = lax.axis_index("dp")
    half = size // 2
    low = me < half
    inner = jnp.where(low, me + 1, me - 1)
    outer = jnp.where(low, jnp.maximum(me - 1, 0), jnp.minimum(me + 1, size - 1))
    end = (me == 0) | (me == size - 1)
    middle = (me == half - 1) | (me == half)

    barrier = pltpu.get_barrier_semaphore()
    pl.semaphore_signal(
        barrier, inc=1, device_id={"dp": inner}, device_id_type=pl.DeviceIdType.MESH
    )

    @pl.when(jnp.logical_not(end))
    def _():
        pl.semaphore_signal(
            barrier, inc=1, device_id={"dp": outer}, device_id_type=pl.DeviceIdType.MESH
        )
        pl.semaphore_wait(barrier, 2)

    @pl.when(end)
    def _():
        pl.semaphore_wait(barrier, 1)

    def copy(source, target, sent, got, to):
        return pltpu.make_async_remote_copy(
            src_ref=source,
            dst_ref=target,
            send_sem=sent,
            recv_sem=got,
            device_id={"dp": to},
            device_id_type=pl.DeviceIdType.MESH,
        )

    def to_inner(k):
        a, start, rows = pieces[k]
        at = pl.ds(start, rows)
        return copy(own[a].at[at], inwards[a].at[at], sent_in.at[k], got_in.at[k], inner)

    def part_to_inner(k):
        a, start, rows = pieces[k]
        at = pl.ds(start, rows)
        return copy(part[a].at[at], inwards[a].at[at], sent_in.at[k], got_in.at[k], inner)

    def part_across(k):
        a, start, rows = pieces[k]
        at = pl.ds(start, rows)
        return copy(part[a].at[at], across[a].at[at], sent_in.at[k], got_across.at[k], inner)

    def to_outer(k):
        a, start, rows = pieces[k]
        at = pl.ds(start, rows)
        return copy(out[a].at[at], out[a].at[at], sent_out.at[k], got_out.at[k], outer)

    def add(first, second, target, k):
        a, start, rows = pieces[k]
        at = pl.ds(start, rows)
        target[a][at] = (
            first[a][at].astype(F32) + second[a][at].astype(F32)
        ).astype(kinds[a])

    total = len(pieces)

    @pl.when(end)
    def _():
        for k in range(total):
            if k >= WINDOW:
                to_inner(k - WINDOW).wait_send()
            to_inner(k).start()
        for k in range(max(total - WINDOW, 0), total):
            to_inner(k).wait_send()
        for k in range(total):
            to_outer(k).wait_recv()

    def inward(k):
        to_inner(k).wait_recv()
        add(own, inwards, part, k)

        @pl.when(middle)
        def _():
            part_across(k).start()

        @pl.when(jnp.logical_not(middle))
        def _():
            part_to_inner(k).start()

    def outward(k):
        @pl.when(middle)
        def _():
            part_across(k).wait_recv()
            add(part, across, out, k)
            to_outer(k).start()

        @pl.when(jnp.logical_not(middle))
        def _():
            to_outer(k).wait_recv()
            to_outer(k).start()

    @pl.when(jnp.logical_not(end))
    def _():
        for k in range(total + 1):
            if k < total:
                inward(k)
            if k:
                outward(k - 1)
        for k in range(total):
            part_across(k).wait_send()
            to_outer(k).wait_send()


def line_sum(arrays, splits):
    pieces = []
    for a, (array, split) in enumerate(zip(arrays, splits)):
        rows = array.shape[0] // split
        pieces += [(a, i * rows, rows) for i in range(split)]
    kinds = [array.dtype for array in arrays]
    vmem = pl.BlockSpec(memory_space=pltpu.VMEM)
    scratch = [pltpu.VMEM(array.shape, array.dtype) for array in arrays]
    sems = [pltpu.SemaphoreType.DMA((len(pieces),)) for _ in range(5)]
    return pl.pallas_call(
        functools.partial(line_kernel, pieces, kinds),
        out_shape=[jax.ShapeDtypeStruct(array.shape, array.dtype) for array in arrays],
        in_specs=[vmem] * len(arrays),
        out_specs=[vmem] * len(arrays),
        scratch_shapes=scratch * 3 + sems,
        compiler_params=pltpu.CompilerParams(
            collective_id=1, has_side_effects=True, vmem_limit_bytes=60 << 20
        ),
        name="line_sum",
    )(*arrays)


def rotary_tables(positions, head_size):
    half = head_size // 8
    lane = jnp.arange(2 * head_size) % head_size
    freq = jnp.exp((lane % half).astype(F32) * (-math.log(10000.0) / half))
    theta = positions.reshape(-1).astype(jnp.float32)[:, None] * freq
    first, second = lane < half, (lane >= half) & (lane < 2 * half)
    sine = jnp.sin(theta)
    return [
        jnp.where(first | second, jnp.cos(theta), 1.0),
        jnp.where(first, -sine, 0.0),
        jnp.where(second, sine, 0.0),
    ]


def scores_of(queries, keys, allowed):
    scores = lax.dot_general(
        queries, keys, (((1,), (1,)), ((), ())), preferred_element_type=F32
    ) * (1.0 / math.sqrt(HD))
    return jnp.where(allowed, scores, MASKED)


def allowed_of(position):
    length = position.shape[0]
    cols = lax.axis_size("col")
    col = lax.axis_index("col")
    own = length * pl.num_programs(0) // cols

    def order_of(axis):
        shape = (length, 1) if axis == 0 else (1, length)
        index = lax.broadcasted_iota(jnp.int32, shape, axis)
        order = jnp.zeros(shape, jnp.int32)
        for k in range(length // own):
            block = pl.program_id(0) * (length // own) + k
            block = 2 * lax.rem(lax.div(col, 2) + lax.div(block, 2), 2) + lax.rem(col + block, 2)
            start = lax.rem(block * own, length)
            order = jnp.where(index >= k * own, start + index - k * own, order)
        return order

    order_q, order_k = order_of(0), order_of(1)
    return (order_k <= order_q) & (order_k >= order_q - position[...])


def attend_kernel(
    q_in, k_in, v_in, q_bias, k_bias, v_bias, same, above, below, position, near_hbm,
    q_out, k_out, v_out, attended_out, total_out, blocks_out, blocks, load_sem, sems,
):
    step = HD // 8
    wide = q_in.shape[1]

    near, far, _ = partners()
    size = blocks.shape[0] // 4
    part = size // 2
    copies = [
        remote(blocks.at[pl.ds(2 * size, part)], blocks.at[pl.ds(3 * size, part)], sems, 0, near),
        remote(
            blocks.at[pl.ds(size + part, part)],
            blocks.at[pl.ds(3 * size + part, part)],
            sems,
            1,
            far,
        ),
        remote(blocks.at[pl.ds(0, part)], blocks.at[pl.ds(size, part)], sems, 2, near),
        remote(blocks.at[pl.ds(part, part)], blocks.at[pl.ds(2 * size + part, part)], sems, 3, far),
    ]
    at_end = (pl.program_id(0) == pl.num_programs(0) - 1) & (
        pl.program_id(1) == pl.num_programs(1) - 1
    )

    @pl.when((pl.program_id(0) == 0) & (pl.program_id(1) == 0))
    def _():
        loads = [
            pltpu.make_async_copy(
                near_hbm.at[pl.ds(k * size, size)],
                blocks.at[pl.ds(k * (size + part), size)],
                load_sem.at[k],
            )
            for k in range(2)
        ]
        for load in loads:
            load.start()
        meet((near, far))
        for load in loads:
            load.wait()
        for copy in copies:
            copy.start()

    def rotate(values):
        return (
            values * same[...]
            + pltpu.roll(values, wide - step, 1) * above[...]
            + pltpu.roll(values, step, 1) * below[...]
        )

    queries = rotate(q_in[...] + q_bias[...]).astype(BF16)
    keys = rotate(k_in[...] + k_bias[...]).astype(BF16)
    values = (v_in[...] + v_bias[...]).astype(BF16)
    q_out[...] = queries
    k_out[...] = keys
    v_out[...] = values
    allowed = allowed_of(position)
    results, totals = [], []
    for h in range(wide // HD):
        at = slice(h * HD, (h + 1) * HD)
        scores = scores_of(queries[:, at], keys[:, at], allowed)
        peak = jnp.max(scores, -1, keepdims=True)
        raised = jnp.exp(scores - peak)
        denominator = jnp.sum(raised, -1, keepdims=True)
        probs = (raised / denominator).astype(BF16)
        results.append(jnp.dot(probs, values[:, at], preferred_element_type=F32))
        totals.append(peak + jnp.log(denominator))
    attended_out[...] = jnp.concatenate(results, 1).astype(BF16)
    total_out[0] = jnp.concatenate(totals, 1)

    @pl.when(at_end)
    def _():
        for copy in copies:
            copy.wait()
        blocks_out[...] = blocks[...]


def attend_back_kernel(
    q_in, k_in, v_in, attended_in, grad_in, total_in, same, above, below, position, q_out, k_out, v_out,
):
    step = HD // 8
    wide = q_in.shape[1]

    def rotate_back(grads):
        return (
            grads * same[...]
            + pltpu.roll(grads * above[...], step, 1)
            + pltpu.roll(grads * below[...], wide - step, 1)
        )

    allowed = allowed_of(position)
    products = grad_in[...].astype(F32) * attended_in[...].astype(F32)
    q_grads, k_grads, v_grads = [], [], []
    for h in range(wide // HD):
        at = slice(h * HD, (h + 1) * HD)
        queries, keys, values = q_in[:, at], k_in[:, at], v_in[:, at]
        grad = grad_in[:, at]
        recovered = jnp.exp(scores_of(queries, keys, allowed) - total_in[0][:, h : h + 1])
        prob_grad = lax.dot_general(
            grad, values, (((1,), (1,)), ((), ())), preferred_element_type=F32
        )
        row_dot = jnp.sum(products[:, at], 1, keepdims=True)
        score_grad = (recovered * (prob_grad - row_dot) * (1.0 / math.sqrt(HD))).astype(BF16)
        q_grads.append(jnp.dot(score_grad, keys, preferred_element_type=F32))
        k_grads.append(t_dot(score_grad, queries))
        v_grads.append(t_dot(recovered.astype(BF16), grad))
    q_out[...] = rotate_back(jnp.concatenate(q_grads, 1)).astype(BF16)
    k_out[...] = rotate_back(jnp.concatenate(k_grads, 1)).astype(BF16)
    v_out[...] = jnp.concatenate(v_grads, 1).astype(BF16)


def attention_specs(tables, seq_len, wide):
    block = pl.BlockSpec((seq_len, wide), lambda s, p: (s, p))
    table = pl.BlockSpec((seq_len, wide), lambda s, p: (s, 0))
    tall = pl.BlockSpec((seq_len, 1), lambda s, p: (s, 0))
    total = pl.BlockSpec((1, seq_len, wide // HD), lambda s, p: (p, s, 0))
    return block, [table] * 3 + [tall], total


def attend(projected, bias, tables, nearby, seq_here, seq_len):
    tokens, piece = projected.shape[0], projected.shape[1] // 3
    wide = 2 * HD
    pairs = piece // wide
    block, extra, total = attention_specs(tables, seq_len, wide)
    shifted = [
        pl.BlockSpec((seq_len, wide), functools.partial(lambda k, s, p: (s, p + k * pairs), k))
        for k in range(3)
    ]
    biases = [
        pl.BlockSpec((1, wide), functools.partial(lambda k, s, p: (0, p + k * pairs), k))
        for k in range(3)
    ]
    whole = jax.ShapeDtypeStruct((tokens, piece), BF16)
    return pl.pallas_call(
        attend_kernel,
        grid=(seq_here, pairs),
        in_specs=shifted + biases + extra + [pl.BlockSpec(memory_space=pl.ANY)],
        out_specs=[block] * 4 + [total, pl.BlockSpec((tokens, nearby.shape[1]), lambda s, p: (0, 0))],
        out_shape=[whole] * 4
        + [
            jax.ShapeDtypeStruct((pairs, tokens, wide // HD), F32),
            jax.ShapeDtypeStruct((tokens, nearby.shape[1]), BF16),
        ],
        scratch_shapes=[
            pltpu.VMEM((tokens, nearby.shape[1]), BF16),
            pltpu.SemaphoreType.DMA((2,)),
            remote_sems(4),
        ],
        compiler_params=pltpu.CompilerParams(
            collective_id=4, has_side_effects=True, vmem_limit_bytes=61 << 20
        ),
        cost_estimate=pl.CostEstimate(
            flops=4 * tokens * seq_len * piece, bytes_accessed=20 * tokens * piece,
            transcendentals=tokens * seq_len * piece // HD,
        ),
        name="attend",
    )(projected, projected, projected, bias, bias, bias, *tables, nearby)


def attend_back(queries, keys, values, attended, grad, total_log, tables, seq_here, seq_len):
    tokens, piece = queries.shape
    wide = 2 * HD
    pairs = piece // wide
    block, extra, total = attention_specs(tables, seq_len, wide)
    whole = jax.ShapeDtypeStruct((tokens, piece), BF16)
    return pl.pallas_call(
        attend_back_kernel,
        grid=(seq_here, pairs),
        in_specs=[block] * 5 + [total] + extra,
        out_specs=[block] * 3,
        out_shape=[whole] * 3,
        cost_estimate=pl.CostEstimate(
            flops=10 * tokens * seq_len * piece, bytes_accessed=20 * tokens * piece,
            transcendentals=tokens * seq_len * piece // HD,
        ),
        name="attend_back",
    )(queries, keys, values, attended, grad, total_log, *tables)


MESH = pl.DeviceIdType.MESH


def partners():
    col = lax.axis_index("col")
    cols = lax.axis_size("col")
    across = lax.rem(col + cols // 2, cols)
    return {"col": col + 1 - 2 * lax.rem(col, 2)}, {"col": across}, {"row": 1 - lax.axis_index("row")}


def meet(devices):
    barrier = pltpu.get_barrier_semaphore()
    for device in devices:
        pl.semaphore_signal(barrier, inc=1, device_id=device, device_id_type=MESH)
    pl.semaphore_wait(barrier, len(devices))


def remote(source, target, sems, k, device):
    return pltpu.make_async_remote_copy(
        src_ref=source,
        dst_ref=target,
        send_sem=sems.at[0, k],
        recv_sem=sems.at[1, k],
        device_id=device,
        device_id_type=MESH,
    )


def remote_sems(count):
    return pltpu.SemaphoreType.DMA((2, count))


def sum_scratch(size, width):
    half = size // 2
    return [
        pltpu.VMEM((3, size, width), BF16),
        pltpu.VMEM((2, half, width), BF16),
        pltpu.VMEM((2, size, width), BF16),
        pltpu.VMEM((2, half, width), F32),
        remote_sems(6),
    ]


def block_sum(part_of, filler, sent, passed, got, kept, sems):
    near, far, _ = partners()
    size = sent.shape[1]
    half = size // 2
    low, high = pl.ds(0, half), pl.ds(half, half)
    copies = [
        remote(sent.at[2, low], passed.at[0], sems, 0, near),
        remote(sent.at[2, high], passed.at[1], sems, 1, far),
        remote(sent.at[0, low], got.at[0, low], sems, 2, near),
        remote(sent.at[1, high], got.at[1, high], sems, 3, far),
        remote(sent.at[1, low], got.at[1, low], sems, 4, far),
        remote(sent.at[0, high], got.at[0, high], sems, 5, near),
    ]
    sent[2] = part_of(3).astype(BF16)
    copies[0].start()
    copies[1].start()
    part = part_of(1)
    sent[0, low] = part[:half].astype(BF16)
    copies[2].start()
    kept[0] = part[half:]
    part = part_of(2)
    sent[1, high] = part[half:].astype(BF16)
    copies[3].start()
    kept[1] = part[:half]
    copies[0].wait_recv()
    sent[1, low] = (kept[1] + passed[0].astype(F32)).astype(BF16)
    copies[4].start()
    copies[1].wait_recv()
    sent[0, high] = (kept[0] + passed[1].astype(F32)).astype(BF16)
    copies[5].start()
    own = part_of(0)
    filler()
    for copy in copies[2:]:
        copy.wait_recv()
    own = own + got[0].astype(F32) + got[1].astype(F32)
    for copy in copies:
        copy.wait_send()
    return own


def block_gather(blocks, use, sems):
    near, far, _ = partners()
    size = blocks.shape[0] // 4
    half = size // 2
    copies = [
        remote(blocks.at[pl.ds(0, size)], blocks.at[pl.ds(size, size)], sems, 0, near),
        remote(blocks.at[pl.ds(0, size)], blocks.at[pl.ds(2 * size, size)], sems, 1, far),
        remote(
            blocks.at[pl.ds(2 * size, half)], blocks.at[pl.ds(3 * size, half)], sems, 2, near
        ),
        remote(
            blocks.at[pl.ds(size + half, half)],
            blocks.at[pl.ds(3 * size + half, half)],
            sems,
            3,
            far,
        ),
    ]
    copies[0].start()
    copies[1].start()
    use(0)
    copies[1].wait_recv()
    copies[2].start()
    copies[0].wait_recv()
    copies[3].start()
    use(1)
    use(2)
    copies[2].wait_recv()
    copies[3].wait_recv()
    use(3)
    for copy in copies:
        copy.wait_send()


def pair_sums(first, second, stats, sems, k):
    _, _, other = partners()
    lane = lax.broadcasted_iota(jnp.int32, stats.shape[1:], 1)
    stats[0] = jnp.where(lane == 0, first, jnp.where(lane == 1, second, 0.0))
    copy = remote(stats.at[0], stats.at[1], sems, k, other)
    copy.start()
    copy.wait()
    both = stats[0] + stats[1]
    return both[:, 0:1], both[:, 1:2]


def scale_rows(values, stats, sems, k):
    total, squares = pair_sums(
        jnp.sum(values, 1, keepdims=True), jnp.sum(values * values, 1, keepdims=True), stats, sems, k
    )
    center = total / D
    inverse = lax.rsqrt(squares / D - center * center + EPSILON)
    return (values - center) * inverse, inverse


def project_kernel(
    x_in, gain, shift, weight, own_hbm, mixed_hbm,
    full_out, proj_out, scaled_out, inverse_out, near_out, pair_hbm,
    loaded, sent, got, blocks, mixed, pair, stats, load_sem, own_sem, pair_sems, gather_sems, sems,
):
    near, far, other = partners()
    row = lax.axis_index("row")
    size = x_in.shape[0]
    kinds, _, width = weight.shape
    half = width // 2
    load = pltpu.make_async_copy(weight, loaded, load_sem)
    load.start()
    pair_load = pltpu.make_async_copy(mixed_hbm, mixed, pair_sems.at[0])
    pair_load.start()
    pair_store = pltpu.make_async_copy(pair, pair_hbm, pair_sems.at[1])
    own_at = pl.ds(0, size)
    own_load = pltpu.make_async_copy(own_hbm, blocks.at[own_at], own_sem)
    own_load.start()
    part = size // 2
    hops = [
        remote(blocks.at[pl.ds(part, part)], blocks.at[pl.ds(size, part)], sems, 5, near),
        remote(blocks.at[pl.ds(0, part)], blocks.at[pl.ds(size + part, part)], sems, 6, far),
    ]
    meet((near, far, other))
    scaled, inverse = scale_rows(x_in[...].astype(F32), stats, sems, 0)
    scaled_out[...] = scaled
    inverse_out[...] = jnp.broadcast_to(inverse, inverse_out.shape)
    full_out[pl.ds(0, size)] = (scaled * gain[...] + shift[...]).astype(BF16)
    mine = pl.ds(pl.multiple_of(row * half, half), half)
    theirs = pl.ds(pl.multiple_of((1 - row) * half, half), half)
    swaps = [
        remote(
            sent.at[pl.ds(b * size, size)], got.at[pl.ds(b * size, size)], sems, 1 + b, other
        )
        for b in range(4)
    ]

    def finish(b):
        at = pl.ds(b * size, size)
        swaps[b].wait_recv()
        proj_out[at] += got[at]

    rows = 16
    steps = mixed.shape[0] // rows

    def split(first, last):
        def body(i, carry):
            at = pl.ds(pl.multiple_of(i * rows, rows), rows)
            values = mixed[at]
            pair[0, at] = values[:, 0]
            pair[1, at] = values[:, 1]
            return carry

        lax.fori_loop(first, last, body, 0)

    def use(b):
        at = pl.ds(b * size, size)
        if b == 0:
            load.wait()
            pair_load.wait()
            split(0, steps * 3 // 4)
        if b == 2:
            split(steps * 3 // 4, steps)
            pair_store.start()
        if b == 1:
            own_load.wait()
            for hop in hops:
                hop.start()
        values = full_out[at]
        for k in range(kinds):
            sent[at, k * half : (k + 1) * half] = dot(values, loaded[k, :, theirs])
        swaps[b].start()
        for k in range(kinds):
            proj_out[at, k * half : (k + 1) * half] = dot(values, loaded[k, :, mine])
        if b == 3:
            for done in range(4):
                finish(done)

    block_gather(full_out, use, gather_sems)
    for swap in swaps:
        swap.wait_send()
    for hop in hops:
        hop.wait()
    near_out[...] = blocks[...]
    pair_store.wait()


def project(x, gain, shift, weight, own, gating):
    size, width = x.shape
    kinds, _, columns = weight.shape
    piece = kinds * columns // 2
    vmem = pl.BlockSpec(memory_space=pltpu.VMEM)
    return pl.pallas_call(
        project_kernel,
        in_specs=[vmem] * 3 + [pl.BlockSpec(memory_space=pl.ANY)] * 3,
        out_specs=[vmem] * 5 + [pl.BlockSpec(memory_space=pl.ANY)],
        out_shape=[
            jax.ShapeDtypeStruct((4 * size, width), BF16),
            jax.ShapeDtypeStruct((4 * size, piece), F32),
            jax.ShapeDtypeStruct((size, width), F32),
            jax.ShapeDtypeStruct((size, LANES), F32),
            jax.ShapeDtypeStruct((2 * size, width), BF16),
            jax.ShapeDtypeStruct((2, gating.shape[0], gating.shape[2]), BF16),
        ],
        scratch_shapes=[
            pltpu.VMEM(weight.shape, BF16),
            pltpu.VMEM((4 * size, piece), F32),
            pltpu.VMEM((4 * size, piece), F32),
            pltpu.VMEM((2 * size, width), BF16),
            pltpu.VMEM(gating.shape, BF16),
            pltpu.VMEM((2, gating.shape[0], gating.shape[2]), BF16),
            pltpu.VMEM((2, size, LANES), F32),
            pltpu.SemaphoreType.DMA,
            pltpu.SemaphoreType.DMA,
            pltpu.SemaphoreType.DMA((2,)),
            remote_sems(4),
            remote_sems(7),
        ],
        compiler_params=pltpu.CompilerParams(
            collective_id=2, has_side_effects=True, vmem_limit_bytes=60 << 20
        ),
        name="project",
    )(x, gain, shift, weight, own, gating)


def hidden_kernel(
    attended, mixing, x_in, gain, shift, gating_hbm, upstream_hbm, lowering_hbm,
    middle_hbm, scaled_hbm, inverse_out, full_hbm, hidden_hbm, gate_hbm, up_hbm,
    middle_out, scaled_out, full_out, hidden_out, gate_out, up_out, row_sems, unit_sems,
    gate_w, up_w, upstream, lowering, attended_got, back_sent, back_got, back, stats,
    gates_sent, gates_got, gates_kept,
    s_sent, s_passed, s_got, s_kept, s_sems, load_sems, gather_sems, sems,
):
    near, far, other = partners()
    row = lax.axis_index("row")
    size = x_in.shape[0]
    part = size // 2
    depth = attended.shape[1]
    units = gate_w.shape[1]
    loads = [
        pltpu.make_async_copy(source, target, load_sems.at[k])
        for k, (source, target) in enumerate(
            (
                (upstream_hbm, upstream),
                (lowering_hbm, lowering),
                (gating_hbm.at[0], gate_w),
                (gating_hbm.at[1], up_w),
            )
        )
    ]
    for load in loads:
        load.start()
    meet((near, far, other))
    swap = remote(attended, attended_got, sems, 0, other)
    swap.start()

    def rows_of(b, whose):
        return pl.ds(pl.multiple_of(b * size + whose * part, part), part)

    back_swap = remote(back_sent, back_got, sems, 1, other)
    swap.wait_recv()
    mine = pl.ds(pl.multiple_of(row * depth, depth), depth)
    theirs = pl.ds(pl.multiple_of((1 - row) * depth, depth), depth)

    def part_of(b):
        at = pl.ds(b * size, size)
        return dot(attended[at], mixing[mine]) + dot(attended_got[at], mixing[theirs])

    def filler():
        loads[0].wait()
        loads[1].wait()
        for b in range(4):
            back_sent[pl.ds(b * part, part)] = dot_t(
                upstream[rows_of(b, 1 - row)], lowering[...], BF16
            )
        back_swap.start()
        back_swap.wait_recv()
        for b in range(4):
            at = pl.ds(b * part, part)
            back[at] = dot_t(upstream[rows_of(b, row)], lowering[...]) + back_got[at].astype(F32)
        loads[2].wait()
        loads[3].wait()

    middle = x_in[...].astype(F32) + block_sum(
        part_of, filler, s_sent, s_passed, s_got, s_kept, s_sems
    )
    middle_out[...] = middle
    stores = [
        pltpu.make_async_copy(source, target, row_sems.at[k])
        for k, (source, target) in enumerate(
            ((middle_out, middle_hbm), (scaled_out, scaled_hbm), (full_out, full_hbm))
        )
    ]
    stores[0].start()
    scaled, inverse = scale_rows(middle, stats, sems, 2)
    scaled_out[...] = scaled
    stores[1].start()
    inverse_out[...] = jnp.broadcast_to(inverse, inverse_out.shape)
    full_out[pl.ds(0, size)] = (scaled * gain[...] + shift[...]).astype(BF16)
    gate_swaps = [remote(gates_sent.at[b], gates_got.at[b], sems, 3 + b, other) for b in range(4)]

    def returns(b):
        at = rows_of(b, row)
        return [
            remote(ref.at[at], ref.at[at], sems, 7 + 3 * b + k, other)
            for k, ref in enumerate((gate_out, up_out, hidden_out))
        ]

    def unit_stores(b, whose, group):
        at = rows_of(b, whose)
        return [
            pltpu.make_async_copy(source.at[at], target.at[at], unit_sems.at[group, b, k])
            for k, (source, target) in enumerate(
                ((gate_out, gate_hbm), (up_out, up_hbm), (hidden_out, hidden_hbm))
            )
        ]

    def finish(b):
        gate_swaps[b].wait_recv()
        gate = gates_kept[b % 2, :, :units] + gates_got[b, :, :units].astype(F32)
        up = gates_kept[b % 2, :, units:] + gates_got[b, :, units:].astype(F32)
        grad = back[pl.ds(b * part, part)]
        sigmoid = jax.nn.sigmoid(gate)
        at = rows_of(b, row)
        gate_out[at] = (grad * up * sigmoid * (1.0 + gate * (1.0 - sigmoid))).astype(BF16)
        up_out[at] = (grad * gate * sigmoid).astype(BF16)
        hidden_out[at] = (gate * sigmoid * up).astype(BF16)
        for copy in returns(b) + unit_stores(b, row, 0):
            copy.start()

    def use(b):
        if b == 3:
            stores[2].start()
        values = full_out[rows_of(b, 1 - row)]
        gates_sent[b, :, :units] = dot(values, gate_w[...], BF16)
        gates_sent[b, :, units:] = dot(values, up_w[...], BF16)
        gate_swaps[b].start()
        values = full_out[rows_of(b, row)]
        gates_kept[b % 2, :, :units] = dot(values, gate_w[...])
        gates_kept[b % 2, :, units:] = dot(values, up_w[...])
        finish(b)

    block_gather(full_out, use, gather_sems)
    swap.wait_send()
    back_swap.wait_send()
    for b in range(4):
        gate_swaps[b].wait_send()
        at = rows_of(b, 1 - row)
        for copy in returns(b):
            copy.wait_send()
        for k, ref in enumerate((gate_out, up_out, hidden_out)):
            remote(ref.at[at], ref.at[at], sems, 7 + 3 * b + k, other).wait_recv()
        for copy in unit_stores(b, 1 - row, 1):
            copy.start()
    for store in stores:
        store.wait()
    for b in range(4):
        for copy in unit_stores(b, row, 0) + unit_stores(b, 1 - row, 1):
            copy.wait()


def hidden_units(attended, mixing, x, gain, shift, gating, upstream, lowering):
    size, width = x.shape
    tokens = 4 * size
    units = gating.shape[2]
    part = size // 2
    vmem = pl.BlockSpec(memory_space=pltpu.VMEM)
    anywhere = pl.BlockSpec(memory_space=pl.ANY)
    return pl.pallas_call(
        hidden_kernel,
        in_specs=[vmem] * 5 + [anywhere] * 3,
        out_specs=[anywhere] * 2 + [vmem] + [anywhere] * 4,
        out_shape=[
            jax.ShapeDtypeStruct((size, width), F32),
            jax.ShapeDtypeStruct((size, width), F32),
            jax.ShapeDtypeStruct((size, LANES), F32),
            jax.ShapeDtypeStruct((tokens, width), BF16),
        ]
        + [jax.ShapeDtypeStruct((tokens, units), BF16)] * 3,
        scratch_shapes=[
            pltpu.VMEM((size, width), F32),
            pltpu.VMEM((size, width), F32),
            pltpu.VMEM((tokens, width), BF16),
            pltpu.VMEM((tokens, units), BF16),
            pltpu.VMEM((tokens, units), BF16),
            pltpu.VMEM((tokens, units), BF16),
            pltpu.SemaphoreType.DMA((3,)),
            pltpu.SemaphoreType.DMA((2, 4, 3)),
            pltpu.VMEM(gating.shape[1:], BF16),
            pltpu.VMEM(gating.shape[1:], BF16),
            pltpu.VMEM(upstream.shape, BF16),
            pltpu.VMEM(lowering.shape, BF16),
            pltpu.VMEM(attended.shape, BF16),
            pltpu.VMEM((tokens // 2, units), BF16),
            pltpu.VMEM((tokens // 2, units), BF16),
            pltpu.VMEM((tokens // 2, units), F32),
            pltpu.VMEM((2, size, LANES), F32),
            pltpu.VMEM((4, part, 2 * units), BF16),
            pltpu.VMEM((4, part, 2 * units), BF16),
            pltpu.VMEM((2, part, 2 * units), F32),
            *sum_scratch(size, width),
            pltpu.SemaphoreType.DMA((4,)),
            remote_sems(4),
            remote_sems(19),
        ],
        compiler_params=pltpu.CompilerParams(
            collective_id=3, has_side_effects=True, vmem_limit_bytes=61 << 20
        ),
        name="hidden_units",
    )(attended, mixing, x, gain, shift, gating, upstream, lowering)


def local(
    block_input,
    segment_ids,
    positions,
    attention_gain,
    attention_shift,
    projection_weight,
    projection_bias,
    mixing_weight,
    feedforward_gain,
    feedforward_shift,
    gating_weight,
    lowering_weight,
    cotangent,
):
    own_tokens, local_width = block_input.shape
    seq_here, seq_len = segment_ids.shape
    tokens = seq_here * seq_len
    row = lax.axis_index("row")
    col = lax.axis_index("col")
    cols = lax.axis_size("col")
    tie = lax.optimization_barrier

    def mine(values, axis):
        size = values.shape[axis] // 2
        return lax.dynamic_slice_in_dim(values, row * size, size, axis)

    def theirs(values, axis):
        size = values.shape[axis] // 2
        return lax.dynamic_slice_in_dim(values, (1 - row) * size, size, axis)

    def both(values, axis):
        other = row_swap(values)
        return jnp.concatenate(
            [jnp.where(row == 0, values, other), jnp.where(row == 0, other, values)], axis
        )

    def reorder(table):
        blocks = table.reshape(cols, own_tokens)
        return jnp.take(blocks, col ^ jnp.arange(cols), axis=0).reshape(-1)

    position = reorder(positions)
    tables = rotary_tables(position, HD) + [position[:, None]]

    bias = mine(projection_bias, 1).reshape(1, -1)
    normed_full, projected, scaled_one, inverse_one, nearby, gating_pair = project(
        block_input,
        attention_gain[None],
        attention_shift[None],
        jnp.swapaxes(projection_weight, 0, 1),
        cotangent,
        gating_weight,
    )
    inverse_one = inverse_one[:, :1]
    gate_weight, up_weight = gating_pair[0], gating_pair[1]
    queries, keys, values, attended, total_log, upstream_full = attend(
        projected, bias, tables, nearby, seq_here, seq_len
    )
    middle, scaled_two, inverse_two, normed_two_full, hidden_full, gate_back, up_back = (
        hidden_units(
            attended,
            mixing_weight,
            block_input,
            feedforward_gain[None],
            feedforward_shift[None],
            gating_pair,
            upstream_full,
            lowering_weight,
        )
    )
    inverse_two = inverse_two[:, :1]
    attended_full = both(attended, 1)

    early = local_width * 11 // 16
    first_rows, last_rows = normed_two_full[:, :early], normed_two_full[:, early:]
    parts = (t_dot(first_rows, gate_back, BF16), t_dot(first_rows, up_back, BF16))
    gate_back, up_back, parts = tie((gate_back, up_back, parts))
    gating_sums = lax.psum(parts, "dp")

    normed_two_grad = sum_tokens(dot_t(gate_back, gate_weight) + dot_t(up_back, up_weight))
    middle_grad = cotangent.astype(jnp.float32) + norm_back(
        normed_two_grad, feedforward_gain, scaled_two, inverse_two
    )
    middle_wire = middle_grad.astype(jnp.bfloat16)
    middle_full = gather_tokens(middle_wire)
    attended_sent = row_swap(dot_t(middle_full, theirs(mixing_weight, 0), BF16))
    attended_grad = dot_t(middle_full, mine(mixing_weight, 0)) + attended_sent.astype(F32)
    grads = attend_back(
        queries, keys, values, attended, attended_grad.astype(BF16), total_log, tables,
        seq_here, seq_len,
    )
    backs = [both(grad, 1) for grad in grads]
    projection_bgrad = jnp.concatenate([jnp.sum(back, 0, dtype=F32) for back in backs])
    normed_one_grad = sum_tokens(
        sum(dot_t(back, projection_weight[:, i]) for i, back in enumerate(backs))
    )
    input_grad = (
        middle_grad + norm_back(normed_one_grad, attention_gain, scaled_one, inverse_one)
    ).astype(jnp.bfloat16)
    block_output = (middle + sum_tokens(dot(hidden_full, lowering_weight))).astype(jnp.bfloat16)

    sums = jnp.concatenate(
        [
            jnp.sum(normed_one_grad * scaled_one, 0),
            jnp.sum(normed_one_grad, 0),
            jnp.sum(normed_two_grad * scaled_two, 0),
            jnp.sum(normed_two_grad, 0),
        ]
    )
    bit = 1
    while bit < cols:
        sums = sums + col_swap(sums, bit)
        bit *= 2
    small = jnp.concatenate([sums, projection_bgrad])
    lanes = 128
    unit = 8 * lanes
    small = jnp.pad(small, (0, -small.shape[0] % unit)).reshape(-1, lanes)

    totals = line_sum(
        [
            t_dot(hidden_full, upstream_full, BF16),
            t_dot(attended_full, middle_full, BF16),
            *(t_dot(normed_full, back, BF16) for back in backs),
            t_dot(last_rows, gate_back, BF16),
            t_dot(last_rows, up_back, BF16),
            small,
        ],
        [11, 4, 4, 4, 4, 4, 4, 1],
    )
    lowering_wgrad, mixing_wgrad = totals[0], totals[1]
    sums = totals[7].reshape(-1)
    projection_bgrad = sums[4 * local_width : 4 * local_width + projection_bgrad.shape[0]]
    return (
        block_output,
        input_grad,
        sums[:local_width],
        sums[local_width : 2 * local_width],
        jnp.stack(totals[2:5], 1).astype(F32),
        projection_bgrad.reshape(3, -1),
        mixing_wgrad.astype(F32),
        sums[2 * local_width : 3 * local_width],
        sums[3 * local_width : 4 * local_width],
        tie(
            jnp.stack([jnp.concatenate([gating_sums[k], totals[5 + k]]) for k in range(2)], 1)
        ).astype(F32),
        lowering_wgrad.astype(F32),
    )


def solution(mesh):
    return jax.shard_map(
        local,
        mesh=mesh,
        in_specs=(
            P(("dp", "col"), "row"),
            P("dp", None),
            P("dp", None),
            P("row"),
            P("row"),
            P("row", None, "col"),
            P(None, "col"),
            P("col", "row"),
            P("row"),
            P("row"),
            P("row", None, "col"),
            P("col", "row"),
            P(("dp", "col"), "row"),
        ),
        out_specs=(
            P(("dp", "col"), "row"),
            P(("dp", "col"), "row"),
            P("row"),
            P("row"),
            P("row", None, "col"),
            P(None, "col"),
            P("col", "row"),
            P("row"),
            P("row"),
            P("row", None, "col"),
            P("col", "row"),
        ),
        check_vma=False,
    )
```
